32 devices in a mesh: ha: 8 (over z, core), wa: 2 (over y), ba: 2 (over x).
Axes of the slice: x: 2, y: 2, z: 4, core: 2. Of those that a mesh axis runs over, the one named last changes fastest.
Arguments:
- tokens: bfloat16 [2, 128, 64, 384], P('ba', 'ha', 'wa'), may hold values from -6 to 6
- cotangent: bfloat16 [2, 128, 64, 384], P('ba', 'ha', 'wa'), may hold values from -6 to 6
- w_qkv: bfloat16 [384, 1152], replicated, may hold values from -0.20412415 to 0.20412415
- w_proj: bfloat16 [384, 384], replicated, may hold values from -0.3125 to 0.3125
- table_logits: float32 [12, 225], replicated, may hold values from -6 to 6
- logit_scale: float32 [12], replicated, may hold values from 1 to 5.5
- gain: float32 [384], replicated, may hold values from 0.5 to 1.5
Outputs:
- d_tokens: bfloat16 [2, 128, 64, 384], P('ba', 'ha', 'wa')
- d_wqkv: float32 [384, 1152], P(None, 'ba')
- d_wproj: float32 [384, 384], P(None, 'ba')
- d_table: float32 [12, 225], replicated
- d_scale: float32 [12], replicated
- d_gain: float32 [384], replicated
The draws below stay inside these ranges and needn't reach their ends.
All inputs are finite; a program needn't handle non-finite values.
Results may differ from the reference program's by a relative error of at most 0.01.
The reference program's roundings to bfloat16 on the way count: a program that leaves them out, or rounds other values in their place, can miss the bound.
Values may be sent and summed in bfloat16 or wider, within the bound.
A program may use at most 64 MiB of HBM per device.

```python
import math
import jax
import jax.numpy as jnp
from jax import lax

HEADS = 12
C = 384
WIN = 8
TABLE = 225
HEIGHT = 128
WIDTH = 64
BATCH = 2


def draw_w_qkv(key, part):
    spread = C ** (-0.5)
    base = jax.random.normal(key, (C, 3 * C), jnp.float32) * spread
    base = jnp.clip(base, -4.0 * spread, 4.0 * spread)
    return base.astype(jnp.bfloat16)


def shard_levels(key, shape, cuts, low, largest):
    factor_of, own = 1.0, jax.random.fold_in(key, 6)
    for dim, shards_of in cuts:
        heights = jnp.exp(jax.random.uniform(jax.random.fold_in(own, dim), (shards_of,), jnp.float32, low / len(cuts), largest / len(cuts)))
        factor_of = factor_of * jnp.repeat(heights, shape[dim] // shards_of).reshape([-1 if axis == dim else 1 for axis in range(len(shape))])
    return factor_of


def normal_values(own_key, shape, deviation, most, shards=(), kind=jnp.bfloat16):
    values = jax.random.normal(own_key, shape, jnp.float32) * deviation
    if len(shards) > 0:
        values = shard_levels(own_key, shape, shards, -0.22, 0.18) * values
    return jnp.clip(values, min=-most, max=most).astype(kind)


def setup_inputs(seed: int = 0) -> dict:
    splits = jax.random.split(jax.random.key(seed), 8)
    return {
        "tokens": normal_values(splits[0], (BATCH, HEIGHT, WIDTH, C), 1.0, 6.0, ((0, 2), (1, 8), (2, 2))),
        "cotangent": normal_values(splits[1], (BATCH, HEIGHT, WIDTH, C), 1.0, 6.0, ((0, 2), (1, 8), (2, 2))),
        "w_qkv": draw_w_qkv(jax.random.fold_in(splits[7], 71), 0),
        "w_proj": normal_values(splits[3], (C, C), C ** -0.5, 0.3125),
        "table_logits": normal_values(splits[4], (HEADS, TABLE), 1.5, 6.0, (), jnp.float32),
        "logit_scale": jnp.clip(jax.random.uniform(splits[5], (HEADS,), jnp.float32, 1.0, 5.5), 1.0, 5.5),
        "gain": jnp.clip(1.0 + 0.1 * jax.random.normal(splits[6], (C,), jnp.float32), 0.5, 1.5),
    }


EPS_NORM = 1e-05
MASK_FILL = -100.0
SCALE_CAP = math.log(100.0)
BIAS_RANGE = 16.0
HIGHEST = lax.Precision.HIGHEST

def coarse_product(form, left, right):
    return jnp.einsum(form, left.astype(jnp.float32), right.astype(jnp.float32), precision=HIGHEST)

def fine_product(form, left, right):
    return jnp.einsum(form, left, right, precision=HIGHEST)

def to_windows(block, window):
    images, height, width, depth = block.shape
    tiles = block.reshape(images, height // window, window, width // window, window, depth)
    tiles = tiles.transpose(0, 1, 3, 2, 4, 5)
    return tiles.reshape(images, height // window * (width // window), window * window, depth)

def from_windows(tiles, images, height, width, window):
    depth = tiles.shape[-1]
    grid = tiles.reshape(images, height // window, width // window, window, window, depth)
    return grid.transpose(0, 1, 3, 2, 4, 5).reshape(images, height, width, depth)

def position_onehot(window):
    places = jnp.arange(window * window, dtype=jnp.int32)
    row_of = places // window
    col_of = places % window
    offset = (row_of[:, None] - row_of[None, :] + window - 1) * (2 * window - 1) + (col_of[:, None] - col_of[None, :] + window - 1)
    entries = jnp.arange((2 * window - 1) ** 2, dtype=jnp.int32)
    return (offset.reshape(-1)[:, None] == entries[None, :]).astype(jnp.float32)

def region_of(coords, extent, window):
    return (coords >= extent - window).astype(jnp.int32) + (coords >= extent - window // 2).astype(jnp.int32)

def region_mask(row_start, col_start, rows, cols, height, width, window):
    row_label = region_of(row_start + jnp.arange(rows, dtype=jnp.int32), height, window)
    col_label = region_of(col_start + jnp.arange(cols, dtype=jnp.int32), width, window)
    labels = row_label[:, None] * 3 + col_label[None, :]
    labels = labels.reshape(rows // window, window, cols // window, window).transpose(0, 2, 1, 3)
    labels = labels.reshape(-1, window * window)
    return jnp.where(labels[:, :, None] != labels[:, None, :], MASK_FILL, 0.0).astype(jnp.float32)

def grads_region(block, grad_block, row_start, col_start, height, width, window, params):
    w_qkv, w_proj, table_logits, logit_scale, gain = params
    images, rows, cols, depth = block.shape
    heads = logit_scale.shape[0]
    head_dim = depth // heads
    tiles = to_windows(block, window)
    grad_tiles = to_windows(grad_block, window)
    count = tiles.shape[1]
    length = window * window
    flat = tiles.reshape(-1, depth)
    qkv = jnp.dot(flat, w_qkv, preferred_element_type=jnp.float32).astype(jnp.bfloat16)
    qkv = qkv.reshape(images, count, length, 3, heads, head_dim)
    query = qkv[:, :, :, 0].astype(jnp.float32)
    keys = qkv[:, :, :, 1].astype(jnp.float32)
    values = qkv[:, :, :, 2]
    query_inv = lax.rsqrt(lax.optimization_barrier(jnp.sum(query * query, -1, keepdims=True)) + 1.0)
    key_inv = lax.rsqrt(lax.optimization_barrier(jnp.sum(keys * keys, -1, keepdims=True)) + 1.0)
    unit_query = query * query_inv
    unit_key = keys * key_inv
    scale = jnp.exp(jnp.minimum(logit_scale, SCALE_CAP))
    onehot = position_onehot(window)
    sigma = jax.nn.sigmoid(table_logits)
    rel_bias = jnp.dot(sigma * BIAS_RANGE, onehot.T, precision=HIGHEST).reshape(heads, length, length)
    mask = region_mask(row_start, col_start, rows, cols, height, width, window)
    cosine = fine_product('bnqhd,bnkhd->bnhqk', unit_query, unit_key)
    scores = scale[:, None, None] * cosine + rel_bias[None, None] + mask[None, :, None]
    top = lax.optimization_barrier(jnp.max(scores, -1, keepdims=True))
    expo = jnp.exp(scores - top)
    probs = expo / lax.optimization_barrier(jnp.sum(expo, -1, keepdims=True))
    probs_low = probs.astype(jnp.bfloat16)
    attended = coarse_product('bnhqk,bnkhd->bnqhd', probs_low, values).astype(jnp.bfloat16).reshape(-1, depth)
    proj = jnp.dot(attended, w_proj, preferred_element_type=jnp.float32)
    centre = proj - lax.optimization_barrier(jnp.mean(proj, -1, keepdims=True))
    inv_std = lax.rsqrt(lax.optimization_barrier(jnp.mean(centre * centre, -1, keepdims=True)) + EPS_NORM)
    normed = centre * inv_std
    upstream = grad_tiles.reshape(-1, depth).astype(jnp.float32)
    d_gain = lax.optimization_barrier(jnp.sum(upstream * normed, 0))
    scaled = upstream * gain
    d_proj = inv_std * (scaled - lax.optimization_barrier(jnp.mean(scaled, -1, keepdims=True)) - normed * lax.optimization_barrier(jnp.mean(scaled * normed, -1, keepdims=True)))
    d_proj = d_proj.astype(jnp.bfloat16)
    d_wproj = jnp.dot(attended.T, d_proj, preferred_element_type=jnp.float32)
    d_att = jnp.dot(d_proj, w_proj.T, preferred_element_type=jnp.float32).astype(jnp.bfloat16)
    d_att = d_att.reshape(images, count, length, heads, head_dim)
    d_probs = coarse_product('bnqhd,bnkhd->bnhqk', d_att, values)
    d_values = coarse_product('bnhqk,bnqhd->bnkhd', probs_low, d_att)
    d_scores = probs * (d_probs - lax.optimization_barrier(jnp.sum(d_probs * probs, -1, keepdims=True)))
    d_bias = lax.optimization_barrier(jnp.sum(d_scores, (0, 1))).reshape(heads, length * length)
    d_table = jnp.dot(d_bias, onehot, precision=HIGHEST) * (BIAS_RANGE * sigma * (1.0 - sigma))
    live = (logit_scale < SCALE_CAP).astype(jnp.float32)
    d_scale = lax.optimization_barrier(jnp.sum(d_scores * cosine, (0, 1, 3, 4))) * scale * live
    d_cos = d_scores * scale[:, None, None]
    d_unit_q = fine_product('bnhqk,bnkhd->bnqhd', d_cos, unit_key)
    d_unit_k = fine_product('bnhqk,bnqhd->bnkhd', d_cos, unit_query)
    d_query = query_inv * (d_unit_q - unit_query * lax.optimization_barrier(jnp.sum(unit_query * d_unit_q, -1, keepdims=True)))
    d_key = key_inv * (d_unit_k - unit_key * lax.optimization_barrier(jnp.sum(unit_key * d_unit_k, -1, keepdims=True)))
    d_qkv = jnp.stack([d_query, d_key, d_values], 3).astype(jnp.bfloat16).reshape(-1, 3 * depth)
    d_wqkv = jnp.dot(flat.T, d_qkv, preferred_element_type=jnp.float32)
    d_flat = jnp.dot(d_qkv, w_qkv.T, preferred_element_type=jnp.float32).astype(jnp.bfloat16)
    d_block = from_windows(d_flat.reshape(images, count, length, depth), images, rows, cols, window)
    return (d_block, (d_wqkv, d_wproj, d_table, d_scale, d_gain))

def reference(tokens, cotangent, w_qkv, w_proj, table_logits, logit_scale, gain):
    shift = WIN // 2
    images, height, width, depth = tokens.shape
    moved = jnp.roll(tokens, (-shift, -shift), axis=(1, 2))
    moved_grad = jnp.roll(cotangent, (-shift, -shift), axis=(1, 2))
    params = (w_qkv, w_proj, table_logits, logit_scale, gain)
    bands = height // WIN
    anchor = jnp.zeros((), jnp.int32)

    def one_band(totals, index):
        image = (index // bands).astype(jnp.int32)
        start = (index % bands * WIN).astype(jnp.int32)
        block = lax.dynamic_slice(moved, (image, start, anchor, anchor), (1, WIN, width, depth))
        grad_block = lax.dynamic_slice(moved_grad, (image, start, anchor, anchor), (1, WIN, width, depth))
        d_block, parts = grads_region(block, grad_block, start, anchor, height, width, WIN, params)
        return (jax.tree.map(jnp.add, totals, parts), d_block[0])
    initial = (jnp.zeros((depth, 3 * depth), jnp.float32), jnp.zeros((depth, depth), jnp.float32), jnp.zeros(table_logits.shape, jnp.float32), jnp.zeros(logit_scale.shape, jnp.float32), jnp.zeros(gain.shape, jnp.float32))
    totals, pieces = lax.scan(one_band, initial, jnp.arange(images * bands, dtype=jnp.int32))
    d_moved = pieces.reshape(images, height, width, depth)
    back = jnp.roll(d_moved, (shift, shift), axis=(1, 2))
    d_tokens = (cotangent.astype(jnp.float32) + back.astype(jnp.float32)).astype(jnp.bfloat16)
    return (d_tokens, totals[0], totals[1], totals[2], totals[3], totals[4])
```

```python
import math

import functools

import jax
import jax.numpy as jnp
import numpy as np
from jax import lax
from jax.experimental import pallas as pl
from jax.experimental.pallas import tpu as pltpu
from jax.sharding import PartitionSpec as P

WIN = 8


EPS_NORM = 1e-05
MASK_FILL = -100.0
SCALE_CAP = math.log(100.0)
BIAS_RANGE = 16.0


def from_behind(block, axis, distance):
    devices = range(lax.axis_size(axis))
    route = [((i - distance) % len(devices), i) for i in devices]
    return lax.ppermute(block, axis, route)


def to_windows(block, window):
    images, height, width, depth = block.shape
    tiles = block.reshape(images, height // window, window, width // window, window, depth)
    tiles = tiles.transpose(0, 1, 3, 2, 4, 5)
    return tiles.reshape(images, height // window * (width // window), window * window, depth)


def from_windows(tiles, images, height, width, window):
    depth = tiles.shape[-1]
    grid = tiles.reshape(images, height // window, width // window, window, window, depth)
    return grid.transpose(0, 1, 3, 2, 4, 5).reshape(images, height, width, depth)


def region_of(coords, extent, window):
    return (coords >= extent - window).astype(jnp.int32) + (coords >= extent - window // 2).astype(
        jnp.int32
    )

GROUP = 4
FWD = 2
BWD = 4
LOG2E = math.log2(math.e)
MESH = pl.DeviceIdType.MESH
VMEM = pl.BlockSpec(memory_space=pltpu.VMEM)
NN = (((1,), (0,)), ((), ()))
NT = (((1,), (1,)), ((), ()))
TN = (((0,), (0,)), ((), ()))


def mxu(left, right, dims):
    return lax.dot_general(left, right, dims, preferred_element_type=jnp.float32)


def split(value):
    high = value.astype(jnp.bfloat16)
    return high, (value - high.astype(jnp.float32)).astype(jnp.bfloat16)


def mxu_fine(left, right, dims):
    high, low = split(left)
    return mxu(high, right, dims) + mxu(low, right, dims)


def same_block(rows, cols, row_size, col_size):
    row = lax.broadcasted_iota(jnp.int32, (rows, cols), 0) // row_size
    col = lax.broadcasted_iota(jnp.int32, (rows, cols), 1) // col_size
    return (row == col).astype(jnp.bfloat16)


def tile_heads(value, width, reps):
    lane = lax.broadcasted_iota(jnp.int32, (1, value.shape[1]), 1) % (GROUP * width) // width
    rows = []
    for head in range(GROUP):
        rows.append(value * (lane == head).astype(jnp.bfloat16))
    return jnp.concatenate(rows, 0)


def gather_heads(value, width, length):
    lane = lax.broadcasted_iota(jnp.int32, (length, value.shape[1]), 1) // width
    total = value[:length]
    for head in range(1, GROUP):
        total = jnp.where(lane == head, value[head * length : (head + 1) * length], total)
    return total


def local_kernel(
    grid_cols, height, width, window,
    flat_ref, grad_ref, w_qkv_ref, w_proj_ref, bias_ref, scale_ref, gain_ref,
    d_flat_ref, d_wqkv_ref, d_wproj_ref, d_bias_ref, d_cos_ref, d_gain_ref,
    qkv_ref, att_ref, d_att_ref, d_qkv_ref, probs_ref, kinv_ref, qrow_ref, masked_ref, raw_q_ref, raw_k_ref,
    norm_ref,
):
    tokens, depth = flat_ref.shape
    f32, b16 = jnp.float32, jnp.bfloat16
    length = window * window
    count = tokens // length
    groups = bias_ref.shape[0]
    lanes = depth // groups
    heads = groups * GROUP
    head_dim = lanes // GROUP
    wide = GROUP * length
    row_base = lax.axis_index("ha") * (count // grid_cols * window)
    col_base = lax.axis_index("wa") * (grid_cols * window)

    qkv_ref[...] = mxu(flat_ref[...], w_qkv_ref[...], NN).astype(b16)
    lane_ones = same_block(lanes, wide, head_dim, length)
    lane_lane = same_block(lanes, lanes, head_dim, head_dim)

    head_rows = scale_ref.shape[0]
    pick = same_block(head_rows, depth, 1, head_dim)
    high, low = split(jnp.square(qkv_ref[:, :depth].astype(f32)))
    q_sums = mxu(pick, high, NT) + mxu(pick, low, NT)
    q_rows = lax.rsqrt(q_sums + 1.0) * scale_ref[:, :1]
    half = lax.broadcasted_iota(jnp.int32, (1, 2 * length), 1) < length
    for j in range(count // 2):
        base = q_rows[:, j * 2 * length : (j + 1) * 2 * length]
        turned = pltpu.roll(base, length, 1)
        for g in range(groups):
            for p in range(GROUP // 2):
                one, two = g * GROUP + 2 * p, g * GROUP + 2 * p + 1
                place = slice(p * 2 * length, (p + 1) * 2 * length)
                qrow_ref[2 * j, g, :, place] = jnp.where(half, base[one : one + 1], turned[two : two + 1])
                qrow_ref[2 * j + 1, g, :, place] = jnp.where(half, turned[one : one + 1], base[two : two + 1])
    for g in range(groups):
        query = qkv_ref[:, g * lanes : (g + 1) * lanes].astype(f32)
        key = qkv_ref[:, depth + g * lanes : depth + (g + 1) * lanes].astype(f32)
        high, low = split(jnp.square(key))
        kinv_ref[g] = lax.rsqrt(mxu(high, lane_ones, NN) + mxu(low, lane_ones, NN) + 1.0)
        norm_ref[1, g] = 1.0 / (mxu(high, lane_lane, NN) + mxu(low, lane_lane, NN) + 1.0)
        high, low = split(jnp.square(query))
        norm_ref[0, g] = 1.0 / (mxu(high, lane_lane, NN) + mxu(low, lane_lane, NN) + 1.0)

    mine = lax.broadcasted_iota(jnp.int32, (length, wide), 0)
    other = lax.broadcasted_iota(jnp.int32, (length, wide), 1) % length
    cut = window // 2
    row_off = (mine // window // cut) != (other // window // cut)
    col_off = (mine % window // cut) != (other % window // cut)
    for g in range(groups):
        bias = bias_ref[g] * LOG2E
        masked_ref[0, g] = bias
        masked_ref[1, g] = jnp.where(col_off, bias + MASK_FILL * LOG2E, bias)
        masked_ref[2, g] = jnp.where(row_off, bias + MASK_FILL * LOG2E, bias)
        masked_ref[3, g] = jnp.where(row_off | col_off, bias + MASK_FILL * LOG2E, bias)

    def load(ref, w, g, part):
        return ref[
            pl.ds(pl.multiple_of(w * length, length), length),
            part * depth + g * lanes : part * depth + (g + 1) * lanes,
        ]

    def forward(step, carry):
        units = [(step * FWD + k, g) for k in range(FWD) for g in range(groups)]
        scores = []
        for w, g in units:
            query, key = load(qkv_ref, w, g, 0), load(qkv_ref, w, g, 1)
            raw = mxu(key, tile_heads(query, head_dim, length), NT)
            last_row = (row_base + w // grid_cols * window) // (height - window)
            last_col = (col_base + w % grid_cols * window) // (width - window)
            kinv = kinv_ref[g, pl.ds(pl.multiple_of(w * length, length), length), :]
            scores.append(raw * kinv * (qrow_ref[w, g] * LOG2E) + masked_ref[last_row * 2 + last_col, g])
        for (w, g), score in zip(units, scores):
            expo = jnp.exp2(score - jnp.max(score, 0, keepdims=True))
            probs = expo * (1.0 / jnp.sum(expo, 0, keepdims=True))
            probs_ref[w, g] = probs
            att = gather_heads(mxu(probs.astype(b16), load(qkv_ref, w, g, 2), TN), head_dim, length)
            att_ref[
                pl.ds(pl.multiple_of(w * length, length), length), g * lanes : (g + 1) * lanes
            ] = att.astype(b16)
        return carry

    lax.fori_loop(0, count // FWD, forward, 0)

    proj = mxu(att_ref[...], w_proj_ref[...], NN)
    centre = proj - jnp.mean(proj, -1, keepdims=True)
    inv_std = lax.rsqrt(jnp.mean(centre * centre, -1, keepdims=True) + EPS_NORM)
    normed = centre * inv_std
    upstream = grad_ref[...].astype(f32)
    d_gain_ref[...] = jnp.sum(upstream * normed, 0, keepdims=True)
    scaled = upstream * gain_ref[...]
    d_proj = inv_std * (
        scaled
        - jnp.mean(scaled, -1, keepdims=True)
        - normed * jnp.mean(scaled * normed, -1, keepdims=True)
    )
    d_proj = d_proj.astype(b16)
    d_wproj_ref[...] = mxu(att_ref[...], d_proj, TN)
    d_att_ref[...] = mxu(d_proj, w_proj_ref[...], NT).astype(b16)
    d_bias_ref[...] = jnp.zeros_like(d_bias_ref)

    for g in range(groups):

        def backward(step, carry):
            units = [step * BWD + k for k in range(BWD)]
            grads = []
            for w in units:
                d_tall = tile_heads(load(d_att_ref, w, g, 0), head_dim, length)
                d_probs = mxu(load(qkv_ref, w, g, 2), d_tall, NT)
                d_value = mxu(probs_ref[w, g].astype(b16), d_tall, NN)
                d_qkv_ref[
                    pl.ds(pl.multiple_of(w * length, length), length),
                    2 * depth + g * lanes : 2 * depth + (g + 1) * lanes,
                ] = d_value.astype(b16)
                grads.append(d_probs)
            total = d_bias_ref[g]
            for w, d_probs in zip(units, grads):
                rows = pl.ds(pl.multiple_of(w * length, length), length)
                probs = probs_ref[w, g]
                d_scores = probs * (d_probs - jnp.sum(d_probs * probs, 0, keepdims=True))
                total = total + d_scores
                high, low = split(d_scores * kinv_ref[g, rows, :] * qrow_ref[w, g])
                both = jnp.concatenate([high, low], 0)
                query, key = load(qkv_ref, w, g, 0), load(qkv_ref, w, g, 1)
                pair = mxu(both, tile_heads(query, head_dim, length), NN)
                raw_k_ref[rows, :] = pair[:length] + pair[length:]
                tall = mxu(both, jnp.concatenate([key, key], 0), TN)
                raw_q_ref[rows, :] = gather_heads(tall, head_dim, length)
            d_bias_ref[g] = total
            return carry

        lax.fori_loop(0, count // BWD, backward, 0)
        for part, ref in enumerate((raw_q_ref, raw_k_ref)):
            place = slice(part * depth + g * lanes, part * depth + (g + 1) * lanes)
            value, grad = qkv_ref[:, place].astype(f32), ref[...]
            along = value * grad
            if part == 0:
                d_cos_ref[g] = jnp.sum(along, 0, keepdims=True)
            d_qkv_ref[:, place] = (
                grad - value * norm_ref[part, g] * mxu_fine(along, lane_lane, NN)
            ).astype(b16)
    d_wqkv_ref[...] = mxu(flat_ref[...], d_qkv_ref[...], TN)
    d_flat_ref[...] = mxu(d_qkv_ref[...], w_qkv_ref[...], NT).astype(b16)


def offset_onehot(window):
    places = np.arange(window * window)
    row_of, col_of = places // window, places % window
    offset = (row_of[:, None] - row_of[None, :] + window - 1) * (2 * window - 1) + (
        col_of[:, None] - col_of[None, :] + window - 1
    )
    return jnp.asarray(offset.reshape(-1), jnp.int32)


def three_parts(value):
    high = lax.reduce_precision(value, 8, 7)
    middle = lax.reduce_precision(value - high, 8, 7)
    return jnp.concatenate([high, middle, value - high - middle], 0).astype(jnp.bfloat16)


def local_grads(block, grad_block, row_base, col_base, height, width, window, params):
    w_qkv, w_proj, table_logits, logit_scale, gain = params
    images, rows, cols, depth = block.shape
    heads = logit_scale.shape[0]
    length = window * window
    groups = heads // GROUP
    wide = GROUP * length
    flat = to_windows(block, window).reshape(-1, depth)
    grad_flat = to_windows(grad_block, window).reshape(-1, depth)
    tokens = flat.shape[0]
    count = tokens // length
    scale = jnp.exp(jnp.minimum(logit_scale, SCALE_CAP))
    scale_rows = jnp.pad(scale, (0, -heads % 16)).reshape(-1, 1) * jnp.ones((1, 128), jnp.float32)
    sigma = jax.nn.sigmoid(table_logits)
    entries = table_logits.shape[1]
    hot = offset_onehot(window)[None, :] == jnp.arange(entries, dtype=jnp.int32)[:, None]
    hot = hot.astype(jnp.bfloat16)
    parts = jnp.dot(three_parts(sigma * BIAS_RANGE), hot, preferred_element_type=jnp.float32)
    rel_bias = jnp.sum(parts.reshape(3, heads, -1), 0).reshape(groups, GROUP, length, length)
    rel_bias = rel_bias.transpose(0, 3, 1, 2).reshape(groups, length, wide)
    f32, b16 = jnp.float32, jnp.bfloat16
    d_flat, d_wqkv, d_wproj, d_bias, d_cos, d_gain = pl.pallas_call(
        functools.partial(local_kernel, cols // window, height, width, window),
        out_shape=[
            jax.ShapeDtypeStruct((tokens, depth), b16),
            jax.ShapeDtypeStruct((depth, 3 * depth), f32),
            jax.ShapeDtypeStruct((depth, depth), f32),
            jax.ShapeDtypeStruct((groups, length, wide), f32),
            jax.ShapeDtypeStruct((groups, 1, depth // groups), f32),
            jax.ShapeDtypeStruct((1, depth), f32),
        ],
        in_specs=[VMEM] * 7,
        out_specs=[VMEM] * 6,
        scratch_shapes=[
            pltpu.VMEM((tokens, 3 * depth), b16),
            pltpu.VMEM((tokens, depth), b16),
            pltpu.VMEM((tokens, depth), b16),
            pltpu.VMEM((tokens, 3 * depth), b16),
            pltpu.VMEM((count, groups, length, wide), f32),
            pltpu.VMEM((groups, tokens, wide), f32),
            pltpu.VMEM((count, groups, 1, wide), f32),
            pltpu.VMEM((4, groups, length, wide), f32),
            pltpu.VMEM((tokens, depth // groups), f32),
            pltpu.VMEM((tokens, depth // groups), f32),
            pltpu.VMEM((2, groups, tokens, depth // groups), f32),
        ],
        compiler_params=pltpu.CompilerParams(vmem_limit_bytes=48 * 2**20),
        cost_estimate=pl.CostEstimate(
            flops=4_000_000_000, bytes_accessed=8_000_000, transcendentals=400_000
        ),
        name="local_grads",
    )(flat, grad_flat, w_qkv, w_proj, rel_bias, scale_rows, gain.reshape(1, depth))
    heads_bias = d_bias.reshape(groups, length, GROUP, length).transpose(0, 2, 3, 1)
    heads_bias = heads_bias.reshape(heads, length * length)
    sums = lax.dot_general(three_parts(heads_bias), hot, NT, preferred_element_type=jnp.float32)
    d_table = jnp.sum(sums.reshape(3, heads, entries), 0) * (BIAS_RANGE * sigma * (1.0 - sigma))
    live = (logit_scale < SCALE_CAP).astype(jnp.float32)
    d_scale = jnp.sum(d_cos.reshape(heads, depth // heads), 1) * live
    d_block = from_windows(d_flat.reshape(images, count, length, depth), images, rows, cols, window)
    return (d_block, (d_wqkv, d_wproj, d_table, d_scale, d_gain.reshape(depth)))


def reduce_kernel(
    shape, wqkv_ref, wproj_ref, small_ref, qkv_out, proj_out, small_out,
    core_send, core_get, image_keep, image_send, image_get, near_send, near_get, own, whole, core_all,
    small_core, small_image, small_a, small_b, small_near,
    core_sems, image_sems, near_sems, all_sems, last_sems, tiny_sems,
):
    size_h, size_w = shape
    chips = size_h // 2
    peers = chips * size_w
    ha, wa, ba = lax.axis_index("ha"), lax.axis_index("wa"), lax.axis_index("ba")
    core = ha % 2
    me = wa * chips + ha // 2
    partner = (ha + 1 - 2 * core, wa, ba)
    image = (ha, wa, 1 - ba)

    def peer(step):
        other = lax.rem(me + step, peers)
        return other, (other % chips * 2 + core, other // chips, ba)

    barrier = pltpu.get_barrier_semaphore()
    pl.semaphore_signal(barrier, inc=1, device_id=partner, device_id_type=MESH)
    pl.semaphore_signal(barrier, inc=1, device_id=image, device_id_type=MESH)
    for step in range(1, peers):
        pl.semaphore_signal(barrier, inc=1, device_id=peer(step)[1], device_id_type=MESH)

    depth = wqkv_ref.shape[0]
    half = depth // 2
    q_half, p_half = wqkv_ref.shape[1] // 2, wproj_ref.shape[1] // 2
    f32, b16 = jnp.float32, jnp.bfloat16
    mine = pl.ds(pl.multiple_of(core * half, 16), half)
    theirs = pl.ds(pl.multiple_of((1 - core) * half, 16), half)
    core_send[:, : 2 * q_half] = wqkv_ref[theirs, :].astype(b16)
    core_send[:, 2 * q_half :] = wproj_ref[theirs, :].astype(b16)
    pl.semaphore_wait(barrier, peers + 1)

    def start(src, dst, sems, device):
        copy = pltpu.make_async_remote_copy(
            src_ref=src, dst_ref=dst, send_sem=sems.at[0], recv_sem=sems.at[1],
            device_id=device, device_id_type=MESH,
        )
        copy.start()
        return copy

    big = start(core_send, core_get, core_sems, partner)
    tiny = start(small_ref, small_core, tiny_sems.at[0], partner)
    tiny.wait()
    small_a[...] = small_ref[...] + small_core[...]
    tiny = start(small_a, small_image, tiny_sems.at[1], image)
    big.wait()

    def halves(first):
        q = wqkv_ref[mine, first * q_half : (first + 1) * q_half]
        p = wproj_ref[mine, first * p_half : (first + 1) * p_half]
        gq = core_get[:, first * q_half : (first + 1) * q_half]
        gp = core_get[:, 2 * q_half + first * p_half : 2 * q_half + (first + 1) * p_half]
        return q + gq.astype(f32), p + gp.astype(f32)

    low, high = halves(0), halves(1)
    for part, (a, b) in enumerate(zip(low, high)):
        place = slice(0, q_half) if part == 0 else slice(q_half, q_half + p_half)
        image_send[:, place] = jnp.where(ba == 0, b, a).astype(b16)
        image_keep[:, place] = jnp.where(ba == 0, a, b)
    big = start(image_send, image_get, image_sems, image)
    tiny.wait()
    small_b[...] = small_a[...] + small_image[...]
    tinies = []
    for step in range(1, peers):
        tinies.append(start(small_b, small_near.at[step - 1], tiny_sems.at[step + 1], peer(step)[1]))
    big.wait()
    total = image_keep[...] + image_get[...].astype(f32)
    r, c = near_send.shape[1:]
    split_c = total.shape[1] // c
    for j in range(peers):
        row, col = j // split_c * r, j % split_c * c
        near_send[j] = total[row : row + r, col : col + c].astype(b16)
    copies = []
    for step in range(1, peers):
        other, device = peer(step)
        copies.append(start(near_send.at[other], near_get.at[step - 1], near_sems.at[step - 1], device))
    for copy in tinies:
        copy.wait()
    small = small_b[...]
    for step in range(1, peers):
        small = small + small_near[step - 1]
    small_out[...] = small
    for copy in copies:
        copy.wait()
    total = near_send[me].astype(f32)
    for step in range(1, peers):
        total = total + near_get[step - 1].astype(f32)
    own[...] = total.astype(b16)
    whole[me] = own[...]
    copies = []
    for step in range(1, peers):
        _, device = peer(step)
        copies.append(start(own, whole.at[me], all_sems.at[step - 1], device))
    for copy in copies:
        copy.wait()
    last = start(whole, core_all, last_sems, partner)

    def put(source, first):
        for j in range(peers):
            row, col = j // split_c * r, j % split_c * c
            block = source[j].astype(f32)
            rows = pl.ds(pl.multiple_of(first * half + row, 8), r)
            q_part = max(0, min(c, q_half - col))
            if q_part > 0:
                qkv_out[rows, col : col + q_part] = block[:, :q_part]
            if q_part < c:
                begin = col + q_part - q_half
                proj_out[rows, begin : begin + c - q_part] = block[:, q_part:]

    put(whole, core)
    last.wait()
    put(core_all, 1 - core)


def reduce_all(d_wqkv, d_wproj, small):
    size_h, size_w = lax.axis_size("ha"), lax.axis_size("wa")
    peers = size_h // 2 * size_w
    depth = d_wqkv.shape[0]
    half = depth // 2
    cols = (d_wqkv.shape[1] + d_wproj.shape[1]) // 2
    split_c = 2
    r, c = half * split_c // peers, cols // split_c
    f32, b16 = jnp.float32, jnp.bfloat16
    tiny = small.shape
    return pl.pallas_call(
        functools.partial(reduce_kernel, (size_h, size_w)),
        out_shape=[
            jax.ShapeDtypeStruct((depth, d_wqkv.shape[1] // 2), f32),
            jax.ShapeDtypeStruct((depth, d_wproj.shape[1] // 2), f32),
            jax.ShapeDtypeStruct(tiny, f32),
        ],
        in_specs=[VMEM] * 3,
        out_specs=[VMEM] * 3,
        scratch_shapes=[
            pltpu.VMEM((half, 2 * cols), b16),
            pltpu.VMEM((half, 2 * cols), b16),
            pltpu.VMEM((half, cols), f32),
            pltpu.VMEM((half, cols), b16),
            pltpu.VMEM((half, cols), b16),
            pltpu.VMEM((peers, r, c), b16),
            pltpu.VMEM((peers - 1, r, c), b16),
            pltpu.VMEM((r, c), b16),
            pltpu.VMEM((peers, r, c), b16),
            pltpu.VMEM((peers, r, c), b16),
            pltpu.VMEM(tiny, f32),
            pltpu.VMEM(tiny, f32),
            pltpu.VMEM(tiny, f32),
            pltpu.VMEM(tiny, f32),
            pltpu.VMEM((peers - 1, *tiny), f32),
            pltpu.SemaphoreType.DMA((2,)),
            pltpu.SemaphoreType.DMA((2,)),
            pltpu.SemaphoreType.DMA((peers - 1, 2)),
            pltpu.SemaphoreType.DMA((peers - 1, 2)),
            pltpu.SemaphoreType.DMA((2,)),
            pltpu.SemaphoreType.DMA((peers + 1, 2)),
        ],
        compiler_params=pltpu.CompilerParams(
            collective_id=0, has_side_effects=True, vmem_limit_bytes=48 * 2**20
        ),
        name="reduce_all",
    )(d_wqkv, d_wproj, small)


def can_reduce(d_wqkv):
    peers = lax.axis_size("ha") // 2 * lax.axis_size("wa")
    pairs = lax.axis_size("ha") % 2 == 0 and lax.axis_size("ba") == 2
    return pairs and peers > 1 and d_wqkv.shape[0] % peers == 0 and d_wqkv.shape[0] // peers % 16 == 0


def pack_small(d_table, d_scale, d_gain):
    heads, entries = d_table.shape
    lanes = -(-entries // 128) * 128
    flat = jnp.concatenate([d_scale, d_gain])
    rows = -(-flat.shape[0] // lanes)
    flat = jnp.pad(flat, (0, rows * lanes - flat.shape[0])).reshape(rows, lanes)
    table = jnp.pad(d_table, ((0, 0), (0, lanes - entries)))
    full = jnp.concatenate([table, flat], 0)
    return jnp.pad(full, ((0, -full.shape[0] % 8), (0, 0)))


def unpack_small(full, heads, entries, depth):
    flat = full[heads:].reshape(-1)
    return full[:heads, :entries], flat[:heads], flat[heads : heads + depth]


def shift_in(tokens, cotangent, shift):
    stacked = jnp.stack([tokens, cotangent])
    below = from_behind(stacked[:, :, :shift], "ha", -1)
    tall = jnp.concatenate([stacked[:, :, shift:], below], 2)
    beside = from_behind(tall[:, :, :, :shift], "wa", -1)
    moved = jnp.concatenate([tall[:, :, :, shift:], beside], 3)
    return (moved[0], moved[1])


def shift_out(grads, shift):
    rows = grads.shape[1]
    cols = grads.shape[2]
    right = from_behind(grads[:, :, cols - shift :], "wa", 1)
    wide = jnp.concatenate([right, grads[:, :, : cols - shift]], 2)
    lower = from_behind(wide[:, rows - shift :], "ha", 1)
    return jnp.concatenate([lower, wide[:, : rows - shift]], 1)


def shards(tokens, cotangent, w_qkv, w_proj, table_logits, logit_scale, gain):
    rows = tokens.shape[1]
    cols = tokens.shape[2]
    shift = WIN // 2
    height = rows * lax.axis_size("ha")
    width = cols * lax.axis_size("wa")
    row_base = lax.axis_index("ha") * rows
    col_base = lax.axis_index("wa") * cols
    params = (w_qkv, w_proj, table_logits, logit_scale, gain)
    moved, moved_grad = shift_in(tokens, cotangent, shift)
    d_moved, parts = local_grads(moved, moved_grad, row_base, col_base, height, width, WIN, params)
    back = shift_out(d_moved, shift)
    d_tokens = (cotangent.astype(jnp.float32) + back.astype(jnp.float32)).astype(jnp.bfloat16)
    d_wqkv, d_wproj, d_table, d_scale, d_gain = parts
    if can_reduce(d_wqkv):
        small = pack_small(d_table, d_scale, d_gain)
        half_qkv, half_proj, small = reduce_all(d_wqkv, d_wproj, small)
        d_table, d_scale, d_gain = unpack_small(small, *d_table.shape, d_gain.shape[0])
    else:
        half_qkv, half_proj = (
            lax.psum_scatter(d_wqkv.astype(jnp.bfloat16), "ba", scatter_dimension=1, tiled=True).astype(
                jnp.float32
            ),
            lax.psum_scatter(
                d_wproj.astype(jnp.bfloat16), "ba", scatter_dimension=1, tiled=True
            ).astype(jnp.float32),
        )
        half_qkv, half_proj = lax.psum((half_qkv, half_proj), ("ha", "wa"))
        d_table, d_scale, d_gain = lax.psum((d_table, d_scale, d_gain), ("ha", "wa", "ba"))
    return (d_tokens, half_qkv, half_proj, d_table, d_scale, d_gain)


def solution(mesh):
    return jax.shard_map(
        shards,
        mesh=mesh,
        in_specs=(P("ba", "ha", "wa", None), P("ba", "ha", "wa", None), P(), P(), P(), P(), P()),
        out_specs=(P("ba", "ha", "wa", None), P(None, "ba"), P(None, "ba"), P(), P(), P()),
        check_vma=False,
    )
```

```python
import math

import functools

import jax
import jax.numpy as jnp
import numpy as np
from jax import lax
from jax.experimental import pallas as pl
from jax.experimental.pallas import tpu as pltpu
from jax.sharding import PartitionSpec as P

WIN = 8


EPS_NORM = 1e-05
MASK_FILL = -100.0
SCALE_CAP = math.log(100.0)
BIAS_RANGE = 16.0


def from_behind(block, axis, distance):
    devices = range(lax.axis_size(axis))
    route = [((i - distance) % len(devices), i) for i in devices]
    return lax.ppermute(block, axis, route)


def to_windows(block, window):
    images, height, width, depth = block.shape
    tiles = block.reshape(images, height // window, window, width // window, window, depth)
    tiles = tiles.transpose(0, 1, 3, 2, 4, 5)
    return tiles.reshape(images, height // window * (width // window), window * window, depth)


def from_windows(tiles, images, height, width, window):
    depth = tiles.shape[-1]
    grid = tiles.reshape(images, height // window, width // window, window, window, depth)
    return grid.transpose(0, 1, 3, 2, 4, 5).reshape(images, height, width, depth)


def region_of(coords, extent, window):
    return (coords >= extent - window).astype(jnp.int32) + (coords >= extent - window // 2).astype(
        jnp.int32
    )

GROUP = 4
FWD = 2
BWD = 4
LOG2E = math.log2(math.e)
VMEM_LIMIT = 40 * 2**20
FINISH_LIMIT = 4 * 2**20
MESH = pl.DeviceIdType.MESH
VMEM = pl.BlockSpec(memory_space=pltpu.VMEM)
NN = (((1,), (0,)), ((), ()))
NT = (((1,), (1,)), ((), ()))
TN = (((0,), (0,)), ((), ()))


def mxu(left, right, dims):
    return lax.dot_general(left, right, dims, preferred_element_type=jnp.float32)


def split(value):
    high = value.astype(jnp.bfloat16)
    return high, (value - high.astype(jnp.float32)).astype(jnp.bfloat16)


def mxu_fine(left, right, dims):
    high, low = split(left)
    return mxu(high, right, dims) + mxu(low, right, dims)


def same_block(rows, cols, row_size, col_size):
    row = lax.broadcasted_iota(jnp.int32, (rows, cols), 0) // row_size
    col = lax.broadcasted_iota(jnp.int32, (rows, cols), 1) // col_size
    return (row == col).astype(jnp.bfloat16)


def tile_heads(value, width):
    lane = lax.broadcasted_iota(jnp.int32, (1, value.shape[1]), 1) % (GROUP * width) // width
    rows = []
    for head in range(GROUP):
        rows.append(value * (lane == head).astype(jnp.bfloat16))
    return jnp.concatenate(rows, 0)


def gather_heads(value, width, length):
    lane = lax.broadcasted_iota(jnp.int32, (length, value.shape[1]), 1) // width
    total = value[:length]
    for head in range(1, GROUP):
        total = jnp.where(lane == head, value[head * length : (head + 1) * length], total)
    return total


def local_kernel(
    grid_cols, height, width, window,
    flat_ref, grad_ref, w_qkv_ref, w_proj_ref, bias_ref, scale_ref, gain_ref,
    d_flat_ref, d_wqkv_ref, d_wproj_ref, d_bias_ref, d_cos_ref, d_gain_ref,
    qkv_ref, att_ref, d_att_ref, d_qkv_ref, probs_ref, kinv_ref, qrow_ref, masked_ref, raw_q_ref, raw_k_ref,
    norm_ref,
):
    tokens, depth = flat_ref.shape
    f32, b16 = jnp.float32, jnp.bfloat16
    length = window * window
    count = tokens // length
    groups = bias_ref.shape[0]
    lanes = depth // groups
    heads = groups * GROUP
    head_dim = lanes // GROUP
    wide = GROUP * length
    row_base = lax.axis_index("ha") * (count // grid_cols * window)
    col_base = lax.axis_index("wa") * (grid_cols * window)

    qkv_ref[...] = mxu(flat_ref[...], w_qkv_ref[...], NN).astype(b16)
    lane_ones = same_block(lanes, wide, head_dim, length)
    lane_lane = same_block(lanes, lanes, head_dim, head_dim)

    head_rows = scale_ref.shape[0]
    pick = same_block(head_rows, depth, 1, head_dim)
    high, low = split(jnp.square(qkv_ref[:, :depth].astype(f32)))
    q_sums = mxu(pick, high, NT) + mxu(pick, low, NT)
    q_rows = lax.rsqrt(q_sums + 1.0) * scale_ref[:, :1]
    half = lax.broadcasted_iota(jnp.int32, (1, 2 * length), 1) < length
    for j in range(count // 2):
        base = q_rows[:, j * 2 * length : (j + 1) * 2 * length]
        turned = pltpu.roll(base, length, 1)
        for g in range(groups):
            for p in range(GROUP // 2):
                one, two = g * GROUP + 2 * p, g * GROUP + 2 * p + 1
                place = slice(p * 2 * length, (p + 1) * 2 * length)
                qrow_ref[2 * j, g, :, place] = jnp.where(half, base[one : one + 1], turned[two : two + 1])
                qrow_ref[2 * j + 1, g, :, place] = jnp.where(half, turned[one : one + 1], base[two : two + 1])
    for g in range(groups):
        query = qkv_ref[:, g * lanes : (g + 1) * lanes].astype(f32)
        key = qkv_ref[:, depth + g * lanes : depth + (g + 1) * lanes].astype(f32)
        high, low = split(jnp.square(key))
        kinv_ref[g] = lax.rsqrt(mxu(high, lane_ones, NN) + mxu(low, lane_ones, NN) + 1.0)
        norm_ref[1, g] = 1.0 / (mxu(high, lane_lane, NN) + mxu(low, lane_lane, NN) + 1.0)
        high, low = split(jnp.square(query))
        norm_ref[0, g] = 1.0 / (mxu(high, lane_lane, NN) + mxu(low, lane_lane, NN) + 1.0)

    mine = lax.broadcasted_iota(jnp.int32, (length, wide), 0)
    other = lax.broadcasted_iota(jnp.int32, (length, wide), 1) % length
    cut = window // 2
    row_off = (mine // window // cut) != (other // window // cut)
    col_off = (mine % window // cut) != (other % window // cut)
    for g in range(groups):
        bias = bias_ref[g] * LOG2E
        masked_ref[0, g] = bias
        masked_ref[1, g] = jnp.where(col_off, bias + MASK_FILL * LOG2E, bias)
        masked_ref[2, g] = jnp.where(row_off, bias + MASK_FILL * LOG2E, bias)
        masked_ref[3, g] = jnp.where(row_off | col_off, bias + MASK_FILL * LOG2E, bias)

    def load(ref, w, g, part):
        return ref[
            pl.ds(pl.multiple_of(w * length, length), length),
            part * depth + g * lanes : part * depth + (g + 1) * lanes,
        ]

    def forward(step, carry):
        units = [(step * FWD + k, g) for k in range(FWD) for g in range(groups)]
        scores = []
        for w, g in units:
            query, key = load(qkv_ref, w, g, 0), load(qkv_ref, w, g, 1)
            raw = mxu(key, tile_heads(query, head_dim), NT)
            last_row = (row_base + w // grid_cols * window) // (height - window)
            last_col = (col_base + w % grid_cols * window) // (width - window)
            kinv = kinv_ref[g, pl.ds(pl.multiple_of(w * length, length), length), :]
            scores.append(raw * kinv * (qrow_ref[w, g] * LOG2E) + masked_ref[last_row * 2 + last_col, g])
        for (w, g), score in zip(units, scores):
            expo = jnp.exp2(score - jnp.max(score, 0, keepdims=True))
            probs = expo * (1.0 / jnp.sum(expo, 0, keepdims=True))
            probs_ref[w, g] = probs
            att = gather_heads(mxu(probs.astype(b16), load(qkv_ref, w, g, 2), TN), head_dim, length)
            att_ref[
                pl.ds(pl.multiple_of(w * length, length), length), g * lanes : (g + 1) * lanes
            ] = att.astype(b16)
        return carry

    lax.fori_loop(0, count // FWD, forward, 0)

    proj = mxu(att_ref[...], w_proj_ref[...], NN)
    centre = proj - jnp.mean(proj, -1, keepdims=True)
    inv_std = lax.rsqrt(jnp.mean(centre * centre, -1, keepdims=True) + EPS_NORM)
    normed = centre * inv_std
    upstream = grad_ref[...].astype(f32)
    d_gain_ref[...] = jnp.sum(upstream * normed, 0, keepdims=True)
    scaled = upstream * gain_ref[...]
    d_proj = inv_std * (
        scaled
        - jnp.mean(scaled, -1, keepdims=True)
        - normed * jnp.mean(scaled * normed, -1, keepdims=True)
    )
    d_proj = d_proj.astype(b16)
    d_wproj_ref[...] = mxu(att_ref[...], d_proj, TN)
    d_att_ref[...] = mxu(d_proj, w_proj_ref[...], NT).astype(b16)
    d_bias_ref[...] = jnp.zeros_like(d_bias_ref)

    for g in range(groups):

        def backward(step, carry):
            units = [step * BWD + k for k in range(BWD)]
            grads = []
            for w in units:
                d_tall = tile_heads(load(d_att_ref, w, g, 0), head_dim)
                d_probs = mxu(load(qkv_ref, w, g, 2), d_tall, NT)
                d_value = mxu(probs_ref[w, g].astype(b16), d_tall, NN)
                d_qkv_ref[
                    pl.ds(pl.multiple_of(w * length, length), length),
                    2 * depth + g * lanes : 2 * depth + (g + 1) * lanes,
                ] = d_value.astype(b16)
                grads.append(d_probs)
            total = d_bias_ref[g]
            for w, d_probs in zip(units, grads):
                rows = pl.ds(pl.multiple_of(w * length, length), length)
                probs = probs_ref[w, g]
                d_scores = probs * (d_probs - jnp.sum(d_probs * probs, 0, keepdims=True))
                total = total + d_scores
                high, low = split(d_scores * kinv_ref[g, rows, :] * qrow_ref[w, g])
                both = jnp.concatenate([high, low], 0)
                query, key = load(qkv_ref, w, g, 0), load(qkv_ref, w, g, 1)
                pair = mxu(both, tile_heads(query, head_dim), NN)
                raw_k_ref[rows, :] = pair[:length] + pair[length:]
                tall = mxu(both, jnp.concatenate([key, key], 0), TN)
                raw_q_ref[rows, :] = gather_heads(tall, head_dim, length)
            d_bias_ref[g] = total
            return carry

        lax.fori_loop(0, count // BWD, backward, 0)
        for part, ref in enumerate((raw_q_ref, raw_k_ref)):
            place = slice(part * depth + g * lanes, part * depth + (g + 1) * lanes)
            value, grad = qkv_ref[:, place].astype(f32), ref[...]
            along = value * grad
            if part == 0:
                d_cos_ref[g] = jnp.sum(along, 0, keepdims=True)
            d_qkv_ref[:, place] = (
                grad - value * norm_ref[part, g] * mxu_fine(along, lane_lane, NN)
            ).astype(b16)
    d_wqkv_ref[...] = mxu(flat_ref[...], d_qkv_ref[...], TN)
    d_flat_ref[...] = mxu(d_qkv_ref[...], w_qkv_ref[...], NT).astype(b16)


def offset_onehot(window):
    places = np.arange(window * window)
    row_of, col_of = places // window, places % window
    offset = (row_of[:, None] - row_of[None, :] + window - 1) * (2 * window - 1) + (
        col_of[:, None] - col_of[None, :] + window - 1
    )
    return jnp.asarray(offset.reshape(-1), jnp.int32)


def three_parts(value):
    high = lax.reduce_precision(value, 8, 7)
    middle = lax.reduce_precision(value - high, 8, 7)
    return jnp.concatenate([high, middle, value - high - middle], 0).astype(jnp.bfloat16)


def local_grads(block, grad_block, row_base, col_base, height, width, window, params):
    w_qkv, w_proj, table_logits, logit_scale, gain = params
    images, rows, cols, depth = block.shape
    heads = logit_scale.shape[0]
    length = window * window
    groups = heads // GROUP
    wide = GROUP * length
    flat = to_windows(block, window).reshape(-1, depth)
    grad_flat = to_windows(grad_block, window).reshape(-1, depth)
    tokens = flat.shape[0]
    count = tokens // length
    scale = jnp.exp(jnp.minimum(logit_scale, SCALE_CAP))
    scale_rows = jnp.pad(scale, (0, -heads % 16)).reshape(-1, 1) * jnp.ones((1, 128), jnp.float32)
    sigma = jax.nn.sigmoid(table_logits)
    entries = table_logits.shape[1]
    hot = offset_onehot(window)[None, :] == jnp.arange(entries, dtype=jnp.int32)[:, None]
    hot = hot.astype(jnp.bfloat16)
    parts = jnp.dot(three_parts(sigma * BIAS_RANGE), hot, preferred_element_type=jnp.float32)
    rel_bias = jnp.sum(parts.reshape(3, heads, -1), 0).reshape(groups, GROUP, length, length)
    rel_bias = rel_bias.transpose(0, 3, 1, 2).reshape(groups, length, wide)
    f32, b16 = jnp.float32, jnp.bfloat16
    d_flat, d_wqkv, d_wproj, d_bias, d_cos, d_gain = pl.pallas_call(
        functools.partial(local_kernel, cols // window, height, width, window),
        out_shape=[
            jax.ShapeDtypeStruct((tokens, depth), b16),
            jax.ShapeDtypeStruct((depth, 3 * depth), f32),
            jax.ShapeDtypeStruct((depth, depth), f32),
            jax.ShapeDtypeStruct((groups, length, wide), f32),
            jax.ShapeDtypeStruct((groups, 1, depth // groups), f32),
            jax.ShapeDtypeStruct((1, depth), f32),
        ],
        in_specs=[VMEM] * 7,
        out_specs=[VMEM] * 6,
        scratch_shapes=[
            pltpu.VMEM((tokens, 3 * depth), b16),
            pltpu.VMEM((tokens, depth), b16),
            pltpu.VMEM((tokens, depth), b16),
            pltpu.VMEM((tokens, 3 * depth), b16),
            pltpu.VMEM((count, groups, length, wide), f32),
            pltpu.VMEM((groups, tokens, wide), f32),
            pltpu.VMEM((count, groups, 1, wide), f32),
            pltpu.VMEM((4, groups, length, wide), f32),
            pltpu.VMEM((tokens, depth // groups), f32),
            pltpu.VMEM((tokens, depth // groups), f32),
            pltpu.VMEM((2, groups, tokens, depth // groups), f32),
        ],
        compiler_params=pltpu.CompilerParams(vmem_limit_bytes=48 * 2**20),
        cost_estimate=pl.CostEstimate(
            flops=4_000_000_000, bytes_accessed=8_000_000, transcendentals=400_000
        ),
        name="local_grads",
    )(flat, grad_flat, w_qkv, w_proj, rel_bias, scale_rows, gain.reshape(1, depth))
    heads_bias = d_bias.reshape(groups, length, GROUP, length).transpose(0, 2, 3, 1)
    heads_bias = heads_bias.reshape(heads, length * length)
    sums = lax.dot_general(three_parts(heads_bias), hot, NT, preferred_element_type=jnp.float32)
    d_table = jnp.sum(sums.reshape(3, heads, entries), 0) * (BIAS_RANGE * sigma * (1.0 - sigma))
    live = (logit_scale < SCALE_CAP).astype(jnp.float32)
    d_scale = jnp.sum(d_cos.reshape(heads, depth // heads), 1) * live
    d_block = from_windows(d_flat.reshape(images, count, length, depth), images, rows, cols, window)
    return (d_block, (d_wqkv, d_wproj, d_table, d_scale, d_gain.reshape(depth)))


def half_turn(value, axis):
    return pltpu.roll(value, value.shape[axis] // 2, axis)


def exp_fine(value):
    whole = jnp.floor(value * LOG2E + 0.5)
    rest = value - whole * 0.693359375 + whole * 2.12194440e-4
    total = jnp.ones_like(rest)
    for k in range(8, 0, -1):
        total = 1.0 + total * rest * (1.0 / k)
    return total * jnp.exp2(whole)


def inverse(value):
    guess = 1.0 / value
    return guess * (2.0 - value * guess)


def place_of(index, window):
    return index // window * (2 * window - 1) + index % window


def expand_bias(table, length, window, groups, out_ref):
    span = table.shape[1]
    f32, b16 = jnp.float32, jnp.bfloat16
    heads = groups * GROUP
    base = jnp.concatenate([jnp.broadcast_to(table[h : h + 1], (window, span)) for h in range(heads)], 0)
    sub = lax.broadcasted_iota(jnp.int32, base.shape, 0) % window
    bit = 1
    while bit < window:
        base = jnp.where(sub // bit % 2 == 1, pltpu.roll(base, bit, 1), base)
        bit *= 2
    top = place_of(length - 1, window)
    turned = [
        pltpu.roll(base, (span - top + (2 * window - 1) * r) % span, 1)[:, : span // 2] for r in range(window)
    ]
    wide = GROUP * length
    row = lax.broadcasted_iota(jnp.int32, (span, wide), 0) % (span // 2)
    col = lax.broadcasted_iota(jnp.int32, (span, wide), 1)
    hit = row == place_of(col % length, window)
    for g in range(groups):
        total = jnp.zeros((length, wide), f32)
        for k in range(GROUP):
            h = g * GROUP + k
            block = jnp.concatenate([t[h * window : (h + 1) * window] for t in turned], 0)
            pair = jnp.concatenate(split(block), 1)
            total = total + mxu(pair, (hit & (col // length == k)).astype(b16), NN)
        out_ref[0, g] = total


def fold_bias(grads, length, window, span):
    f32, b16 = jnp.float32, jnp.bfloat16
    wide = GROUP * length
    row = lax.broadcasted_iota(jnp.int32, (wide, span // 2), 0)
    col = lax.broadcasted_iota(jnp.int32, (wide, span // 2), 1)
    hit = col == place_of(row % length, window)
    both = jnp.concatenate([half for grad in grads for half in split(grad)], 0)
    by_head = [None] * (len(grads) * GROUP)
    for k in range(GROUP):
        pairs = mxu(both, (hit & (row // length == k)).astype(b16), NN)
        for g in range(len(grads)):
            pair = pairs[2 * g * length : (2 * g + 2) * length]
            block = pair[:length] + pair[length:]
            by_head[g * GROUP + k] = jnp.concatenate([block, jnp.zeros_like(block)], 1)
    parts = [
        jnp.concatenate([block[r * window : (r + 1) * window] for block in by_head], 0) for r in range(window)
    ]
    step = 2 * window - 1
    while len(parts) > 1:
        parts = [pltpu.roll(parts[i], step, 1) + parts[i + 1] for i in range(0, len(parts), 2)]
        step *= 2
    total = parts[0]
    sub = window - 1 - lax.broadcasted_iota(jnp.int32, total.shape, 0) % window
    bit = 1
    while bit < window:
        total = jnp.where(sub // bit % 2 == 1, pltpu.roll(total, bit, 1), total)
        bit *= 2
    return [jnp.sum(total[k * window : (k + 1) * window], 0, keepdims=True) for k in range(len(by_head))]


def whole_kernel(
    shape, height, width, window,
    tokens_ref, cot_ref, w_qkv_hbm, w_proj_hbm, table_hbm, gain_hbm, scale_ref,
    d_tok_ref, wq_out, wp_out, table_out, scale_out, gain_out,
    tok, cot, w_qkv_ref, w_proj_ref, table_in, gain_ref, table_ref, local_sems,
    col_send, row_get, col_get, diag_get, halo_sems,
    flat_ref, grad_ref, d_flat_ref,
    qkv_ref, att_ref, d_att_ref, d_qkv_ref, probs_ref, kinv_ref, qrow_ref, masked_ref, raw_q_ref, raw_k_ref,
    norm_ref, d_bias_ref, p_mid, product_ref,
    row_back, col_back, row_back_get, col_back_get, diag_back_get, back_sems,
    small, small_core, small_a, small_image, small_b, small_near, tiny_sems,
    *chunk_refs,
):
    size_h, size_w = shape
    chips = size_h // 2
    peers = chips * size_w
    ha, wa, ba = lax.axis_index("ha"), lax.axis_index("wa"), lax.axis_index("ba")
    core = ha % 2
    me = wa * chips + ha // 2
    partner = (ha + 1 - 2 * core, wa, ba)
    image, side, corner = (ha, wa, 1 - ba), (ha, 1 - wa, ba), (ha, 1 - wa, 1 - ba)
    above, below = lax.rem(ha + size_h - 1, size_h), lax.rem(ha + 1, size_h)
    left, right = lax.rem(wa + size_w - 1, size_w), lax.rem(wa + 1, size_w)
    f32, b16 = jnp.float32, jnp.bfloat16

    def peer(step):
        other = lax.rem(me + step, peers)
        return other, (other % chips * 2 + core, other // chips, ba)

    loads = []
    for k, (src, dst) in enumerate(
        (
            (tokens_ref.at[0], tok), (cot_ref.at[0], cot), (w_qkv_hbm, w_qkv_ref), (w_proj_hbm, w_proj_ref),
            (table_hbm, table_in), (gain_hbm, gain_ref),
        )
    ):
        copy = pltpu.make_async_copy(src, dst, local_sems.at[k])
        copy.start()
        loads.append(copy)
    targets = [
        (above, wa, ba), (below, wa, ba), (ha, left, ba), (ha, right, ba), (above, left, ba), (below, right, ba),
        partner, image, corner,
    ] + [peer(step)[1] for step in range(1, peers)]
    barrier = pltpu.get_barrier_semaphore()
    for device in targets:
        pl.semaphore_signal(barrier, inc=1, device_id=device, device_id_type=MESH)

    def start(src, dst, sems, device):
        copy = pltpu.make_async_remote_copy(
            src_ref=src, dst_ref=dst, send_sem=sems.at[0], recv_sem=sems.at[1],
            device_id=device, device_id_type=MESH,
        )
        copy.start()
        return copy

    rows, cols, depth = tok.shape
    cut = window // 2
    length = window * window
    across = cols // window
    count = rows // window * across
    tokens = count * length
    groups = qrow_ref.shape[1]
    lanes = depth // groups
    head_dim = lanes // GROUP
    wide = GROUP * length
    low_sub = lax.broadcasted_iota(jnp.int32, (window, depth), 0) < cut

    for a, ref in enumerate((tok, cot)):
        loads[a].wait()
        for j in range(rows // 2):
            first = ref[2 * j, :window, :].astype(f32)
            second = ref[2 * j + 1, :window, :].astype(f32)
            col_send[a, j] = jnp.where(low_sub, first, half_turn(second, 0)).astype(b16)
    pl.semaphore_wait(barrier, len(targets))
    halos = []
    for a, ref in enumerate((tok, cot)):
        halos.append(start(ref.at[pl.ds(0, cut)], row_get.at[a], halo_sems.at[a, 0], (above, wa, ba)))
        halos.append(start(col_send.at[a], col_get.at[a], halo_sems.at[a, 1], (ha, left, ba)))
        halos.append(
            start(col_send.at[a, pl.ds(0, cut // 2)], diag_get.at[a], halo_sems.at[a, 2], (above, left, ba))
        )

    loads[4].wait()
    loads[5].wait()
    heads = groups * GROUP
    entries = table_in.shape[1]
    table_ref[...] = jnp.zeros_like(table_ref)
    table_ref[:heads, :entries] = table_in[...]
    sigma = inverse(1.0 + exp_fine(-table_ref[...]))
    head_rows, span = table_ref.shape
    spot = lax.broadcasted_iota(jnp.int32, (head_rows, 128), 0)
    logits = jnp.zeros((head_rows, 128), f32)
    for h in range(heads):
        logits = jnp.where(spot == h, scale_ref[h], logits)
    scale = exp_fine(jnp.minimum(logits, SCALE_CAP))
    expand_bias(sigma * (BIAS_RANGE * LOG2E), length, window, groups, masked_ref)
    mine = lax.broadcasted_iota(jnp.int32, (length, wide), 0)
    other = lax.broadcasted_iota(jnp.int32, (length, wide), 1) % length
    row_off = (mine // window // cut) != (other // window // cut)
    col_off = (mine % window // cut) != (other % window // cut)
    for g in range(groups):
        bias = masked_ref[0, g]
        masked_ref[1, g] = jnp.where(col_off, bias + MASK_FILL * LOG2E, bias)
        masked_ref[2, g] = jnp.where(row_off, bias + MASK_FILL * LOG2E, bias)
        masked_ref[3, g] = jnp.where(row_off | col_off, bias + MASK_FILL * LOG2E, bias)
    small[...] = jnp.zeros_like(small)

    def gather_rows(a, ref, out_ref):
        def shifted(i):
            if i + cut < rows:
                row, edge = ref[i + cut], col_get[a, (i + cut) // 2]
            else:
                row, edge = row_get[a, i + cut - rows], diag_get[a, (i + cut - rows) // 2]
            row, edge = row.astype(f32), edge.astype(f32)
            turned = [half_turn(row[k * window : (k + 1) * window], 0) for k in range(across)]
            turned.append(half_turn(edge, 0) if i % 2 == 0 else edge)
            return [jnp.where(low_sub, turned[k], turned[k + 1]) for k in range(across)]

        for i in range(0, rows, 2):
            one, two = shifted(i), shifted(i + 1)
            for k in range(across):
                begin = (i // window * across + k) * length + i % window * window
                out_ref[begin : begin + 2 * window] = jnp.concatenate([one[k], two[k]], 0).astype(b16)

    def settle(a, ref, out_ref):
        for copy in halos[3 * a : 3 * a + 3]:
            copy.wait()
        gather_rows(a, ref, out_ref)

    settle(0, tok, flat_ref)
    loads[2].wait()
    loads[3].wait()

    row_base, col_base = ha * rows, wa * cols
    qkv_ref[...] = mxu(flat_ref[...], w_qkv_ref[...], NN).astype(b16)
    lane_ones = same_block(lanes, wide, head_dim, length)
    lane_lane = same_block(lanes, lanes, head_dim, head_dim)
    pick = same_block(head_rows, depth, 1, head_dim)
    high, low = split(jnp.square(qkv_ref[:, :depth].astype(f32)))
    q_sums = mxu(pick, high, NT) + mxu(pick, low, NT)
    q_rows = lax.rsqrt(q_sums + 1.0) * scale[:, :1]
    half = lax.broadcasted_iota(jnp.int32, (1, 2 * length), 1) < length
    for j in range(count // 2):
        base = q_rows[:, j * 2 * length : (j + 1) * 2 * length]
        turned = half_turn(base, 1)
        for g in range(groups):
            for p in range(GROUP // 2):
                one, two = g * GROUP + 2 * p, g * GROUP + 2 * p + 1
                place = slice(p * 2 * length, (p + 1) * 2 * length)
                qrow_ref[2 * j, g, :, place] = jnp.where(half, base[one : one + 1], turned[two : two + 1])
                qrow_ref[2 * j + 1, g, :, place] = jnp.where(half, turned[one : one + 1], base[two : two + 1])
    for g in range(groups):
        query = qkv_ref[:, g * lanes : (g + 1) * lanes].astype(f32)
        key = qkv_ref[:, depth + g * lanes : depth + (g + 1) * lanes].astype(f32)
        high, low = split(jnp.square(key))
        kinv_ref[g] = lax.rsqrt(mxu(high, lane_ones, NN) + mxu(low, lane_ones, NN) + 1.0)
        norm_ref[1, g] = 1.0 / (mxu(high, lane_lane, NN) + mxu(low, lane_lane, NN) + 1.0)
        high, low = split(jnp.square(query))
        norm_ref[0, g] = 1.0 / (mxu(high, lane_lane, NN) + mxu(low, lane_lane, NN) + 1.0)

    def load(ref, w, g, part):
        return ref[
            pl.ds(pl.multiple_of(w * length, length), length),
            part * depth + g * lanes : part * depth + (g + 1) * lanes,
        ]

    def forward(step, carry):
        units = [(step * FWD + k, g) for k in range(FWD) for g in range(groups)]
        scores = []
        for w, g in units:
            query, key = load(qkv_ref, w, g, 0), load(qkv_ref, w, g, 1)
            raw = mxu(key, tile_heads(query, head_dim), NT)
            last_row = (row_base + w // across * window) // (height - window)
            last_col = (col_base + w % across * window) // (width - window)
            kinv = kinv_ref[g, pl.ds(pl.multiple_of(w * length, length), length), :]
            scores.append(raw * kinv * (qrow_ref[w, g] * LOG2E) + masked_ref[last_row * 2 + last_col, g])
        for (w, g), score in zip(units, scores):
            expo = jnp.exp2(score - jnp.max(score, 0, keepdims=True))
            probs = expo * (1.0 / jnp.sum(expo, 0, keepdims=True))
            probs_ref[w, g] = probs
            att = gather_heads(mxu(probs.astype(b16), load(qkv_ref, w, g, 2), TN), head_dim, length)
            att_ref[
                pl.ds(pl.multiple_of(w * length, length), length), g * lanes : (g + 1) * lanes
            ] = att.astype(b16)
        return carry

    lax.fori_loop(0, count // FWD, forward, 0)

    settle(1, cot, grad_ref)
    proj = mxu(att_ref[...], w_proj_ref[...], NN)
    centre = proj - jnp.mean(proj, -1, keepdims=True)
    inv_std = lax.rsqrt(jnp.mean(centre * centre, -1, keepdims=True) + EPS_NORM)
    normed = centre * inv_std
    upstream = grad_ref[...].astype(f32)
    d_gain = jnp.sum(upstream * normed, 0, keepdims=True)
    scaled = upstream * gain_ref[...].reshape(1, depth)
    d_proj = inv_std * (
        scaled
        - jnp.mean(scaled, -1, keepdims=True)
        - normed * jnp.mean(scaled * normed, -1, keepdims=True)
    )
    d_proj = d_proj.astype(b16)
    small[heads : heads + 1, :] = d_gain[:, :span]
    small[heads + 1 : heads + 2, : depth - span] = d_gain[:, span:]
    per = len(chunk_refs) // 4
    chunks = [chunk_refs[c * per : (c + 1) * per] for c in range(4)]
    flying = {}

    def begin(c):
        core_send, core_mine, core_get = chunks[c][:3]
        w = core_send.shape[0] // 2
        for side_of in range(2):
            here = slice(side_of * w, (side_of + 1) * w)
            base = 2 * side_of * w
            theirs = pl.ds(pl.multiple_of(base + (1 - core) * w, 32), w)
            core_send[here] = product_ref[theirs, :].astype(b16)
        flying[c] = start(core_send, core_get, chunks[c][9], partner)
        for side_of in range(2):
            here = slice(side_of * w, (side_of + 1) * w)
            core_mine[here] = product_ref[pl.ds(pl.multiple_of(2 * side_of * w + core * w, 32), w), :]

    def cross(c):
        core_send, core_mine, core_get, plane_send, plane_get = chunks[c][:5]
        flying[c].wait()
        core_mine[...] = core_mine[...] + core_get[...].astype(f32)
        w = plane_send.shape[1]
        flying[c] = []
        for k, (b, y, device) in enumerate(((1 - ba, wa, image), (ba, 1 - wa, side), (1 - ba, 1 - wa, corner))):
            place = pl.ds(pl.multiple_of((2 * b + y) * w, 32), w)
            plane_send[k] = core_mine[place, :].astype(b16)
            flying[c].append(start(plane_send.at[k], plane_get.at[k], chunks[c][10].at[k], device))

    def scatter(c):
        core_mine, plane_get, near_send, near_get = chunks[c][1], chunks[c][4], chunks[c][5], chunks[c][6]
        for copy in flying[c]:
            copy.wait()
        w = plane_get.shape[1]
        total = core_mine[pl.ds(pl.multiple_of((2 * ba + wa) * w, 32), w), :]
        for k in range(3):
            total = total + plane_get[k].astype(f32)
        r = near_send.shape[1]
        for j in range(chips):
            near_send[j] = total[j * r : (j + 1) * r].astype(b16)
        flying[c] = []
        for step in range(1, chips):
            far_chip = lax.rem(ha // 2 + step, chips)
            flying[c].append(
                start(
                    near_send.at[far_chip], near_get.at[step - 1], chunks[c][11].at[step - 1],
                    (2 * far_chip + core, wa, ba),
                )
            )

    def gather(c):
        near_send, near_get, whole = chunks[c][5:8]
        for copy in flying[c]:
            copy.wait()
        total = near_send[ha // 2].astype(f32)
        for step in range(1, chips):
            total = total + near_get[step - 1].astype(f32)
        whole[me] = total.astype(b16)
        flying[c] = []
        for step in range(1, peers):
            flying[c].append(start(whole.at[me], whole.at[me], chunks[c][12].at[step - 1], peer(step)[1]))

    def mirror(c):
        whole, core_all = chunks[c][7:9]
        for copy in flying[c]:
            copy.wait()
        flying[c] = start(whole, core_all, chunks[c][13], partner)
        put(c, whole, core)

    def finish(c):
        flying[c].wait()
        put(c, chunks[c][8], 1 - core)

    def put(c, source, which):
        r = source.shape[1]
        w = peers * r
        begin_rows = half_starts[c]
        step_rows = lanes // 2
        for first in range(0, 2 * w, step_rows):
            near, away = begin_rows[first // step_rows]
            for j in range(first % w // r, min(peers, (first % w + step_rows) // r)):
                inside = j * r - first % w

                def one(is_wq, near_row, away_row, out):
                    row = jnp.where(ba == 0, near_row, away_row) + inside
                    out[pl.ds(pl.multiple_of(row, 8), r), :] = source[j].astype(f32)

                @pl.when(which == first // w)
                def _():
                    one(near[0], near[1], away[1], near[0])

    unit = lanes // 2
    half_starts = [
        [((wp_out, k * unit), (wp_out, (1 + k) * unit)) for k in range(2)],
        [((wq_out, k * unit), (wq_out, (3 + k) * unit)) for k in range(2)],
        [((wq_out, (4 + k) * unit), (wq_out, (1 + k if k < 2 else 5 + k) * unit)) for k in range(4)],
        [
            ((wq_out, 2 * unit), (wq_out, 5 * unit)), ((wq_out, 3 * unit), (wq_out, 6 * unit)),
            ((wq_out, 8 * unit), (wq_out, 0)), ((wp_out, 2 * unit), (wp_out, 0)),
        ],
    ]

    product = mxu(d_proj, att_ref[...], TN)
    product_ref[:lanes] = product[:lanes]
    p_mid[...] = product[lanes : 2 * lanes]
    product_ref[lanes : 2 * lanes] = product[2 * lanes :]
    begin(0)
    d_att_ref[...] = mxu(d_proj, w_proj_ref[...], NT).astype(b16)

    def backward_group(g):
        def backward(step, total):
            units = [step * BWD + k for k in range(BWD)]
            grads = []
            for w in units:
                d_tall = tile_heads(load(d_att_ref, w, g, 0), head_dim)
                d_probs = mxu(load(qkv_ref, w, g, 2), d_tall, NT)
                d_value = mxu(probs_ref[w, g].astype(b16), d_tall, NN)
                d_qkv_ref[
                    pl.ds(pl.multiple_of(w * length, length), length),
                    2 * depth + g * lanes : 2 * depth + (g + 1) * lanes,
                ] = d_value.astype(b16)
                grads.append(d_probs)
            summed = d_bias_ref[g]
            for w, d_probs in zip(units, grads):
                place = pl.ds(pl.multiple_of(w * length, length), length)
                probs = probs_ref[w, g]
                d_scores = probs * (d_probs - jnp.sum(d_probs * probs, 0, keepdims=True))
                summed = summed + d_scores
                high, low = split(d_scores * kinv_ref[g, place, :] * qrow_ref[w, g])
                both = jnp.concatenate([high, low], 0)
                query, key = load(qkv_ref, w, g, 0), load(qkv_ref, w, g, 1)
                pair = mxu(both, tile_heads(query, head_dim), NN)
                raw_k_ref[place, :] = pair[:length] + pair[length:]
                tall = mxu(both, jnp.concatenate([key, key], 0), TN)
                raw_q_ref[place, :] = gather_heads(tall, head_dim, length)
            d_bias_ref[g] = summed
            return total

        d_bias_ref[g] = jnp.zeros((length, wide), f32)
        lax.fori_loop(0, count // BWD, backward, 0)
        for part, ref in enumerate((raw_q_ref, raw_k_ref)):
            place = slice(part * depth + g * lanes, part * depth + (g + 1) * lanes)
            value, grad = qkv_ref[:, place].astype(f32), ref[...]
            along = value * grad
            if part == 0:
                spot = depth - span + g * lanes
                small[
                    heads + 1 + spot // span : heads + 2 + spot // span, spot % span : spot % span + lanes
                ] = jnp.sum(along, 0, keepdims=True)
            d_qkv_ref[:, place] = (
                grad - value * norm_ref[part, g] * mxu_fine(along, lane_lane, NN)
            ).astype(b16)

    def dense_column(row, part, g, rows_from=0, rows_to=None):
        place = slice(part * depth + g * lanes, part * depth + (g + 1) * lanes)
        product_ref[row : row + lanes] = mxu(d_qkv_ref[:, place], flat_ref[...], TN)

    backward_group(0)
    dense_column(0, 0, 0)
    dense_column(lanes, 2, 0)
    begin(1)
    cross(0)
    backward_group(2)
    dense_column(0, 0, 2)
    dense_column(lanes, 1, 0)
    dense_column(2 * lanes, 1, 2)
    dense_column(3 * lanes, 2, 2)
    begin(2)
    cross(1)
    backward_group(1)
    dense_column(0, 0, 1)
    dense_column(2 * lanes, 2, 1)
    key = mxu(d_qkv_ref[:, depth + lanes : depth + 2 * lanes], flat_ref[...], TN)
    product_ref[lanes : lanes + unit] = key[:unit]
    product_ref[lanes + unit : 2 * lanes] = p_mid[:unit]
    product_ref[3 * lanes : 3 * lanes + unit] = key[unit:]
    product_ref[3 * lanes + unit : 4 * lanes] = p_mid[unit:]
    begin(3)
    scatter(0)
    cross(2)
    d_flat_ref[...] = mxu(d_qkv_ref[...], w_qkv_ref[...], NT).astype(b16)

    def back_tiles(i):
        begin_row = i // window * across * length + i % window * window
        return [
            half_turn(d_flat_ref[begin_row + k * length : begin_row + k * length + window].astype(f32), 0)
            for k in range(across)
        ]

    for i in range(0, rows, 2):
        one, two = back_tiles(i), back_tiles(i + 1)
        col_back[i // 2] = jnp.where(low_sub, one[-1], half_turn(two[-1], 0)).astype(b16)
        if i >= rows - cut:
            row_back[i - (rows - cut)] = jnp.concatenate(one, 0).astype(b16)
            row_back[i + 1 - (rows - cut)] = jnp.concatenate(two, 0).astype(b16)
    far = (rows - cut) // 2
    back = [
        start(row_back, row_back_get, back_sems.at[0], (below, wa, ba)),
        start(col_back.at[pl.ds(0, far)], col_back_get, back_sems.at[1], (ha, right, ba)),
        start(col_back.at[pl.ds(far, cut // 2)], diag_back_get, back_sems.at[2], (below, right, ba)),
    ]
    cross(3)
    for k, row in enumerate(fold_bias([d_bias_ref[g] for g in range(groups)], length, window, span)):
        small[k : k + 1, :] = row
    tiny = start(small, small_core, tiny_sems.at[0], partner)
    scatter(1)
    gather(0)
    tiny.wait()
    small_a[...] = small[...] + small_core[...]
    tiny = start(small_a, small_image, tiny_sems.at[1], image)
    scatter(2)
    tiny.wait()
    small_b[...] = small_a[...] + small_image[...]
    tinies = []
    for step in range(1, peers):
        tinies.append(start(small_b, small_near.at[step - 1], tiny_sems.at[step + 1], peer(step)[1]))

    def put_row(i, turned, edge, odd):
        ahead = [half_turn(edge, 0) if odd else edge] + turned
        out = [jnp.where(low_sub, ahead[k], ahead[k + 1]) for k in range(across)]
        d_tok_ref[i] = (jnp.concatenate(out, 0) + cot[i].astype(f32)).astype(b16)

    back[1].wait()
    for i in range(rows - cut):
        put_row(i + cut, back_tiles(i), col_back_get[i // 2].astype(f32), i % 2 == 1)
    gather(1)
    scatter(3)
    back[0].wait()
    back[2].wait()
    for i in range(cut):
        whole_row = row_back_get[i].astype(f32)
        turned = [whole_row[k * window : (k + 1) * window] for k in range(across)]
        put_row(i, turned, diag_back_get[i // 2].astype(f32), i % 2 == 1)
    gather(2)
    mirror(0)
    mirror(1)
    gather(3)
    for copy in tinies:
        copy.wait()
    total = small_b[...]
    for step in range(1, peers):
        total = total + small_near[step - 1]
    table_out[...] = (total[: head_rows] * (BIAS_RANGE * sigma * (1.0 - sigma)))[:heads, :entries]
    gain_row = jnp.concatenate([total[heads : heads + 1, :], total[heads + 1 : heads + 2, : depth - span]], 1)
    gain_out[...] = gain_row.reshape(depth)
    sums = jnp.concatenate([total[heads + 1 : heads + 2, depth - span :], total[heads + 2 : heads + 3, :]], 1)
    sums = mxu_fine(jnp.broadcast_to(sums, (8, depth)), same_block(depth, 128, head_dim, 1), NN)[:1]
    at = lax.broadcasted_iota(jnp.int32, (1, 128), 1)
    logits = jnp.zeros((1, 128), f32)
    for h in range(heads):
        logits = jnp.where(at == h, scale_ref[h], logits)
    scale_out[...] = jnp.where(logits < SCALE_CAP, sums, 0.0).reshape(128)[:heads]
    finish(0)
    finish(1)
    mirror(2)
    finish(2)
    mirror(3)
    finish(3)


def finish_kernel(*refs):
    count = len(refs) // 2
    sems = refs[-1]
    copies = [pltpu.make_async_copy(refs[k], refs[count + k], sems.at[k]) for k in range(count)]
    for copy in copies:
        copy.start()
    for copy in copies:
        copy.wait()


def whole_grads(tokens, cotangent, w_qkv, w_proj, table_logits, logit_scale, gain, height, width, window):
    size_h, size_w = lax.axis_size("ha"), lax.axis_size("wa")
    peers = size_h // 2 * size_w
    f32, b16 = jnp.float32, jnp.bfloat16
    images, rows, cols, depth = tokens.shape
    heads = logit_scale.shape[0]
    entries = table_logits.shape[1]
    groups = heads // GROUP
    lanes = depth // groups
    length = window * window
    wide = GROUP * length
    total = rows * cols
    count = total // length
    cut = window // 2
    span = 256
    head_rows = -(-heads // 16) * 16
    half = depth // 2
    chips = size_h // 2
    dma, vmem = pltpu.SemaphoreType.DMA, pltpu.VMEM
    chunk_scratch = []
    for w in (lanes // 2, lanes // 2, lanes, lanes):
        r = w // peers
        chunk_scratch += [
            vmem((2 * w, depth), b16), vmem((2 * w, depth), f32), vmem((2 * w, depth), b16),
            vmem((3, w // 2, depth), b16), vmem((3, w // 2, depth), b16),
            vmem((chips, r, depth), b16), vmem((chips - 1, r, depth), b16),
            vmem((peers, r, depth), b16), vmem((peers, r, depth), b16),
            dma((2,)), dma((3, 2)), dma((chips - 1, 2)), dma((peers - 1, 2)), dma((2,)),
        ]
    small = (16, span)
    anywhere = pl.BlockSpec(memory_space=pltpu.HBM)
    pinned = [
        pltpu.with_memory_space_constraint(x, pltpu.HBM)
        for x in (tokens, cotangent, w_qkv, w_proj, table_logits, gain)
    ]
    outs = pl.pallas_call(
        functools.partial(whole_kernel, (size_h, size_w), height, width, window),
        out_shape=[
            jax.ShapeDtypeStruct((rows, cols, depth), b16),
            jax.ShapeDtypeStruct((3 * depth // 2, depth), f32),
            jax.ShapeDtypeStruct((depth // 2, depth), f32),
            jax.ShapeDtypeStruct((heads, entries), f32),
            jax.ShapeDtypeStruct((heads,), f32),
            jax.ShapeDtypeStruct((depth,), f32),
        ],
        in_specs=[anywhere] * 6 + [pl.BlockSpec(memory_space=pltpu.SMEM)],
        out_specs=[VMEM] * 6,
        scratch_shapes=[
            vmem((rows, cols, depth), b16), vmem((rows, cols, depth), b16),
            vmem((depth, 3 * depth), b16), vmem((depth, depth), b16),
            vmem((heads, entries), f32), vmem((depth,), f32), vmem((head_rows, span), f32), dma((6,)),
            vmem((2, rows // 2, window, depth), b16), vmem((2, cut, cols, depth), b16),
            vmem((2, rows // 2, window, depth), b16), vmem((2, cut // 2, window, depth), b16), dma((2, 3, 2)),
            vmem((total, depth), b16), vmem((total, depth), b16), vmem((total, depth), b16),
            vmem((total, 3 * depth), b16), vmem((total, depth), b16), vmem((total, depth), b16),
            vmem((total, 3 * depth), b16), vmem((count, groups, length, wide), f32), vmem((groups, total, wide), f32),
            vmem((count, groups, 1, wide), f32), vmem((4, groups, length, wide), f32),
            vmem((total, lanes), f32), vmem((total, lanes), f32), vmem((2, groups, total, lanes), f32),
            vmem((groups, length, wide), f32), vmem((lanes, depth), f32), vmem((4 * lanes, depth), f32),
            vmem((cut, cols, depth), b16), vmem((rows // 2, window, depth), b16), vmem((cut, cols, depth), b16),
            vmem(((rows - cut) // 2, window, depth), b16), vmem((cut // 2, window, depth), b16), dma((3, 2)),
            vmem(small, f32), vmem(small, f32), vmem(small, f32), vmem(small, f32), vmem(small, f32),
            vmem((peers - 1, *small), f32), dma((peers + 1, 2)),
            *chunk_scratch,
        ],
        compiler_params=pltpu.CompilerParams(
            collective_id=0, has_side_effects=True, vmem_limit_bytes=VMEM_LIMIT
        ),
        name="whole_grads",
    )(*pinned, logit_scale)
    d_tok, half_qkv, half_proj, d_table, d_scale, d_gain = pl.pallas_call(
        finish_kernel,
        out_shape=[jax.ShapeDtypeStruct(x.shape, x.dtype) for x in outs],
        in_specs=[VMEM] * 6,
        out_specs=[anywhere] * 6,
        scratch_shapes=[dma((6,))],
        compiler_params=pltpu.CompilerParams(vmem_limit_bytes=FINISH_LIMIT),
        name="finish",
    )(*outs)
    return d_tok[None], half_qkv.T, half_proj.T, d_table, d_scale, d_gain


def can_join(tokens, logit_scale):
    size_h, size_w, size_b = (lax.axis_size(name) for name in ("ha", "wa", "ba"))
    images, rows, cols, depth = tokens.shape
    peers = size_h // 2 * size_w
    return (
        images == 1 and size_b == 2 and size_w == 2 and size_h % 2 == 0 and size_h > 2
        and logit_scale.shape[0] == 3 * GROUP and depth == 3 * 128 and WIN == 8
        and rows % WIN == 0 and cols % (2 * WIN) == 0 and rows * cols // 64 % BWD == 0
        and 64 % peers == 0 and 64 // peers % 8 == 0
    )


def shift_in(tokens, cotangent, shift):
    stacked = jnp.stack([tokens, cotangent])
    below = from_behind(stacked[:, :, :shift], "ha", -1)
    tall = jnp.concatenate([stacked[:, :, shift:], below], 2)
    beside = from_behind(tall[:, :, :, :shift], "wa", -1)
    moved = jnp.concatenate([tall[:, :, :, shift:], beside], 3)
    return (moved[0], moved[1])


def shift_out(grads, shift):
    rows = grads.shape[1]
    cols = grads.shape[2]
    right = from_behind(grads[:, :, cols - shift :], "wa", 1)
    wide = jnp.concatenate([right, grads[:, :, : cols - shift]], 2)
    lower = from_behind(wide[:, rows - shift :], "ha", 1)
    return jnp.concatenate([lower, wide[:, : rows - shift]], 1)


def shards(tokens, cotangent, w_qkv, w_proj, table_logits, logit_scale, gain):
    rows = tokens.shape[1]
    cols = tokens.shape[2]
    shift = WIN // 2
    height = rows * lax.axis_size("ha")
    width = cols * lax.axis_size("wa")
    row_base = lax.axis_index("ha") * rows
    col_base = lax.axis_index("wa") * cols
    if can_join(tokens, logit_scale):
        return whole_grads(
            tokens, cotangent, w_qkv, w_proj, table_logits, logit_scale, gain, height, width, WIN
        )
    params = (w_qkv, w_proj, table_logits, logit_scale, gain)
    moved, moved_grad = shift_in(tokens, cotangent, shift)
    d_moved, parts = local_grads(moved, moved_grad, row_base, col_base, height, width, WIN, params)
    back = shift_out(d_moved, shift)
    d_tokens = (cotangent.astype(jnp.float32) + back.astype(jnp.float32)).astype(jnp.bfloat16)
    d_wqkv, d_wproj, d_table, d_scale, d_gain = parts
    half_qkv, half_proj = (
        lax.psum_scatter(d_wqkv.astype(jnp.bfloat16), "ba", scatter_dimension=1, tiled=True).astype(jnp.float32),
        lax.psum_scatter(d_wproj.astype(jnp.bfloat16), "ba", scatter_dimension=1, tiled=True).astype(jnp.float32),
    )
    half_qkv, half_proj = lax.psum((half_qkv, half_proj), ("ha", "wa"))
    d_table, d_scale, d_gain = lax.psum((d_table, d_scale, d_gain), ("ha", "wa", "ba"))
    return (d_tokens, half_qkv, half_proj, d_table, d_scale, d_gain)


def solution(mesh):
    return jax.shard_map(
        shards,
        mesh=mesh,
        in_specs=(P("ba", "ha", "wa", None), P("ba", "ha", "wa", None), P(), P(), P(), P(), P()),
        out_specs=(P("ba", "ha", "wa", None), P(None, "ba"), P(None, "ba"), P(), P(), P()),
        check_vma=False,
    )
```

```python
import math

import functools

import jax
import jax.numpy as jnp
import numpy as np
from jax import lax
from jax.experimental import pallas as pl
from jax.experimental.pallas import tpu as pltpu
from jax.sharding import PartitionSpec as P

WIN = 8


EPS_NORM = 1e-05
MASK_FILL = -100.0
SCALE_CAP = math.log(100.0)
BIAS_RANGE = 16.0


def from_behind(block, axis, distance):
    devices = range(lax.axis_size(axis))
    route = [((i - distance) % len(devices), i) for i in devices]
    return lax.ppermute(block, axis, route)


def to_windows(block, window):
    images, height, width, depth = block.shape
    tiles = block.reshape(images, height // window, window, width // window, window, depth)
    tiles = tiles.transpose(0, 1, 3, 2, 4, 5)
    return tiles.reshape(images, height // window * (width // window), window * window, depth)


def from_windows(tiles, images, height, width, window):
    depth = tiles.shape[-1]
    grid = tiles.reshape(images, height // window, width // window, window, window, depth)
    return grid.transpose(0, 1, 3, 2, 4, 5).reshape(images, height, width, depth)


def region_of(coords, extent, window):
    return (coords >= extent - window).astype(jnp.int32) + (coords >= extent - window // 2).astype(
        jnp.int32
    )

GROUP = 4
FWD = 2
BWD = 4
LOG2E = math.log2(math.e)
VMEM_LIMIT = 40 * 2**20
FINISH_LIMIT = 4 * 2**20
MESH = pl.DeviceIdType.MESH
VMEM = pl.BlockSpec(memory_space=pltpu.VMEM)
NN = (((1,), (0,)), ((), ()))
NT = (((1,), (1,)), ((), ()))
TN = (((0,), (0,)), ((), ()))


def mxu(left, right, dims):
    return lax.dot_general(left, right, dims, preferred_element_type=jnp.float32)


def split(value):
    high = value.astype(jnp.bfloat16)
    return high, (value - high.astype(jnp.float32)).astype(jnp.bfloat16)


def mxu_fine(left, right, dims):
    high, low = split(left)
    return mxu(high, right, dims) + mxu(low, right, dims)


def same_block(rows, cols, row_size, col_size):
    row = lax.broadcasted_iota(jnp.int32, (rows, cols), 0) // row_size
    col = lax.broadcasted_iota(jnp.int32, (rows, cols), 1) // col_size
    return (row == col).astype(jnp.bfloat16)


def tile_heads(value, width):
    lane = lax.broadcasted_iota(jnp.int32, (1, value.shape[1]), 1) % (GROUP * width) // width
    rows = []
    for head in range(GROUP):
        rows.append(value * (lane == head).astype(jnp.bfloat16))
    return jnp.concatenate(rows, 0)


def gather_heads(value, width, length):
    lane = lax.broadcasted_iota(jnp.int32, (length, value.shape[1]), 1) // width
    total = value[:length]
    for head in range(1, GROUP):
        total = jnp.where(lane == head, value[head * length : (head + 1) * length], total)
    return total


def local_kernel(
    grid_cols, height, width, window,
    flat_ref, grad_ref, w_qkv_ref, w_proj_ref, bias_ref, scale_ref, gain_ref,
    d_flat_ref, d_wqkv_ref, d_wproj_ref, d_bias_ref, d_cos_ref, d_gain_ref,
    qkv_ref, att_ref, d_att_ref, d_qkv_ref, probs_ref, kinv_ref, qrow_ref, masked_ref, raw_q_ref, raw_k_ref,
    norm_ref,
):
    tokens, depth = flat_ref.shape
    f32, b16 = jnp.float32, jnp.bfloat16
    length = window * window
    count = tokens // length
    groups = bias_ref.shape[0]
    lanes = depth // groups
    heads = groups * GROUP
    head_dim = lanes // GROUP
    wide = GROUP * length
    row_base = lax.axis_index("ha") * (count // grid_cols * window)
    col_base = lax.axis_index("wa") * (grid_cols * window)

    qkv_ref[...] = mxu(flat_ref[...], w_qkv_ref[...], NN).astype(b16)
    lane_ones = same_block(lanes, wide, head_dim, length)
    lane_lane = same_block(lanes, lanes, head_dim, head_dim)

    head_rows = scale_ref.shape[0]
    pick = same_block(head_rows, depth, 1, head_dim)
    high, low = split(jnp.square(qkv_ref[:, :depth].astype(f32)))
    q_sums = mxu(pick, high, NT) + mxu(pick, low, NT)
    q_rows = lax.rsqrt(q_sums + 1.0) * scale_ref[:, :1]
    half = lax.broadcasted_iota(jnp.int32, (1, 2 * length), 1) < length
    for j in range(count // 2):
        base = q_rows[:, j * 2 * length : (j + 1) * 2 * length]
        turned = pltpu.roll(base, length, 1)
        for g in range(groups):
            for p in range(GROUP // 2):
                one, two = g * GROUP + 2 * p, g * GROUP + 2 * p + 1
                place = slice(p * 2 * length, (p + 1) * 2 * length)
                qrow_ref[2 * j, g, :, place] = jnp.where(half, base[one : one + 1], turned[two : two + 1])
                qrow_ref[2 * j + 1, g, :, place] = jnp.where(half, turned[one : one + 1], base[two : two + 1])
    for g in range(groups):
        query = qkv_ref[:, g * lanes : (g + 1) * lanes].astype(f32)
        key = qkv_ref[:, depth + g * lanes : depth + (g + 1) * lanes].astype(f32)
        high, low = split(jnp.square(key))
        kinv_ref[g] = lax.rsqrt(mxu(high, lane_ones, NN) + mxu(low, lane_ones, NN) + 1.0)
        norm_ref[1, g] = 1.0 / (mxu(high, lane_lane, NN) + mxu(low, lane_lane, NN) + 1.0)
        high, low = split(jnp.square(query))
        norm_ref[0, g] = 1.0 / (mxu(high, lane_lane, NN) + mxu(low, lane_lane, NN) + 1.0)

    mine = lax.broadcasted_iota(jnp.int32, (length, wide), 0)
    other = lax.broadcasted_iota(jnp.int32, (length, wide), 1) % length
    cut = window // 2
    row_off = (mine // window // cut) != (other // window // cut)
    col_off = (mine % window // cut) != (other % window // cut)
    for g in range(groups):
        bias = bias_ref[g] * LOG2E
        masked_ref[0, g] = bias
        masked_ref[1, g] = jnp.where(col_off, bias + MASK_FILL * LOG2E, bias)
        masked_ref[2, g] = jnp.where(row_off, bias + MASK_FILL * LOG2E, bias)
        masked_ref[3, g] = jnp.where(row_off | col_off, bias + MASK_FILL * LOG2E, bias)

    def load(ref, w, g, part):
        return ref[
            pl.ds(pl.multiple_of(w * length, length), length),
            part * depth + g * lanes : part * depth + (g + 1) * lanes,
        ]

    def forward(step, carry):
        units = [(step * FWD + k, g) for k in range(FWD) for g in range(groups)]
        scores = []
        for w, g in units:
            query, key = load(qkv_ref, w, g, 0), load(qkv_ref, w, g, 1)
            raw = mxu(key, tile_heads(query, head_dim), NT)
            last_row = (row_base + w // grid_cols * window) // (height - window)
            last_col = (col_base + w % grid_cols * window) // (width - window)
            kinv = kinv_ref[g, pl.ds(pl.multiple_of(w * length, length), length), :]
            scores.append(raw * kinv * (qrow_ref[w, g] * LOG2E) + masked_ref[last_row * 2 + last_col, g])
        for (w, g), score in zip(units, scores):
            expo = jnp.exp2(score - jnp.max(score, 0, keepdims=True))
            probs = expo * (1.0 / jnp.sum(expo, 0, keepdims=True))
            probs_ref[w, g] = probs
            att = gather_heads(mxu(probs.astype(b16), load(qkv_ref, w, g, 2), TN), head_dim, length)
            att_ref[
                pl.ds(pl.multiple_of(w * length, length), length), g * lanes : (g + 1) * lanes
            ] = att.astype(b16)
        return carry

    lax.fori_loop(0, count // FWD, forward, 0)

    proj = mxu(att_ref[...], w_proj_ref[...], NN)
    centre = proj - jnp.mean(proj, -1, keepdims=True)
    inv_std = lax.rsqrt(jnp.mean(centre * centre, -1, keepdims=True) + EPS_NORM)
    normed = centre * inv_std
    upstream = grad_ref[...].astype(f32)
    d_gain_ref[...] = jnp.sum(upstream * normed, 0, keepdims=True)
    scaled = upstream * gain_ref[...]
    d_proj = inv_std * (
        scaled
        - jnp.mean(scaled, -1, keepdims=True)
        - normed * jnp.mean(scaled * normed, -1, keepdims=True)
    )
    d_proj = d_proj.astype(b16)
    d_wproj_ref[...] = mxu(att_ref[...], d_proj, TN)
    d_att_ref[...] = mxu(d_proj, w_proj_ref[...], NT).astype(b16)
    d_bias_ref[...] = jnp.zeros_like(d_bias_ref)

    for g in range(groups):

        def backward(step, carry):
            units = [step * BWD + k for k in range(BWD)]
            grads = []
            for w in units:
                d_tall = tile_heads(load(d_att_ref, w, g, 0), head_dim)
                d_probs = mxu(load(qkv_ref, w, g, 2), d_tall, NT)
                d_value = mxu(probs_ref[w, g].astype(b16), d_tall, NN)
                d_qkv_ref[
                    pl.ds(pl.multiple_of(w * length, length), length),
                    2 * depth + g * lanes : 2 * depth + (g + 1) * lanes,
                ] = d_value.astype(b16)
                grads.append(d_probs)
            total = d_bias_ref[g]
            for w, d_probs in zip(units, grads):
                rows = pl.ds(pl.multiple_of(w * length, length), length)
                probs = probs_ref[w, g]
                d_scores = probs * (d_probs - jnp.sum(d_probs * probs, 0, keepdims=True))
                total = total + d_scores
                high, low = split(d_scores * kinv_ref[g, rows, :] * qrow_ref[w, g])
                both = jnp.concatenate([high, low], 0)
                query, key = load(qkv_ref, w, g, 0), load(qkv_ref, w, g, 1)
                pair = mxu(both, tile_heads(query, head_dim), NN)
                raw_k_ref[rows, :] = pair[:length] + pair[length:]
                tall = mxu(both, jnp.concatenate([key, key], 0), TN)
                raw_q_ref[rows, :] = gather_heads(tall, head_dim, length)
            d_bias_ref[g] = total
            return carry

        lax.fori_loop(0, count // BWD, backward, 0)
        for part, ref in enumerate((raw_q_ref, raw_k_ref)):
            place = slice(part * depth + g * lanes, part * depth + (g + 1) * lanes)
            value, grad = qkv_ref[:, place].astype(f32), ref[...]
            along = value * grad
            if part == 0:
                d_cos_ref[g] = jnp.sum(along, 0, keepdims=True)
            d_qkv_ref[:, place] = (
                grad - value * norm_ref[part, g] * mxu_fine(along, lane_lane, NN)
            ).astype(b16)
    d_wqkv_ref[...] = mxu(flat_ref[...], d_qkv_ref[...], TN)
    d_flat_ref[...] = mxu(d_qkv_ref[...], w_qkv_ref[...], NT).astype(b16)


def offset_onehot(window):
    places = np.arange(window * window)
    row_of, col_of = places // window, places % window
    offset = (row_of[:, None] - row_of[None, :] + window - 1) * (2 * window - 1) + (
        col_of[:, None] - col_of[None, :] + window - 1
    )
    return jnp.asarray(offset.reshape(-1), jnp.int32)


def three_parts(value):
    high = lax.reduce_precision(value, 8, 7)
    middle = lax.reduce_precision(value - high, 8, 7)
    return jnp.concatenate([high, middle, value - high - middle], 0).astype(jnp.bfloat16)


def local_grads(block, grad_block, row_base, col_base, height, width, window, params):
    w_qkv, w_proj, table_logits, logit_scale, gain = params
    images, rows, cols, depth = block.shape
    heads = logit_scale.shape[0]
    length = window * window
    groups = heads // GROUP
    wide = GROUP * length
    flat = to_windows(block, window).reshape(-1, depth)
    grad_flat = to_windows(grad_block, window).reshape(-1, depth)
    tokens = flat.shape[0]
    count = tokens // length
    scale = jnp.exp(jnp.minimum(logit_scale, SCALE_CAP))
    scale_rows = jnp.pad(scale, (0, -heads % 16)).reshape(-1, 1) * jnp.ones((1, 128), jnp.float32)
    sigma = jax.nn.sigmoid(table_logits)
    entries = table_logits.shape[1]
    hot = offset_onehot(window)[None, :] == jnp.arange(entries, dtype=jnp.int32)[:, None]
    hot = hot.astype(jnp.bfloat16)
    parts = jnp.dot(three_parts(sigma * BIAS_RANGE), hot, preferred_element_type=jnp.float32)
    rel_bias = jnp.sum(parts.reshape(3, heads, -1), 0).reshape(groups, GROUP, length, length)
    rel_bias = rel_bias.transpose(0, 3, 1, 2).reshape(groups, length, wide)
    f32, b16 = jnp.float32, jnp.bfloat16
    d_flat, d_wqkv, d_wproj, d_bias, d_cos, d_gain = pl.pallas_call(
        functools.partial(local_kernel, cols // window, height, width, window),
        out_shape=[
            jax.ShapeDtypeStruct((tokens, depth), b16),
            jax.ShapeDtypeStruct((depth, 3 * depth), f32),
            jax.ShapeDtypeStruct((depth, depth), f32),
            jax.ShapeDtypeStruct((groups, length, wide), f32),
            jax.ShapeDtypeStruct((groups, 1, depth // groups), f32),
            jax.ShapeDtypeStruct((1, depth), f32),
        ],
        in_specs=[VMEM] * 7,
        out_specs=[VMEM] * 6,
        scratch_shapes=[
            pltpu.VMEM((tokens, 3 * depth), b16),
            pltpu.VMEM((tokens, depth), b16),
            pltpu.VMEM((tokens, depth), b16),
            pltpu.VMEM((tokens, 3 * depth), b16),
            pltpu.VMEM((count, groups, length, wide), f32),
            pltpu.VMEM((groups, tokens, wide), f32),
            pltpu.VMEM((count, groups, 1, wide), f32),
            pltpu.VMEM((4, groups, length, wide), f32),
            pltpu.VMEM((tokens, depth // groups), f32),
            pltpu.VMEM((tokens, depth // groups), f32),
            pltpu.VMEM((2, groups, tokens, depth // groups), f32),
        ],
        compiler_params=pltpu.CompilerParams(vmem_limit_bytes=48 * 2**20),
        cost_estimate=pl.CostEstimate(
            flops=4_000_000_000, bytes_accessed=8_000_000, transcendentals=400_000
        ),
        name="local_grads",
    )(flat, grad_flat, w_qkv, w_proj, rel_bias, scale_rows, gain.reshape(1, depth))
    heads_bias = d_bias.reshape(groups, length, GROUP, length).transpose(0, 2, 3, 1)
    heads_bias = heads_bias.reshape(heads, length * length)
    sums = lax.dot_general(three_parts(heads_bias), hot, NT, preferred_element_type=jnp.float32)
    d_table = jnp.sum(sums.reshape(3, heads, entries), 0) * (BIAS_RANGE * sigma * (1.0 - sigma))
    live = (logit_scale < SCALE_CAP).astype(jnp.float32)
    d_scale = jnp.sum(d_cos.reshape(heads, depth // heads), 1) * live
    d_block = from_windows(d_flat.reshape(images, count, length, depth), images, rows, cols, window)
    return (d_block, (d_wqkv, d_wproj, d_table, d_scale, d_gain.reshape(depth)))


def half_turn(value, axis):
    return pltpu.roll(value, value.shape[axis] // 2, axis)


def exp_fine(value):
    whole = jnp.floor(value * LOG2E + 0.5)
    rest = value - whole * 0.693359375 + whole * 2.12194440e-4
    total = jnp.ones_like(rest)
    for k in range(8, 0, -1):
        total = 1.0 + total * rest * (1.0 / k)
    return total * jnp.exp2(whole)


def inverse(value):
    guess = 1.0 / value
    return guess * (2.0 - value * guess)


def place_of(index, window):
    return index // window * (2 * window - 1) + index % window


def expand_bias(table, length, window, groups, out_ref):
    span = table.shape[1]
    f32, b16 = jnp.float32, jnp.bfloat16
    heads = groups * GROUP
    base = jnp.concatenate([jnp.broadcast_to(table[h : h + 1], (window, span)) for h in range(heads)], 0)
    sub = lax.broadcasted_iota(jnp.int32, base.shape, 0) % window
    bit = 1
    while bit < window:
        base = jnp.where(sub // bit % 2 == 1, pltpu.roll(base, bit, 1), base)
        bit *= 2
    top = place_of(length - 1, window)
    turned = [
        pltpu.roll(base, (span - top + (2 * window - 1) * r) % span, 1)[:, : span // 2] for r in range(window)
    ]
    wide = GROUP * length
    row = lax.broadcasted_iota(jnp.int32, (span, wide), 0) % (span // 2)
    col = lax.broadcasted_iota(jnp.int32, (span, wide), 1)
    hit = row == place_of(col % length, window)
    for g in range(groups):
        total = jnp.zeros((length, wide), f32)
        for k in range(GROUP):
            h = g * GROUP + k
            block = jnp.concatenate([t[h * window : (h + 1) * window] for t in turned], 0)
            pair = jnp.concatenate(split(block), 1)
            total = total + mxu(pair, (hit & (col // length == k)).astype(b16), NN)
        out_ref[0, g] = total


def fold_bias(grads, length, window, span):
    f32, b16 = jnp.float32, jnp.bfloat16
    wide = GROUP * length
    row = lax.broadcasted_iota(jnp.int32, (wide, span // 2), 0)
    col = lax.broadcasted_iota(jnp.int32, (wide, span // 2), 1)
    hit = col == place_of(row % length, window)
    both = jnp.concatenate([half for grad in grads for half in split(grad)], 0)
    by_head = [None] * (len(grads) * GROUP)
    for k in range(GROUP):
        pairs = mxu(both, (hit & (row // length == k)).astype(b16), NN)
        for g in range(len(grads)):
            pair = pairs[2 * g * length : (2 * g + 2) * length]
            block = pair[:length] + pair[length:]
            by_head[g * GROUP + k] = jnp.concatenate([block, jnp.zeros_like(block)], 1)
    parts = [
        jnp.concatenate([block[r * window : (r + 1) * window] for block in by_head], 0) for r in range(window)
    ]
    step = 2 * window - 1
    while len(parts) > 1:
        parts = [pltpu.roll(parts[i], step, 1) + parts[i + 1] for i in range(0, len(parts), 2)]
        step *= 2
    total = parts[0]
    sub = window - 1 - lax.broadcasted_iota(jnp.int32, total.shape, 0) % window
    bit = 1
    while bit < window:
        total = jnp.where(sub // bit % 2 == 1, pltpu.roll(total, bit, 1), total)
        bit *= 2
    return [jnp.sum(total[k * window : (k + 1) * window], 0, keepdims=True) for k in range(len(by_head))]


def whole_kernel(
    shape, height, width, window,
    tokens_ref, cot_ref, w_qkv_hbm, w_proj_hbm, table_hbm, gain_hbm, scale_ref,
    d_tok_ref, grads_out, table_out, scale_out, gain_out,
    tok, cot, w_qkv_ref, w_proj_ref, table_in, gain_ref, table_ref, local_sems,
    col_send, row_get, col_get, diag_get, halo_sems,
    flat_ref, grad_ref, d_flat_ref, d_proj_ref,
    qkv_ref, att_ref, d_att_ref, d_qkv_ref, probs_ref, kinv_ref, qrow_ref, masked_ref, raw_q_ref, raw_k_ref,
    norm_ref, d_bias_ref, p_mid, k_first, product_ref,
    row_back, col_back, row_back_get, col_back_get, diag_back_get, back_sems,
    small, small_core, small_a, small_image, small_b, small_side, small_c, small_near, small_total, tiny_sems,
    *chunk_refs,
):
    size_h, size_w = shape
    chips = size_h // 2
    peers = chips * size_w
    ha, wa, ba = lax.axis_index("ha"), lax.axis_index("wa"), lax.axis_index("ba")
    core = ha % 2
    me = wa * chips + ha // 2
    partner = (ha + 1 - 2 * core, wa, ba)
    image, side, corner = (ha, wa, 1 - ba), (ha, 1 - wa, ba), (ha, 1 - wa, 1 - ba)
    above, below = lax.rem(ha + size_h - 1, size_h), lax.rem(ha + 1, size_h)
    left, right = lax.rem(wa + size_w - 1, size_w), lax.rem(wa + 1, size_w)
    f32, b16 = jnp.float32, jnp.bfloat16

    def peer(step):
        other = lax.rem(me + step, peers)
        return other, (other % chips * 2 + core, other // chips, ba)

    loads = []
    for k, (src, dst) in enumerate(
        (
            (tokens_ref.at[0], tok), (cot_ref.at[0], cot), (w_qkv_hbm, w_qkv_ref), (w_proj_hbm, w_proj_ref),
            (table_hbm, table_in), (gain_hbm, gain_ref),
        )
    ):
        copy = pltpu.make_async_copy(src, dst, local_sems.at[k])
        copy.start()
        loads.append(copy)
    targets = [
        (above, wa, ba), (below, wa, ba), (ha, left, ba), (ha, right, ba), (above, left, ba), (below, right, ba),
        partner, image, corner,
    ] + [peer(step)[1] for step in range(1, peers)]
    barrier = pltpu.get_barrier_semaphore()
    for device in targets:
        pl.semaphore_signal(barrier, inc=1, device_id=device, device_id_type=MESH)

    def start(src, dst, sems, device):
        copy = pltpu.make_async_remote_copy(
            src_ref=src, dst_ref=dst, send_sem=sems.at[0], recv_sem=sems.at[1],
            device_id=device, device_id_type=MESH,
        )
        copy.start()
        return copy

    rows, cols, depth = tok.shape
    cut = window // 2
    length = window * window
    across = cols // window
    count = rows // window * across
    tokens = count * length
    groups = qrow_ref.shape[1]
    lanes = depth // groups
    head_dim = lanes // GROUP
    wide = GROUP * length
    low_sub = lax.broadcasted_iota(jnp.int32, (window, depth), 0) < cut

    def pack_columns(a, ref):
        loads[a].wait()
        for j in range(rows // 2):
            first = ref[2 * j, :window, :].astype(f32)
            second = ref[2 * j + 1, :window, :].astype(f32)
            col_send[a, j] = jnp.where(low_sub, first, half_turn(second, 0)).astype(b16)

    halos = {}

    def send_halo(a, ref):
        halos[a, 0] = start(col_send.at[a], col_get.at[a], halo_sems.at[a, 1], (ha, left, ba))
        halos[a, 1] = start(ref.at[pl.ds(0, cut)], row_get.at[a], halo_sems.at[a, 0], (above, wa, ba))
        halos[a, 2] = start(
            col_send.at[a, pl.ds(0, cut // 2)], diag_get.at[a], halo_sems.at[a, 2], (above, left, ba)
        )

    pack_columns(0, tok)
    pl.semaphore_wait(barrier, len(targets))
    send_halo(0, tok)
    pack_columns(1, cot)
    send_halo(1, cot)

    loads[4].wait()
    loads[5].wait()
    heads = groups * GROUP
    entries = table_in.shape[1]
    table_ref[...] = jnp.zeros_like(table_ref)
    table_ref[:heads, :entries] = table_in[...]
    sigma = inverse(1.0 + exp_fine(-table_ref[...]))
    head_rows, span = table_ref.shape
    spot = lax.broadcasted_iota(jnp.int32, (head_rows, 128), 0)
    logits = jnp.zeros((head_rows, 128), f32)
    for h in range(heads):
        logits = jnp.where(spot == h, scale_ref[h], logits)
    scale = exp_fine(jnp.minimum(logits, SCALE_CAP))
    expand_bias(sigma * (BIAS_RANGE * LOG2E), length, window, groups, masked_ref)
    mine = lax.broadcasted_iota(jnp.int32, (length, wide), 0)
    other = lax.broadcasted_iota(jnp.int32, (length, wide), 1) % length
    row_off = (mine // window // cut) != (other // window // cut)
    col_off = (mine % window // cut) != (other % window // cut)
    for g in range(groups):
        bias = masked_ref[0, g]
        masked_ref[1, g] = jnp.where(col_off, bias + MASK_FILL * LOG2E, bias)
        masked_ref[2, g] = jnp.where(row_off, bias + MASK_FILL * LOG2E, bias)
        masked_ref[3, g] = jnp.where(row_off | col_off, bias + MASK_FILL * LOG2E, bias)
    small[...] = jnp.zeros_like(small)

    def gather_rows(a, ref, out_ref, from_row, to_row):
        def shifted(i):
            if i + cut < rows:
                row, edge = ref[i + cut], col_get[a, (i + cut) // 2]
            else:
                row, edge = row_get[a, i + cut - rows], diag_get[a, (i + cut - rows) // 2]
            row, edge = row.astype(f32), edge.astype(f32)
            turned = [half_turn(row[k * window : (k + 1) * window], 0) for k in range(across)]
            turned.append(half_turn(edge, 0) if i % 2 == 0 else edge)
            return [jnp.where(low_sub, turned[k], turned[k + 1]) for k in range(across)]

        for i in range(from_row, to_row, 2):
            one, two = shifted(i), shifted(i + 1)
            for k in range(across):
                begin = (i // window * across + k) * length + i % window * window
                out_ref[begin : begin + 2 * window] = jnp.concatenate([one[k], two[k]], 0).astype(b16)

    row_base, col_base = ha * rows, wa * cols
    lane_ones = same_block(lanes, wide, head_dim, length)
    lane_lane = same_block(lanes, lanes, head_dim, head_dim)
    pick = same_block(head_rows, depth, 1, head_dim)
    half = lax.broadcasted_iota(jnp.int32, (1, 2 * length), 1) < length

    def project(begin_window, end_window):
        part_rows = slice(begin_window * length, end_window * length)
        qkv_ref[part_rows] = mxu(flat_ref[part_rows], w_qkv_ref[...], NN).astype(b16)
        high, low = split(jnp.square(qkv_ref[part_rows, :depth].astype(f32)))
        q_sums = mxu(pick, high, NT) + mxu(pick, low, NT)
        q_rows = lax.rsqrt(q_sums + 1.0) * scale[:, :1]
        for j in range(begin_window // 2, end_window // 2):
            shifted_j = 2 * j - begin_window
            base = q_rows[:, shifted_j * length : (shifted_j + 2) * length]
            turned = half_turn(base, 1)
            for g in range(groups):
                for p in range(GROUP // 2):
                    one, two = g * GROUP + 2 * p, g * GROUP + 2 * p + 1
                    place = slice(p * 2 * length, (p + 1) * 2 * length)
                    qrow_ref[2 * j, g, :, place] = jnp.where(half, base[one : one + 1], turned[two : two + 1])
                    qrow_ref[2 * j + 1, g, :, place] = jnp.where(half, turned[one : one + 1], base[two : two + 1])
        for g in range(groups):
            key = qkv_ref[part_rows, depth + g * lanes : depth + (g + 1) * lanes].astype(f32)
            high, low = split(jnp.square(key))
            kinv_ref[g, part_rows] = lax.rsqrt(mxu(high, lane_ones, NN) + mxu(low, lane_ones, NN) + 1.0)

    def norms(begin_window, end_window):
        part_rows = slice(begin_window * length, end_window * length)
        for g in range(groups):
            for part in range(2):
                place = slice(part * depth + g * lanes, part * depth + (g + 1) * lanes)
                high, low = split(jnp.square(qkv_ref[part_rows, place].astype(f32)))
                norm_ref[part, g, part_rows] = 1.0 / (
                    mxu(high, lane_lane, NN) + mxu(low, lane_lane, NN) + 1.0
                )

    def load(ref, w, g, part):
        return ref[
            pl.ds(pl.multiple_of(w * length, length), length),
            part * depth + g * lanes : part * depth + (g + 1) * lanes,
        ]

    def forward(step, carry):
        units = [(step * FWD + k, g) for k in range(FWD) for g in range(groups)]
        scores = []
        for w, g in units:
            query, key = load(qkv_ref, w, g, 0), load(qkv_ref, w, g, 1)
            raw = mxu(key, tile_heads(query, head_dim), NT)
            last_row = (row_base + w // across * window) // (height - window)
            last_col = (col_base + w % across * window) // (width - window)
            kinv = kinv_ref[g, pl.ds(pl.multiple_of(w * length, length), length), :]
            scores.append(raw * kinv * (qrow_ref[w, g] * LOG2E) + masked_ref[last_row * 2 + last_col, g])
        for (w, g), score in zip(units, scores):
            expo = jnp.exp2(score - jnp.max(score, 0, keepdims=True))
            probs = expo * (1.0 / jnp.sum(expo, 0, keepdims=True))
            probs_ref[w, g] = probs
            att = gather_heads(mxu(probs.astype(b16), load(qkv_ref, w, g, 2), TN), head_dim, length)
            att_ref[
                pl.ds(pl.multiple_of(w * length, length), length), g * lanes : (g + 1) * lanes
            ] = att.astype(b16)
        return carry

    def norm_gradient(begin_window, end_window):
        part_rows = slice(begin_window * length, end_window * length)
        proj = mxu(att_ref[part_rows], w_proj_ref[...], NN)
        centre = proj - jnp.mean(proj, -1, keepdims=True)
        inv_std = lax.rsqrt(jnp.mean(centre * centre, -1, keepdims=True) + EPS_NORM)
        normed = centre * inv_std
        upstream = grad_ref[part_rows].astype(f32)
        d_gain = jnp.sum(upstream * normed, 0, keepdims=True)
        scaled = upstream * gain_ref[...].reshape(1, depth)
        d_proj = inv_std * (
            scaled
            - jnp.mean(scaled, -1, keepdims=True)
            - normed * jnp.mean(scaled * normed, -1, keepdims=True)
        )
        d_proj = d_proj.astype(b16)
        d_proj_ref[part_rows] = d_proj
        d_att_ref[part_rows] = mxu(d_proj, w_proj_ref[...], NT).astype(b16)
        return d_gain

    early = count - across
    halos[0, 0].wait()
    gather_rows(0, tok, flat_ref, 0, rows - window)
    loads[2].wait()
    project(0, early)
    lax.fori_loop(0, early // FWD, forward, 0)
    norms(0, early)
    halos[1, 0].wait()
    gather_rows(1, cot, grad_ref, 0, rows - window)
    loads[3].wait()
    d_gain = norm_gradient(0, early)
    halos[0, 1].wait()
    halos[0, 2].wait()
    gather_rows(0, tok, flat_ref, rows - window, rows)
    project(early, count)
    lax.fori_loop(early // FWD, count // FWD, forward, 0)
    halos[1, 1].wait()
    halos[1, 2].wait()
    gather_rows(1, cot, grad_ref, rows - window, rows)
    d_gain = d_gain + norm_gradient(early, count)
    small[heads : heads + 1, :] = d_gain[:, :span]
    small[heads + 1 : heads + 2, : depth - span] = d_gain[:, span:]
    per = len(chunk_refs) // 4
    chunks = [chunk_refs[c * per : (c + 1) * per] for c in range(4)]
    flying = {}

    def begin(c):
        core_send, core_mine, core_get = chunks[c][:3]
        w = core_send.shape[0] // 2
        for side_of in range(2):
            here = slice(side_of * w, (side_of + 1) * w)
            base = 2 * side_of * w
            theirs = pl.ds(pl.multiple_of(base + (1 - core) * w, 32), w)
            core_send[here] = product_ref[theirs, :].astype(b16)
        flying[c] = start(core_send, core_get, chunks[c][9], partner)
        for side_of in range(2):
            here = slice(side_of * w, (side_of + 1) * w)
            core_mine[here] = product_ref[pl.ds(pl.multiple_of(2 * side_of * w + core * w, 32), w), :]

    def cross(c):
        core_send, core_mine, core_get, plane_send, plane_get = chunks[c][:5]
        flying[c].wait()
        core_mine[...] = core_mine[...] + core_get[...].astype(f32)
        w = plane_send.shape[1]
        flying[c] = []
        for k, (b, y, device) in enumerate(((1 - ba, wa, image), (ba, 1 - wa, side), (1 - ba, 1 - wa, corner))):
            place = pl.ds(pl.multiple_of((2 * b + y) * w, 32), w)
            plane_send[k] = core_mine[place, :].astype(b16)
            flying[c].append(start(plane_send.at[k], plane_get.at[k], chunks[c][10].at[k], device))

    def scatter(c):
        core_mine, plane_get, near_send, near_get = chunks[c][1], chunks[c][4], chunks[c][5], chunks[c][6]
        for copy in flying[c]:
            copy.wait()
        w = plane_get.shape[1]
        total = core_mine[pl.ds(pl.multiple_of((2 * ba + wa) * w, 32), w), :]
        for k in range(3):
            total = total + plane_get[k].astype(f32)
        r = near_send.shape[1]
        for j in range(chips):
            near_send[j] = total[j * r : (j + 1) * r].astype(b16)
        flying[c] = []
        for step in range(1, chips):
            far_chip = lax.rem(ha // 2 + step, chips)
            flying[c].append(
                start(
                    near_send.at[far_chip], near_get.at[step - 1], chunks[c][11].at[step - 1],
                    (2 * far_chip + core, wa, ba),
                )
            )

    def gather(c):
        near_send, near_get, whole = chunks[c][5:8]
        for copy in flying[c]:
            copy.wait()
        total = near_send[ha // 2].astype(f32)
        for step in range(1, chips):
            total = total + near_get[step - 1].astype(f32)
        whole[me] = total.astype(b16)
        flying[c] = []
        for step in range(1, peers):
            flying[c].append(start(whole.at[me], whole.at[me], chunks[c][12].at[step - 1], peer(step)[1]))

    def spread_column(c):
        near_send, near_get, whole = chunks[c][5:8]
        for copy in flying[c]:
            copy.wait()
        total = near_send[ha // 2].astype(f32)
        for step in range(1, chips):
            total = total + near_get[step - 1].astype(f32)
        whole[me] = total.astype(b16)
        flying[c] = []
        for step in range(1, chips):
            far_chip = lax.rem(ha // 2 + step, chips)
            flying[c].append(
                start(whole.at[me], whole.at[me], chunks[c][12].at[step - 1], (2 * far_chip + core, wa, ba))
            )

    def relay(c):
        whole = chunks[c][7]
        for copy in flying[c]:
            copy.wait()
        held = pl.ds(wa * chips, chips)
        flying[c] = [start(whole.at[held], whole.at[held], chunks[c][12].at[chips - 1], side)]

    def mirror(c):
        whole, core_all = chunks[c][7:9]
        for copy in flying[c]:
            copy.wait()
        flying[c] = start(whole, core_all, chunks[c][13], partner)

    def finish(c):
        put(c, chunks[c][7], core)
        flying[c].wait()
        put(c, chunks[c][8], 1 - core)

    unit = lanes // 2
    proj_at = 3 * depth // 2

    targets_of = [
        [(proj_at + k * unit, proj_at + (1 + k) * unit) for k in range(2)],
        [(k * unit, (3 + k) * unit) for k in range(2)],
        [((4 + k) * unit, (1 + k if k < 2 else 5 + k) * unit) for k in range(4)],
        [(2 * unit, 5 * unit), (3 * unit, 6 * unit), (8 * unit, 0), (proj_at + 2 * unit, proj_at)],
    ]

    def put(c, source, which):
        r = source.shape[1]
        blocks = peers * r // unit
        for k in range(blocks):
            zero, one = targets_of[c][k], targets_of[c][blocks + k]
            row = jnp.where(
                which == 0, jnp.where(ba == 0, zero[0], zero[1]), jnp.where(ba == 0, one[0], one[1])
            )
            for j in range(unit // r):
                grads_out[pl.ds(pl.multiple_of(row + j * r, 8), r), :] = source[k * (unit // r) + j].astype(f32)

    product = mxu(d_proj_ref[...], att_ref[...], TN)
    product_ref[:lanes] = product[:lanes]
    p_mid[...] = product[lanes : 2 * lanes]
    product_ref[lanes : 2 * lanes] = product[2 * lanes :]
    begin(0)

    def backward_group(g, between=None):
        def backward(step, total):
            units = [step * BWD + k for k in range(BWD)]
            grads = []
            for w in units:
                d_tall = tile_heads(load(d_att_ref, w, g, 0), head_dim)
                d_probs = mxu(load(qkv_ref, w, g, 2), d_tall, NT)
                d_value = mxu(probs_ref[w, g].astype(b16), d_tall, NN)
                d_qkv_ref[
                    pl.ds(pl.multiple_of(w * length, length), length),
                    2 * depth + g * lanes : 2 * depth + (g + 1) * lanes,
                ] = d_value.astype(b16)
                grads.append(d_probs)
            summed = d_bias_ref[g]
            for w, d_probs in zip(units, grads):
                place = pl.ds(pl.multiple_of(w * length, length), length)
                probs = probs_ref[w, g]
                d_scores = probs * (d_probs - jnp.sum(d_probs * probs, 0, keepdims=True))
                summed = summed + d_scores
                high, low = split(d_scores * kinv_ref[g, place, :] * qrow_ref[w, g])
                both = jnp.concatenate([high, low], 0)
                query, key = load(qkv_ref, w, g, 0), load(qkv_ref, w, g, 1)
                pair = mxu(both, tile_heads(query, head_dim), NN)
                raw_k_ref[place, :] = pair[:length] + pair[length:]
                tall = mxu(both, jnp.concatenate([key, key], 0), TN)
                raw_q_ref[place, :] = gather_heads(tall, head_dim, length)
            d_bias_ref[g] = summed
            return total

        d_bias_ref[g] = jnp.zeros((length, wide), f32)
        cut_at = count // BWD // 2 if between else count // BWD
        lax.fori_loop(0, cut_at, backward, 0)
        if between:
            between()
            lax.fori_loop(cut_at, count // BWD, backward, 0)
        for part, ref in enumerate((raw_q_ref, raw_k_ref)):
            place = slice(part * depth + g * lanes, part * depth + (g + 1) * lanes)
            value, grad = qkv_ref[:, place].astype(f32), ref[...]
            along = value * grad
            if part == 0:
                spot = depth - span + g * lanes
                small[
                    heads + 1 + spot // span : heads + 2 + spot // span, spot % span : spot % span + lanes
                ] = jnp.sum(along, 0, keepdims=True)
            d_qkv_ref[:, place] = (
                grad - value * norm_ref[part, g] * mxu_fine(along, lane_lane, NN)
            ).astype(b16)

    def dense(g):
        joined = jnp.concatenate(
            [d_qkv_ref[:, part * depth + g * lanes : part * depth + (g + 1) * lanes] for part in range(3)], 1
        )
        return mxu(joined, flat_ref[...], TN)

    norms(early, count)
    backward_group(0)
    product = dense(0)
    product_ref[:lanes] = product[:lanes]
    product_ref[lanes : 2 * lanes] = product[2 * lanes :]
    k_first[...] = product[lanes : 2 * lanes]
    begin(1)
    cross(0)
    backward_group(2, lambda: cross(1))
    product = dense(2)
    product_ref[:lanes] = product[:lanes]
    product_ref[lanes : 2 * lanes] = k_first[...]
    product_ref[2 * lanes : 4 * lanes] = product[lanes:]
    begin(2)
    scatter(0)
    backward_group(1, lambda: cross(2))
    product = dense(1)
    product_ref[:lanes] = product[:lanes]
    product_ref[lanes : lanes + unit] = product[lanes : lanes + unit]
    product_ref[lanes + unit : 2 * lanes] = p_mid[:unit]
    product_ref[2 * lanes : 3 * lanes] = product[2 * lanes :]
    product_ref[3 * lanes : 3 * lanes + unit] = product[lanes + unit : 2 * lanes]
    product_ref[3 * lanes + unit : 4 * lanes] = p_mid[unit:]
    begin(3)
    scatter(1)
    d_flat_ref[...] = mxu(d_qkv_ref[...], w_qkv_ref[...], NT).astype(b16)

    def back_tiles(i):
        begin_row = i // window * across * length + i % window * window
        return [
            half_turn(d_flat_ref[begin_row + k * length : begin_row + k * length + window].astype(f32), 0)
            for k in range(across)
        ]

    for i in range(0, rows, 2):
        one, two = back_tiles(i), back_tiles(i + 1)
        col_back[i // 2] = jnp.where(low_sub, one[-1], half_turn(two[-1], 0)).astype(b16)
        if i >= rows - cut:
            row_back[i - (rows - cut)] = jnp.concatenate(one, 0).astype(b16)
            row_back[i + 1 - (rows - cut)] = jnp.concatenate(two, 0).astype(b16)
    far = (rows - cut) // 2
    back = [
        start(row_back, row_back_get, back_sems.at[0], (below, wa, ba)),
        start(col_back.at[pl.ds(0, far)], col_back_get, back_sems.at[1], (ha, right, ba)),
        start(col_back.at[pl.ds(far, cut // 2)], diag_back_get, back_sems.at[2], (below, right, ba)),
    ]
    cross(3)
    spread_column(0)
    for k, row in enumerate(fold_bias([d_bias_ref[g] for g in range(groups)], length, window, span)):
        small[k : k + 1, :] = row
    tiny = start(small, small_core, tiny_sems.at[0], partner)

    def put_row(i, turned, edge, odd):
        ahead = [half_turn(edge, 0) if odd else edge] + turned
        out = [jnp.where(low_sub, ahead[k], ahead[k + 1]) for k in range(across)]
        d_tok_ref[i] = (jnp.concatenate(out, 0) + cot[i].astype(f32)).astype(b16)

    scatter(2)
    back[1].wait()
    for i in range(rows - cut):
        put_row(i + cut, back_tiles(i), col_back_get[i // 2].astype(f32), i % 2 == 1)
    spread_column(1)
    tiny.wait()
    small_half = small_a.shape[0]
    my_rows = pl.ds(pl.multiple_of(core * small_half, 8), small_half)
    small_a[...] = small[my_rows, :] + small_core[my_rows, :]
    tiny = start(small_a, small_image, tiny_sems.at[1], image)
    relay(0)
    back[0].wait()
    back[2].wait()
    for i in range(cut):
        whole_row = row_back_get[i].astype(f32)
        turned = [whole_row[k * window : (k + 1) * window] for k in range(across)]
        put_row(i, turned, diag_back_get[i // 2].astype(f32), i % 2 == 1)
    scatter(3)
    tiny.wait()
    small_b[...] = small_a[...] + small_image[...]
    tiny = start(small_b, small_side, tiny_sems.at[2], side)
    spread_column(2)
    mirror(0)
    relay(1)
    tiny.wait()
    small_c[...] = small_b[...] + small_side[...]
    tinies = []
    for step in range(1, chips):
        far_chip = lax.rem(ha // 2 + step, chips)
        tinies.append(
            start(small_c, small_near.at[step - 1], tiny_sems.at[step + 2], (2 * far_chip + core, wa, ba))
        )
    finish(0)
    gather(3)
    relay(2)
    mirror(1)
    for copy in tinies:
        copy.wait()
    total = small_c[...]
    for step in range(1, chips):
        total = total + small_near[step - 1]
    small_total[my_rows, :] = total
    tiny = start(small_total.at[my_rows], small_total.at[my_rows], tiny_sems.at[chips + 2], partner)
    finish(1)
    mirror(2)
    tiny.wait()
    total = small_total[...]
    table_out[...] = (total[: head_rows] * (BIAS_RANGE * sigma * (1.0 - sigma)))[:heads, :entries]
    gain_row = jnp.concatenate([total[heads : heads + 1, :], total[heads + 1 : heads + 2, : depth - span]], 1)
    gain_out[...] = gain_row.reshape(depth)
    sums = jnp.concatenate([total[heads + 1 : heads + 2, depth - span :], total[heads + 2 : heads + 3, :]], 1)
    sums = mxu_fine(jnp.broadcast_to(sums, (8, depth)), same_block(depth, 128, head_dim, 1), NN)[:1]
    at = lax.broadcasted_iota(jnp.int32, (1, 128), 1)
    logits = jnp.zeros((1, 128), f32)
    for h in range(heads):
        logits = jnp.where(at == h, scale_ref[h], logits)
    scale_out[...] = jnp.where(logits < SCALE_CAP, sums, 0.0).reshape(128)[:heads]
    mirror(3)
    finish(2)
    finish(3)


def finish_kernel(tok_ref, grads_ref, table_ref, scale_ref, gain_ref, tok, wq, wp, table, scale, gain, sems):
    cut = wq.shape[0]
    pairs = (
        (grads_ref.at[pl.ds(0, cut)], wq), (grads_ref.at[pl.ds(cut, wp.shape[0])], wp), (tok_ref, tok),
        (table_ref, table), (scale_ref, scale), (gain_ref, gain),
    )
    copies = [pltpu.make_async_copy(src, dst, sems.at[k]) for k, (src, dst) in enumerate(pairs)]
    for copy in copies:
        copy.start()
    for copy in copies:
        copy.wait()


def whole_grads(tokens, cotangent, w_qkv, w_proj, table_logits, logit_scale, gain, height, width, window):
    size_h, size_w = lax.axis_size("ha"), lax.axis_size("wa")
    peers = size_h // 2 * size_w
    f32, b16 = jnp.float32, jnp.bfloat16
    images, rows, cols, depth = tokens.shape
    heads = logit_scale.shape[0]
    entries = table_logits.shape[1]
    groups = heads // GROUP
    lanes = depth // groups
    length = window * window
    wide = GROUP * length
    total = rows * cols
    count = total // length
    cut = window // 2
    span = 256
    head_rows = -(-heads // 16) * 16
    half = depth // 2
    chips = size_h // 2
    dma, vmem = pltpu.SemaphoreType.DMA, pltpu.VMEM
    chunk_scratch = []
    for w in (lanes // 2, lanes // 2, lanes, lanes):
        r = w // peers
        chunk_scratch += [
            vmem((2 * w, depth), b16), vmem((2 * w, depth), f32), vmem((2 * w, depth), b16),
            vmem((3, w // 2, depth), b16), vmem((3, w // 2, depth), b16),
            vmem((chips, r, depth), b16), vmem((chips - 1, r, depth), b16),
            vmem((peers, r, depth), b16), vmem((peers, r, depth), b16),
            dma((2,)), dma((3, 2)), dma((chips - 1, 2)), dma((peers - 1, 2)), dma((2,)),
        ]
    small, part = (16, span), (8, span)
    anywhere = pl.BlockSpec(memory_space=pltpu.HBM)
    pinned = [
        pltpu.with_memory_space_constraint(x, pltpu.HBM)
        for x in (tokens, cotangent, w_qkv, w_proj, table_logits, gain)
    ]
    outs = pl.pallas_call(
        functools.partial(whole_kernel, (size_h, size_w), height, width, window),
        out_shape=[
            jax.ShapeDtypeStruct((rows, cols, depth), b16),
            jax.ShapeDtypeStruct((2 * depth, depth), f32),
            jax.ShapeDtypeStruct((heads, entries), f32),
            jax.ShapeDtypeStruct((heads,), f32),
            jax.ShapeDtypeStruct((depth,), f32),
        ],
        in_specs=[anywhere] * 6 + [pl.BlockSpec(memory_space=pltpu.SMEM)],
        out_specs=[VMEM] * 5,
        scratch_shapes=[
            vmem((rows, cols, depth), b16), vmem((rows, cols, depth), b16),
            vmem((depth, 3 * depth), b16), vmem((depth, depth), b16),
            vmem((heads, entries), f32), vmem((depth,), f32), vmem((head_rows, span), f32), dma((6,)),
            vmem((2, rows // 2, window, depth), b16), vmem((2, cut, cols, depth), b16),
            vmem((2, rows // 2, window, depth), b16), vmem((2, cut // 2, window, depth), b16), dma((2, 3, 2)),
            vmem((total, depth), b16), vmem((total, depth), b16), vmem((total, depth), b16), vmem((total, depth), b16),
            vmem((total, 3 * depth), b16), vmem((total, depth), b16), vmem((total, depth), b16),
            vmem((total, 3 * depth), b16), vmem((count, groups, length, wide), f32), vmem((groups, total, wide), f32),
            vmem((count, groups, 1, wide), f32), vmem((4, groups, length, wide), f32),
            vmem((total, lanes), f32), vmem((total, lanes), f32), vmem((2, groups, total, lanes), f32),
            vmem((groups, length, wide), f32), vmem((lanes, depth), f32), vmem((lanes, depth), f32),
            vmem((4 * lanes, depth), f32),
            vmem((cut, cols, depth), b16), vmem((rows // 2, window, depth), b16), vmem((cut, cols, depth), b16),
            vmem(((rows - cut) // 2, window, depth), b16), vmem((cut // 2, window, depth), b16), dma((3, 2)),
            vmem(small, f32), vmem(small, f32), vmem(part, f32), vmem(part, f32), vmem(part, f32), vmem(part, f32),
            vmem(part, f32), vmem((chips - 1, *part), f32), vmem(small, f32), dma((chips + 3, 2)),
            *chunk_scratch,
        ],
        compiler_params=pltpu.CompilerParams(
            collective_id=0, has_side_effects=True, vmem_limit_bytes=VMEM_LIMIT
        ),
        name="whole_grads",
    )(*pinned, logit_scale)
    d_tok, half_qkv, half_proj, d_table, d_scale, d_gain = pl.pallas_call(
        finish_kernel,
        out_shape=[
            jax.ShapeDtypeStruct((rows, cols, depth), b16),
            jax.ShapeDtypeStruct((3 * depth // 2, depth), f32),
            jax.ShapeDtypeStruct((depth // 2, depth), f32),
            jax.ShapeDtypeStruct((heads, entries), f32),
            jax.ShapeDtypeStruct((heads,), f32),
            jax.ShapeDtypeStruct((depth,), f32),
        ],
        in_specs=[VMEM] * 5,
        out_specs=[anywhere] * 6,
        scratch_shapes=[dma((6,))],
        compiler_params=pltpu.CompilerParams(vmem_limit_bytes=FINISH_LIMIT),
        name="finish",
    )(*outs)
    return d_tok[None], half_qkv.T, half_proj.T, d_table, d_scale, d_gain


def can_join(tokens, logit_scale):
    size_h, size_w, size_b = (lax.axis_size(name) for name in ("ha", "wa", "ba"))
    images, rows, cols, depth = tokens.shape
    peers = size_h // 2 * size_w
    return (
        images == 1 and size_b == 2 and size_w == 2 and size_h % 2 == 0 and size_h > 2
        and logit_scale.shape[0] == 3 * GROUP and depth == 3 * 128 and WIN == 8
        and rows % WIN == 0 and cols % (2 * WIN) == 0 and rows * cols // 64 % (2 * BWD) == 0 and rows > WIN
        and 64 % peers == 0 and 64 // peers % 8 == 0
    )


def shift_in(tokens, cotangent, shift):
    stacked = jnp.stack([tokens, cotangent])
    below = from_behind(stacked[:, :, :shift], "ha", -1)
    tall = jnp.concatenate([stacked[:, :, shift:], below], 2)
    beside = from_behind(tall[:, :, :, :shift], "wa", -1)
    moved = jnp.concatenate([tall[:, :, :, shift:], beside], 3)
    return (moved[0], moved[1])


def shift_out(grads, shift):
    rows = grads.shape[1]
    cols = grads.shape[2]
    right = from_behind(grads[:, :, cols - shift :], "wa", 1)
    wide = jnp.concatenate([right, grads[:, :, : cols - shift]], 2)
    lower = from_behind(wide[:, rows - shift :], "ha", 1)
    return jnp.concatenate([lower, wide[:, : rows - shift]], 1)


def shards(tokens, cotangent, w_qkv, w_proj, table_logits, logit_scale, gain):
    rows = tokens.shape[1]
    cols = tokens.shape[2]
    shift = WIN // 2
    height = rows * lax.axis_size("ha")
    width = cols * lax.axis_size("wa")
    row_base = lax.axis_index("ha") * rows
    col_base = lax.axis_index("wa") * cols
    if can_join(tokens, logit_scale):
        return whole_grads(
            tokens, cotangent, w_qkv, w_proj, table_logits, logit_scale, gain, height, width, WIN
        )
    params = (w_qkv, w_proj, table_logits, logit_scale, gain)
    moved, moved_grad = shift_in(tokens, cotangent, shift)
    d_moved, parts = local_grads(moved, moved_grad, row_base, col_base, height, width, WIN, params)
    back = shift_out(d_moved, shift)
    d_tokens = (cotangent.astype(jnp.float32) + back.astype(jnp.float32)).astype(jnp.bfloat16)
    d_wqkv, d_wproj, d_table, d_scale, d_gain = parts
    half_qkv, half_proj = (
        lax.psum_scatter(d_wqkv.astype(jnp.bfloat16), "ba", scatter_dimension=1, tiled=True).astype(jnp.float32),
        lax.psum_scatter(d_wproj.astype(jnp.bfloat16), "ba", scatter_dimension=1, tiled=True).astype(jnp.float32),
    )
    half_qkv, half_proj = lax.psum((half_qkv, half_proj), ("ha", "wa"))
    d_table, d_scale, d_gain = lax.psum((d_table, d_scale, d_gain), ("ha", "wa", "ba"))
    return (d_tokens, half_qkv, half_proj, d_table, d_scale, d_gain)


def solution(mesh):
    return jax.shard_map(
        shards,
        mesh=mesh,
        in_specs=(P("ba", "ha", "wa", None), P("ba", "ha", "wa", None), P(), P(), P(), P(), P()),
        out_specs=(P("ba", "ha", "wa", None), P(None, "ba"), P(None, "ba"), P(), P(), P()),
        check_vma=False,
    )
```

```python
import math

import functools

import jax
import jax.numpy as jnp
import numpy as np
from jax import lax
from jax.experimental import pallas as pl
from jax.experimental.pallas import tpu as pltpu
from jax.sharding import PartitionSpec as P

WIN = 8


EPS_NORM = 1e-05
MASK_FILL = -100.0
SCALE_CAP = math.log(100.0)
BIAS_RANGE = 16.0


def from_behind(block, axis, distance):
    devices = range(lax.axis_size(axis))
    route = [((i - distance) % len(devices), i) for i in devices]
    return lax.ppermute(block, axis, route)


def to_windows(block, window):
    images, height, width, depth = block.shape
    tiles = block.reshape(images, height // window, window, width // window, window, depth)
    tiles = tiles.transpose(0, 1, 3, 2, 4, 5)
    return tiles.reshape(images, height // window * (width // window), window * window, depth)


def from_windows(tiles, images, height, width, window):
    depth = tiles.shape[-1]
    grid = tiles.reshape(images, height // window, width // window, window, window, depth)
    return grid.transpose(0, 1, 3, 2, 4, 5).reshape(images, height, width, depth)


def region_of(coords, extent, window):
    return (coords >= extent - window).astype(jnp.int32) + (coords >= extent - window // 2).astype(
        jnp.int32
    )

GROUP = 4
FWD = 2
BWD = 4
LOG2E = math.log2(math.e)
VMEM_LIMIT = 40 * 2**20
FINISH_LIMIT = 4 * 2**20
MESH = pl.DeviceIdType.MESH
VMEM = pl.BlockSpec(memory_space=pltpu.VMEM)
NN = (((1,), (0,)), ((), ()))
NT = (((1,), (1,)), ((), ()))
TN = (((0,), (0,)), ((), ()))


def mxu(left, right, dims):
    return lax.dot_general(left, right, dims, preferred_element_type=jnp.float32)


def split(value):
    high = value.astype(jnp.bfloat16)
    return high, (value - high.astype(jnp.float32)).astype(jnp.bfloat16)


def mxu_fine(left, right, dims):
    high, low = split(left)
    return mxu(high, right, dims) + mxu(low, right, dims)


def same_block(rows, cols, row_size, col_size):
    row = lax.broadcasted_iota(jnp.int32, (rows, cols), 0) // row_size
    col = lax.broadcasted_iota(jnp.int32, (rows, cols), 1) // col_size
    return (row == col).astype(jnp.bfloat16)


def tile_heads(value, width):
    lane = lax.broadcasted_iota(jnp.int32, (1, value.shape[1]), 1) % (GROUP * width) // width
    rows = []
    for head in range(GROUP):
        rows.append(value * (lane == head).astype(jnp.bfloat16))
    return jnp.concatenate(rows, 0)


def gather_heads(value, width, length):
    lane = lax.broadcasted_iota(jnp.int32, (length, value.shape[1]), 1) // width
    total = value[:length]
    for head in range(1, GROUP):
        total = jnp.where(lane == head, value[head * length : (head + 1) * length], total)
    return total


def local_kernel(
    grid_cols, height, width, window,
    flat_ref, grad_ref, w_qkv_ref, w_proj_ref, bias_ref, scale_ref, gain_ref,
    d_flat_ref, d_wqkv_ref, d_wproj_ref, d_bias_ref, d_cos_ref, d_gain_ref,
    qkv_ref, att_ref, d_att_ref, d_qkv_ref, probs_ref, kinv_ref, qrow_ref, masked_ref, raw_q_ref, raw_k_ref,
    norm_ref,
):
    tokens, depth = flat_ref.shape
    f32, b16 = jnp.float32, jnp.bfloat16
    length = window * window
    count = tokens // length
    groups = bias_ref.shape[0]
    lanes = depth // groups
    heads = groups * GROUP
    head_dim = lanes // GROUP
    wide = GROUP * length
    row_base = lax.axis_index("ha") * (count // grid_cols * window)
    col_base = lax.axis_index("wa") * (grid_cols * window)

    qkv_ref[...] = mxu(flat_ref[...], w_qkv_ref[...], NN).astype(b16)
    lane_ones = same_block(lanes, wide, head_dim, length)
    lane_lane = same_block(lanes, lanes, head_dim, head_dim)

    head_rows = scale_ref.shape[0]
    pick = same_block(head_rows, depth, 1, head_dim)
    high, low = split(jnp.square(qkv_ref[:, :depth].astype(f32)))
    q_sums = mxu(pick, high, NT) + mxu(pick, low, NT)
    q_rows = lax.rsqrt(q_sums + 1.0) * scale_ref[:, :1]
    half = lax.broadcasted_iota(jnp.int32, (1, 2 * length), 1) < length
    for j in range(count // 2):
        base = q_rows[:, j * 2 * length : (j + 1) * 2 * length]
        turned = pltpu.roll(base, length, 1)
        for g in range(groups):
            for p in range(GROUP // 2):
                one, two = g * GROUP + 2 * p, g * GROUP + 2 * p + 1
                place = slice(p * 2 * length, (p + 1) * 2 * length)
                qrow_ref[2 * j, g, :, place] = jnp.where(half, base[one : one + 1], turned[two : two + 1])
                qrow_ref[2 * j + 1, g, :, place] = jnp.where(half, turned[one : one + 1], base[two : two + 1])
    for g in range(groups):
        query = qkv_ref[:, g * lanes : (g + 1) * lanes].astype(f32)
        key = qkv_ref[:, depth + g * lanes : depth + (g + 1) * lanes].astype(f32)
        high, low = split(jnp.square(key))
        kinv_ref[g] = lax.rsqrt(mxu(high, lane_ones, NN) + mxu(low, lane_ones, NN) + 1.0)
        norm_ref[1, g] = 1.0 / (mxu(high, lane_lane, NN) + mxu(low, lane_lane, NN) + 1.0)
        high, low = split(jnp.square(query))
        norm_ref[0, g] = 1.0 / (mxu(high, lane_lane, NN) + mxu(low, lane_lane, NN) + 1.0)

    mine = lax.broadcasted_iota(jnp.int32, (length, wide), 0)
    other = lax.broadcasted_iota(jnp.int32, (length, wide), 1) % length
    cut = window // 2
    row_off = (mine // window // cut) != (other // window // cut)
    col_off = (mine % window // cut) != (other % window // cut)
    for g in range(groups):
        bias = bias_ref[g] * LOG2E
        masked_ref[0, g] = bias
        masked_ref[1, g] = jnp.where(col_off, bias + MASK_FILL * LOG2E, bias)
        masked_ref[2, g] = jnp.where(row_off, bias + MASK_FILL * LOG2E, bias)
        masked_ref[3, g] = jnp.where(row_off | col_off, bias + MASK_FILL * LOG2E, bias)

    def load(ref, w, g, part):
        return ref[
            pl.ds(pl.multiple_of(w * length, length), length),
            part * depth + g * lanes : part * depth + (g + 1) * lanes,
        ]

    def forward(step, carry):
        units = [(step * FWD + k, g) for k in range(FWD) for g in range(groups)]
        scores = []
        for w, g in units:
            query, key = load(qkv_ref, w, g, 0), load(qkv_ref, w, g, 1)
            raw = mxu(key, tile_heads(query, head_dim), NT)
            last_row = (row_base + w // grid_cols * window) // (height - window)
            last_col = (col_base + w % grid_cols * window) // (width - window)
            kinv = kinv_ref[g, pl.ds(pl.multiple_of(w * length, length), length), :]
            scores.append(raw * kinv * (qrow_ref[w, g] * LOG2E) + masked_ref[last_row * 2 + last_col, g])
        for (w, g), score in zip(units, scores):
            expo = jnp.exp2(score - jnp.max(score, 0, keepdims=True))
            probs = expo * (1.0 / jnp.sum(expo, 0, keepdims=True))
            probs_ref[w, g] = probs
            att = gather_heads(mxu(probs.astype(b16), load(qkv_ref, w, g, 2), TN), head_dim, length)
            att_ref[
                pl.ds(pl.multiple_of(w * length, length), length), g * lanes : (g + 1) * lanes
            ] = att.astype(b16)
        return carry

    lax.fori_loop(0, count // FWD, forward, 0)

    proj = mxu(att_ref[...], w_proj_ref[...], NN)
    centre = proj - jnp.mean(proj, -1, keepdims=True)
    inv_std = lax.rsqrt(jnp.mean(centre * centre, -1, keepdims=True) + EPS_NORM)
    normed = centre * inv_std
    upstream = grad_ref[...].astype(f32)
    d_gain_ref[...] = jnp.sum(upstream * normed, 0, keepdims=True)
    scaled = upstream * gain_ref[...]
    d_proj = inv_std * (
        scaled
        - jnp.mean(scaled, -1, keepdims=True)
        - normed * jnp.mean(scaled * normed, -1, keepdims=True)
    )
    d_proj = d_proj.astype(b16)
    d_wproj_ref[...] = mxu(att_ref[...], d_proj, TN)
    d_att_ref[...] = mxu(d_proj, w_proj_ref[...], NT).astype(b16)
    d_bias_ref[...] = jnp.zeros_like(d_bias_ref)

    for g in range(groups):

        def backward(step, carry):
            units = [step * BWD + k for k in range(BWD)]
            grads = []
            for w in units:
                d_tall = tile_heads(load(d_att_ref, w, g, 0), head_dim)
                d_probs = mxu(load(qkv_ref, w, g, 2), d_tall, NT)
                d_value = mxu(probs_ref[w, g].astype(b16), d_tall, NN)
                d_qkv_ref[
                    pl.ds(pl.multiple_of(w * length, length), length),
                    2 * depth + g * lanes : 2 * depth + (g + 1) * lanes,
                ] = d_value.astype(b16)
                grads.append(d_probs)
            total = d_bias_ref[g]
            for w, d_probs in zip(units, grads):
                rows = pl.ds(pl.multiple_of(w * length, length), length)
                probs = probs_ref[w, g]
                d_scores = probs * (d_probs - jnp.sum(d_probs * probs, 0, keepdims=True))
                total = total + d_scores
                high, low = split(d_scores * kinv_ref[g, rows, :] * qrow_ref[w, g])
                both = jnp.concatenate([high, low], 0)
                query, key = load(qkv_ref, w, g, 0), load(qkv_ref, w, g, 1)
                pair = mxu(both, tile_heads(query, head_dim), NN)
                raw_k_ref[rows, :] = pair[:length] + pair[length:]
                tall = mxu(both, jnp.concatenate([key, key], 0), TN)
                raw_q_ref[rows, :] = gather_heads(tall, head_dim, length)
            d_bias_ref[g] = total
            return carry

        lax.fori_loop(0, count // BWD, backward, 0)
        for part, ref in enumerate((raw_q_ref, raw_k_ref)):
            place = slice(part * depth + g * lanes, part * depth + (g + 1) * lanes)
            value, grad = qkv_ref[:, place].astype(f32), ref[...]
            along = value * grad
            if part == 0:
                d_cos_ref[g] = jnp.sum(along, 0, keepdims=True)
            d_qkv_ref[:, place] = (
                grad - value * norm_ref[part, g] * mxu_fine(along, lane_lane, NN)
            ).astype(b16)
    d_wqkv_ref[...] = mxu(flat_ref[...], d_qkv_ref[...], TN)
    d_flat_ref[...] = mxu(d_qkv_ref[...], w_qkv_ref[...], NT).astype(b16)


def offset_onehot(window):
    places = np.arange(window * window)
    row_of, col_of = places // window, places % window
    offset = (row_of[:, None] - row_of[None, :] + window - 1) * (2 * window - 1) + (
        col_of[:, None] - col_of[None, :] + window - 1
    )
    return jnp.asarray(offset.reshape(-1), jnp.int32)


def three_parts(value):
    high = lax.reduce_precision(value, 8, 7)
    middle = lax.reduce_precision(value - high, 8, 7)
    return jnp.concatenate([high, middle, value - high - middle], 0).astype(jnp.bfloat16)


def local_grads(block, grad_block, row_base, col_base, height, width, window, params):
    w_qkv, w_proj, table_logits, logit_scale, gain = params
    images, rows, cols, depth = block.shape
    heads = logit_scale.shape[0]
    length = window * window
    groups = heads // GROUP
    wide = GROUP * length
    flat = to_windows(block, window).reshape(-1, depth)
    grad_flat = to_windows(grad_block, window).reshape(-1, depth)
    tokens = flat.shape[0]
    count = tokens // length
    scale = jnp.exp(jnp.minimum(logit_scale, SCALE_CAP))
    scale_rows = jnp.pad(scale, (0, -heads % 16)).reshape(-1, 1) * jnp.ones((1, 128), jnp.float32)
    sigma = jax.nn.sigmoid(table_logits)
    entries = table_logits.shape[1]
    hot = offset_onehot(window)[None, :] == jnp.arange(entries, dtype=jnp.int32)[:, None]
    hot = hot.astype(jnp.bfloat16)
    parts = jnp.dot(three_parts(sigma * BIAS_RANGE), hot, preferred_element_type=jnp.float32)
    rel_bias = jnp.sum(parts.reshape(3, heads, -1), 0).reshape(groups, GROUP, length, length)
    rel_bias = rel_bias.transpose(0, 3, 1, 2).reshape(groups, length, wide)
    f32, b16 = jnp.float32, jnp.bfloat16
    d_flat, d_wqkv, d_wproj, d_bias, d_cos, d_gain = pl.pallas_call(
        functools.partial(local_kernel, cols // window, height, width, window),
        out_shape=[
            jax.ShapeDtypeStruct((tokens, depth), b16),
            jax.ShapeDtypeStruct((depth, 3 * depth), f32),
            jax.ShapeDtypeStruct((depth, depth), f32),
            jax.ShapeDtypeStruct((groups, length, wide), f32),
            jax.ShapeDtypeStruct((groups, 1, depth // groups), f32),
            jax.ShapeDtypeStruct((1, depth), f32),
        ],
        in_specs=[VMEM] * 7,
        out_specs=[VMEM] * 6,
        scratch_shapes=[
            pltpu.VMEM((tokens, 3 * depth), b16),
            pltpu.VMEM((tokens, depth), b16),
            pltpu.VMEM((tokens, depth), b16),
            pltpu.VMEM((tokens, 3 * depth), b16),
            pltpu.VMEM((count, groups, length, wide), f32),
            pltpu.VMEM((groups, tokens, wide), f32),
            pltpu.VMEM((count, groups, 1, wide), f32),
            pltpu.VMEM((4, groups, length, wide), f32),
            pltpu.VMEM((tokens, depth // groups), f32),
            pltpu.VMEM((tokens, depth // groups), f32),
            pltpu.VMEM((2, groups, tokens, depth // groups), f32),
        ],
        compiler_params=pltpu.CompilerParams(vmem_limit_bytes=48 * 2**20),
        cost_estimate=pl.CostEstimate(
            flops=4_000_000_000, bytes_accessed=8_000_000, transcendentals=400_000
        ),
        name="local_grads",
    )(flat, grad_flat, w_qkv, w_proj, rel_bias, scale_rows, gain.reshape(1, depth))
    heads_bias = d_bias.reshape(groups, length, GROUP, length).transpose(0, 2, 3, 1)
    heads_bias = heads_bias.reshape(heads, length * length)
    sums = lax.dot_general(three_parts(heads_bias), hot, NT, preferred_element_type=jnp.float32)
    d_table = jnp.sum(sums.reshape(3, heads, entries), 0) * (BIAS_RANGE * sigma * (1.0 - sigma))
    live = (logit_scale < SCALE_CAP).astype(jnp.float32)
    d_scale = jnp.sum(d_cos.reshape(heads, depth // heads), 1) * live
    d_block = from_windows(d_flat.reshape(images, count, length, depth), images, rows, cols, window)
    return (d_block, (d_wqkv, d_wproj, d_table, d_scale, d_gain.reshape(depth)))


def half_turn(value, axis):
    return pltpu.roll(value, value.shape[axis] // 2, axis)


def exp_fine(value):
    whole = jnp.floor(value * LOG2E + 0.5)
    rest = value - whole * 0.693359375 + whole * 2.12194440e-4
    total = jnp.ones_like(rest)
    for k in range(8, 0, -1):
        total = 1.0 + total * rest * (1.0 / k)
    return total * jnp.exp2(whole)


def inverse(value):
    guess = 1.0 / value
    return guess * (2.0 - value * guess)


def place_of(index, window):
    return index // window * (2 * window - 1) + index % window


def expand_bias(table, length, window, groups, out_ref):
    span = table.shape[1]
    f32, b16 = jnp.float32, jnp.bfloat16
    heads = groups * GROUP
    base = jnp.concatenate([jnp.broadcast_to(table[h : h + 1], (window, span)) for h in range(heads)], 0)
    sub = lax.broadcasted_iota(jnp.int32, base.shape, 0) % window
    bit = 1
    while bit < window:
        base = jnp.where(sub // bit % 2 == 1, pltpu.roll(base, bit, 1), base)
        bit *= 2
    top = place_of(length - 1, window)
    turned = [
        pltpu.roll(base, (span - top + (2 * window - 1) * r) % span, 1)[:, : span // 2] for r in range(window)
    ]
    wide = GROUP * length
    row = lax.broadcasted_iota(jnp.int32, (span, wide), 0) % (span // 2)
    col = lax.broadcasted_iota(jnp.int32, (span, wide), 1)
    hit = row == place_of(col % length, window)
    for g in range(groups):
        total = jnp.zeros((length, wide), f32)
        for k in range(GROUP):
            h = g * GROUP + k
            block = jnp.concatenate([t[h * window : (h + 1) * window] for t in turned], 0)
            pair = jnp.concatenate(split(block), 1)
            total = total + mxu(pair, (hit & (col // length == k)).astype(b16), NN)
        out_ref[0, g] = total


def fold_bias(grads, length, window, span):
    f32, b16 = jnp.float32, jnp.bfloat16
    wide = GROUP * length
    row = lax.broadcasted_iota(jnp.int32, (wide, span // 2), 0)
    col = lax.broadcasted_iota(jnp.int32, (wide, span // 2), 1)
    hit = col == place_of(row % length, window)
    both = jnp.concatenate([half for grad in grads for half in split(grad)], 0)
    by_head = [None] * (len(grads) * GROUP)
    for k in range(GROUP):
        pairs = mxu(both, (hit & (row // length == k)).astype(b16), NN)
        for g in range(len(grads)):
            pair = pairs[2 * g * length : (2 * g + 2) * length]
            block = pair[:length] + pair[length:]
            by_head[g * GROUP + k] = jnp.concatenate([block, jnp.zeros_like(block)], 1)
    parts = [
        jnp.concatenate([block[r * window : (r + 1) * window] for block in by_head], 0) for r in range(window)
    ]
    step = 2 * window - 1
    while len(parts) > 1:
        parts = [pltpu.roll(parts[i], step, 1) + parts[i + 1] for i in range(0, len(parts), 2)]
        step *= 2
    total = parts[0]
    sub = window - 1 - lax.broadcasted_iota(jnp.int32, total.shape, 0) % window
    bit = 1
    while bit < window:
        total = jnp.where(sub // bit % 2 == 1, pltpu.roll(total, bit, 1), total)
        bit *= 2
    return [jnp.sum(total[k * window : (k + 1) * window], 0, keepdims=True) for k in range(len(by_head))]


def whole_kernel(
    shape, height, width, window,
    tokens_ref, cot_ref, w_qkv_hbm, w_proj_hbm, table_hbm, gain_hbm, scale_ref,
    d_tok_ref, grads_out, table_out, scale_out, gain_out,
    tok, cot, w_qkv_ref, w_proj_ref, table_in, gain_ref, table_ref, local_sems,
    col_send, row_get, col_get, diag_get, halo_sems,
    flat_ref, grad_ref, d_flat_ref, d_proj_ref,
    qkv_ref, att_ref, d_att_ref, d_qkv_ref, probs_ref, kinv_ref, qrow_ref, masked_ref, raw_q_ref, raw_k_ref,
    norm_ref, d_bias_ref, p_mid, k_first, product_ref,
    row_back, col_back, row_back_get, col_back_get, diag_back_get, back_sems,
    small, small_core, small_a, small_image, small_b, small_side, small_c, small_near, small_total, tiny_sems,
    *chunk_refs,
):
    size_h, size_w = shape
    chips = size_h // 2
    peers = chips * size_w
    ha, wa, ba = lax.axis_index("ha"), lax.axis_index("wa"), lax.axis_index("ba")
    core = ha % 2
    me = wa * chips + ha // 2
    partner = (ha + 1 - 2 * core, wa, ba)
    image, side, corner = (ha, wa, 1 - ba), (ha, 1 - wa, ba), (ha, 1 - wa, 1 - ba)
    above, below = lax.rem(ha + size_h - 1, size_h), lax.rem(ha + 1, size_h)
    left, right = lax.rem(wa + size_w - 1, size_w), lax.rem(wa + 1, size_w)
    f32, b16 = jnp.float32, jnp.bfloat16

    def peer(step):
        other = lax.rem(me + step, peers)
        return other, (other % chips * 2 + core, other // chips, ba)

    loads = []
    for k, (src, dst) in enumerate(
        (
            (tokens_ref.at[0], tok), (cot_ref.at[0], cot), (w_qkv_hbm, w_qkv_ref), (w_proj_hbm, w_proj_ref),
            (table_hbm, table_in), (gain_hbm, gain_ref),
        )
    ):
        copy = pltpu.make_async_copy(src, dst, local_sems.at[k])
        copy.start()
        loads.append(copy)
    targets = [
        (above, wa, ba), (below, wa, ba), (ha, left, ba), (ha, right, ba), (above, left, ba), (below, right, ba),
        partner, image, corner,
    ] + [peer(step)[1] for step in range(1, peers)]
    barrier = pltpu.get_barrier_semaphore()
    for device in targets:
        pl.semaphore_signal(barrier, inc=1, device_id=device, device_id_type=MESH)

    def start(src, dst, sems, device):
        copy = pltpu.make_async_remote_copy(
            src_ref=src, dst_ref=dst, send_sem=sems.at[0], recv_sem=sems.at[1],
            device_id=device, device_id_type=MESH,
        )
        copy.start()
        return copy

    def all_of(src, dst, sems, device):
        return pltpu.make_async_remote_copy(
            src_ref=src, dst_ref=dst, send_sem=sems.at[0], recv_sem=sems.at[1],
            device_id=device, device_id_type=MESH,
        )

    rows, cols, depth = tok.shape
    cut = window // 2
    length = window * window
    across = cols // window
    count = rows // window * across
    tokens = count * length
    groups = qrow_ref.shape[1]
    lanes = depth // groups
    head_dim = lanes // GROUP
    wide = GROUP * length
    low_sub = lax.broadcasted_iota(jnp.int32, (window, depth), 0) < cut

    def pack_columns(a, ref):
        loads[a].wait()
        for j in range(rows // 2):
            first = ref[2 * j, :window, :].astype(f32)
            second = ref[2 * j + 1, :window, :].astype(f32)
            col_send[a, j] = jnp.where(low_sub, first, half_turn(second, 0)).astype(b16)

    halos = {}

    def send_halo(a, ref):
        halos[a, 0] = start(col_send.at[a], col_get.at[a], halo_sems.at[a, 1], (ha, left, ba))
        halos[a, 1] = start(ref.at[pl.ds(0, cut)], row_get.at[a], halo_sems.at[a, 0], (above, wa, ba))
        halos[a, 2] = start(
            col_send.at[a, pl.ds(0, cut // 2)], diag_get.at[a], halo_sems.at[a, 2], (above, left, ba)
        )

    pack_columns(0, tok)
    pl.semaphore_wait(barrier, len(targets))
    send_halo(0, tok)
    pack_columns(1, cot)
    send_halo(1, cot)

    loads[4].wait()
    loads[5].wait()
    heads = groups * GROUP
    entries = table_in.shape[1]
    table_ref[...] = jnp.zeros_like(table_ref)
    table_ref[:heads, :entries] = table_in[...]
    sigma = inverse(1.0 + exp_fine(-table_ref[...]))
    head_rows, span = table_ref.shape
    spot = lax.broadcasted_iota(jnp.int32, (head_rows, 128), 0)
    logits = jnp.zeros((head_rows, 128), f32)
    for h in range(heads):
        logits = jnp.where(spot == h, scale_ref[h], logits)
    scale = exp_fine(jnp.minimum(logits, SCALE_CAP))
    expand_bias(sigma * (BIAS_RANGE * LOG2E), length, window, groups, masked_ref)
    mine = lax.broadcasted_iota(jnp.int32, (length, wide), 0)
    other = lax.broadcasted_iota(jnp.int32, (length, wide), 1) % length
    row_off = (mine // window // cut) != (other // window // cut)
    col_off = (mine % window // cut) != (other % window // cut)
    for g in range(groups):
        bias = masked_ref[0, g]
        masked_ref[1, g] = jnp.where(col_off, bias + MASK_FILL * LOG2E, bias)
        masked_ref[2, g] = jnp.where(row_off, bias + MASK_FILL * LOG2E, bias)
        masked_ref[3, g] = jnp.where(row_off | col_off, bias + MASK_FILL * LOG2E, bias)
    small[...] = jnp.zeros_like(small)

    def gather_rows(a, ref, out_ref, from_row, to_row):
        def shifted(i):
            if i + cut < rows:
                row, edge = ref[i + cut], col_get[a, (i + cut) // 2]
            else:
                row, edge = row_get[a, i + cut - rows], diag_get[a, (i + cut - rows) // 2]
            row, edge = row.astype(f32), edge.astype(f32)
            turned = [half_turn(row[k * window : (k + 1) * window], 0) for k in range(across)]
            turned.append(half_turn(edge, 0) if i % 2 == 0 else edge)
            return [jnp.where(low_sub, turned[k], turned[k + 1]) for k in range(across)]

        for i in range(from_row, to_row, 2):
            one, two = shifted(i), shifted(i + 1)
            for k in range(across):
                begin = (i // window * across + k) * length + i % window * window
                out_ref[begin : begin + 2 * window] = jnp.concatenate([one[k], two[k]], 0).astype(b16)

    row_base, col_base = ha * rows, wa * cols
    lane_ones = same_block(lanes, wide, head_dim, length)
    lane_lane = same_block(lanes, lanes, head_dim, head_dim)
    pick = same_block(head_rows, depth, 1, head_dim)
    half = lax.broadcasted_iota(jnp.int32, (1, 2 * length), 1) < length

    def project(begin_window, end_window):
        part_rows = slice(begin_window * length, end_window * length)
        qkv_ref[part_rows] = mxu(flat_ref[part_rows], w_qkv_ref[...], NN).astype(b16)
        high, low = split(jnp.square(qkv_ref[part_rows, :depth].astype(f32)))
        q_sums = mxu(pick, high, NT) + mxu(pick, low, NT)
        q_rows = lax.rsqrt(q_sums + 1.0) * scale[:, :1]
        for j in range(begin_window // 2, end_window // 2):
            shifted_j = 2 * j - begin_window
            base = q_rows[:, shifted_j * length : (shifted_j + 2) * length]
            turned = half_turn(base, 1)
            for g in range(groups):
                for p in range(GROUP // 2):
                    one, two = g * GROUP + 2 * p, g * GROUP + 2 * p + 1
                    place = slice(p * 2 * length, (p + 1) * 2 * length)
                    qrow_ref[2 * j, g, :, place] = jnp.where(half, base[one : one + 1], turned[two : two + 1])
                    qrow_ref[2 * j + 1, g, :, place] = jnp.where(half, turned[one : one + 1], base[two : two + 1])
        for g in range(groups):
            key = qkv_ref[part_rows, depth + g * lanes : depth + (g + 1) * lanes].astype(f32)
            high, low = split(jnp.square(key))
            kinv_ref[g, part_rows] = lax.rsqrt(mxu(high, lane_ones, NN) + mxu(low, lane_ones, NN) + 1.0)

    def norms(begin_window, end_window):
        part_rows = slice(begin_window * length, end_window * length)
        for g in range(groups):
            for part in range(2):
                place = slice(part * depth + g * lanes, part * depth + (g + 1) * lanes)
                high, low = split(jnp.square(qkv_ref[part_rows, place].astype(f32)))
                norm_ref[part, g, part_rows] = 1.0 / (
                    mxu(high, lane_lane, NN) + mxu(low, lane_lane, NN) + 1.0
                )

    def load(ref, w, g, part):
        return ref[
            pl.ds(pl.multiple_of(w * length, length), length),
            part * depth + g * lanes : part * depth + (g + 1) * lanes,
        ]

    def forward(step, carry):
        units = [(step * FWD + k, g) for k in range(FWD) for g in range(groups)]
        scores = []
        for w, g in units:
            query, key = load(qkv_ref, w, g, 0), load(qkv_ref, w, g, 1)
            raw = mxu(key, tile_heads(query, head_dim), NT)
            last_row = (row_base + w // across * window) // (height - window)
            last_col = (col_base + w % across * window) // (width - window)
            kinv = kinv_ref[g, pl.ds(pl.multiple_of(w * length, length), length), :]
            scores.append(raw * kinv * (qrow_ref[w, g] * LOG2E) + masked_ref[last_row * 2 + last_col, g])
        for (w, g), score in zip(units, scores):
            expo = jnp.exp2(score - jnp.max(score, 0, keepdims=True))
            probs = expo * (1.0 / jnp.sum(expo, 0, keepdims=True))
            probs_ref[w, g] = probs
            att = gather_heads(mxu(probs.astype(b16), load(qkv_ref, w, g, 2), TN), head_dim, length)
            att_ref[
                pl.ds(pl.multiple_of(w * length, length), length), g * lanes : (g + 1) * lanes
            ] = att.astype(b16)
        return carry

    def norm_gradient(begin_window, end_window):
        part_rows = slice(begin_window * length, end_window * length)
        proj = mxu(att_ref[part_rows], w_proj_ref[...], NN)
        centre = proj - jnp.mean(proj, -1, keepdims=True)
        inv_std = lax.rsqrt(jnp.mean(centre * centre, -1, keepdims=True) + EPS_NORM)
        normed = centre * inv_std
        upstream = grad_ref[part_rows].astype(f32)
        d_gain = jnp.sum(upstream * normed, 0, keepdims=True)
        scaled = upstream * gain_ref[...].reshape(1, depth)
        d_proj = inv_std * (
            scaled
            - jnp.mean(scaled, -1, keepdims=True)
            - normed * jnp.mean(scaled * normed, -1, keepdims=True)
        )
        d_proj = d_proj.astype(b16)
        d_proj_ref[part_rows] = d_proj
        d_att_ref[part_rows] = mxu(d_proj, w_proj_ref[...], NT).astype(b16)
        return d_gain

    early = count - across
    halos[0, 0].wait()
    gather_rows(0, tok, flat_ref, 0, rows - window)
    loads[2].wait()
    project(0, early)
    lax.fori_loop(0, early // FWD, forward, 0)
    norms(0, early)
    halos[1, 0].wait()
    gather_rows(1, cot, grad_ref, 0, rows - window)
    loads[3].wait()
    d_gain = norm_gradient(0, early)
    halos[0, 1].wait()
    halos[0, 2].wait()
    gather_rows(0, tok, flat_ref, rows - window, rows)
    project(early, count)
    lax.fori_loop(early // FWD, count // FWD, forward, 0)
    halos[1, 1].wait()
    halos[1, 2].wait()
    gather_rows(1, cot, grad_ref, rows - window, rows)
    d_gain = d_gain + norm_gradient(early, count)
    small[heads : heads + 1, :] = d_gain[:, :span]
    small[heads + 1 : heads + 2, : depth - span] = d_gain[:, span:]
    per = len(chunk_refs) // 4
    chunks = [chunk_refs[c * per : (c + 1) * per] for c in range(4)]
    flying = {}

    def begin(c):
        core_send, core_mine, core_get = chunks[c][:3]
        w = core_send.shape[0] // 2
        for side_of in range(2):
            here = slice(side_of * w, (side_of + 1) * w)
            base = 2 * side_of * w
            theirs = pl.ds(pl.multiple_of(base + (1 - core) * w, 32), w)
            core_send[here] = product_ref[theirs, :].astype(b16)
        flying[c] = start(core_send, core_get, chunks[c][9], partner)
        for side_of in range(2):
            here = slice(side_of * w, (side_of + 1) * w)
            core_mine[here] = product_ref[pl.ds(pl.multiple_of(2 * side_of * w + core * w, 32), w), :]

    def cross(c):
        core_send, core_mine, core_get, plane_send, plane_get = chunks[c][:5]
        flying[c].wait()
        core_mine[...] = core_mine[...] + core_get[...].astype(f32)
        w = plane_send.shape[1]
        for k, (b, y, device) in enumerate(((1 - ba, wa, image), (ba, 1 - wa, side), (1 - ba, 1 - wa, corner))):
            place = pl.ds(pl.multiple_of((2 * b + y) * w, 32), w)
            plane_send[k] = core_mine[place, :].astype(b16)
            start(plane_send.at[k], plane_get.at[k], chunks[c][10], device)
        flying[c] = [all_of(plane_send, plane_get, chunks[c][10], image)]

    def scatter(c):
        core_mine, plane_get, near_send, near_get = chunks[c][1], chunks[c][4], chunks[c][5], chunks[c][6]
        for copy in flying[c]:
            copy.wait()
        w = plane_get.shape[1]
        total = core_mine[pl.ds(pl.multiple_of((2 * ba + wa) * w, 32), w), :]
        for k in range(3):
            total = total + plane_get[k].astype(f32)
        r = near_send.shape[1]
        for j in range(chips):
            near_send[j] = total[j * r : (j + 1) * r].astype(b16)
        for step in range(1, chips):
            far_chip = lax.rem(ha // 2 + step, chips)
            start(near_send.at[far_chip], near_get.at[step - 1], chunks[c][11], (2 * far_chip + core, wa, ba))
        flying[c] = [all_of(near_send.at[pl.ds(0, chips - 1)], near_get, chunks[c][11], partner)]

    def gather(c):
        near_send, near_get, whole = chunks[c][5:8]
        for copy in flying[c]:
            copy.wait()
        total = near_send[ha // 2].astype(f32)
        for step in range(1, chips):
            total = total + near_get[step - 1].astype(f32)
        whole[me] = total.astype(b16)
        for step in range(1, peers):
            start(whole.at[me], whole.at[me], chunks[c][12], peer(step)[1])
        several = whole.at[pl.ds(0, peers - 1)]
        flying[c] = [all_of(several, several, chunks[c][12], partner)]

    def spread_column(c):
        near_send, near_get, whole = chunks[c][5:8]
        for copy in flying[c]:
            copy.wait()
        total = near_send[ha // 2].astype(f32)
        for step in range(1, chips):
            total = total + near_get[step - 1].astype(f32)
        whole[me] = total.astype(b16)
        for step in range(1, chips):
            far_chip = lax.rem(ha // 2 + step, chips)
            start(whole.at[me], whole.at[me], chunks[c][12], (2 * far_chip + core, wa, ba))
        several = whole.at[pl.ds(0, chips - 1)]
        flying[c] = [all_of(several, several, chunks[c][12], partner)]

    def relay(c):
        whole = chunks[c][7]
        for copy in flying[c]:
            copy.wait()
        held = pl.ds(wa * chips, chips)
        flying[c] = [start(whole.at[held], whole.at[held], chunks[c][14], side)]

    def mirror(c):
        whole, core_all = chunks[c][7:9]
        for copy in flying[c]:
            copy.wait()
        flying[c] = start(whole, core_all, chunks[c][13], partner)

    def finish(c):
        put(c, chunks[c][7], core)
        flying[c].wait()
        put(c, chunks[c][8], 1 - core)

    unit = lanes // 2
    proj_at = 3 * depth // 2

    targets_of = [
        [(proj_at + k * unit, proj_at + (1 + k) * unit) for k in range(2)],
        [(k * unit, (3 + k) * unit) for k in range(2)],
        [((4 + k) * unit, (1 + k if k < 2 else 5 + k) * unit) for k in range(4)],
        [(2 * unit, 5 * unit), (3 * unit, 6 * unit), (8 * unit, 0), (proj_at + 2 * unit, proj_at)],
    ]

    def put(c, source, which):
        r = source.shape[1]
        blocks = peers * r // unit
        for k in range(blocks):
            zero, one = targets_of[c][k], targets_of[c][blocks + k]
            row = jnp.where(
                which == 0, jnp.where(ba == 0, zero[0], zero[1]), jnp.where(ba == 0, one[0], one[1])
            )
            for j in range(unit // r):
                grads_out[pl.ds(pl.multiple_of(row + j * r, 8), r), :] = source[k * (unit // r) + j].astype(f32)

    product = mxu(d_proj_ref[...], att_ref[...], TN)
    product_ref[:lanes] = product[:lanes]
    p_mid[...] = product[lanes : 2 * lanes]
    product_ref[lanes : 2 * lanes] = product[2 * lanes :]
    begin(0)

    def backward_group(g):
        def backward(step, total):
            units = [step * BWD + k for k in range(BWD)]
            grads = []
            for w in units:
                d_tall = tile_heads(load(d_att_ref, w, g, 0), head_dim)
                d_probs = mxu(load(qkv_ref, w, g, 2), d_tall, NT)
                d_value = mxu(probs_ref[w, g].astype(b16), d_tall, NN)
                d_qkv_ref[
                    pl.ds(pl.multiple_of(w * length, length), length),
                    2 * depth + g * lanes : 2 * depth + (g + 1) * lanes,
                ] = d_value.astype(b16)
                grads.append(d_probs)
            summed = d_bias_ref[g]
            for w, d_probs in zip(units, grads):
                place = pl.ds(pl.multiple_of(w * length, length), length)
                probs = probs_ref[w, g]
                d_scores = probs * (d_probs - jnp.sum(d_probs * probs, 0, keepdims=True))
                summed = summed + d_scores
                high, low = split(d_scores * kinv_ref[g, place, :] * qrow_ref[w, g])
                both = jnp.concatenate([high, low], 0)
                query, key = load(qkv_ref, w, g, 0), load(qkv_ref, w, g, 1)
                pair = mxu(both, tile_heads(query, head_dim), NN)
                raw_k_ref[place, :] = pair[:length] + pair[length:]
                tall = mxu(both, jnp.concatenate([key, key], 0), TN)
                raw_q_ref[place, :] = gather_heads(tall, head_dim, length)
            d_bias_ref[g] = summed
            return total

        d_bias_ref[g] = jnp.zeros((length, wide), f32)
        lax.fori_loop(0, count // BWD, backward, 0)
        for part, ref in enumerate((raw_q_ref, raw_k_ref)):
            place = slice(part * depth + g * lanes, part * depth + (g + 1) * lanes)
            value, grad = qkv_ref[:, place].astype(f32), ref[...]
            along = value * grad
            if part == 0:
                spot = depth - span + g * lanes
                small[
                    heads + 1 + spot // span : heads + 2 + spot // span, spot % span : spot % span + lanes
                ] = jnp.sum(along, 0, keepdims=True)
            d_qkv_ref[:, place] = (
                grad - value * norm_ref[part, g] * mxu_fine(along, lane_lane, NN)
            ).astype(b16)

    def dense(g):
        joined = jnp.concatenate(
            [d_qkv_ref[:, part * depth + g * lanes : part * depth + (g + 1) * lanes] for part in range(3)], 1
        )
        return mxu(joined, flat_ref[...], TN)

    norms(early, count)
    backward_group(0)
    product = dense(0)
    product_ref[:lanes] = product[:lanes]
    product_ref[lanes : 2 * lanes] = product[2 * lanes :]
    k_first[...] = product[lanes : 2 * lanes]
    begin(1)
    cross(0)
    backward_group(2)
    cross(1)
    product = dense(2)
    product_ref[:lanes] = product[:lanes]
    product_ref[lanes : 2 * lanes] = k_first[...]
    product_ref[2 * lanes : 4 * lanes] = product[lanes:]
    begin(2)
    scatter(0)
    backward_group(1)
    cross(2)
    product = dense(1)
    product_ref[:lanes] = product[:lanes]
    product_ref[lanes : lanes + unit] = product[lanes : lanes + unit]
    product_ref[lanes + unit : 2 * lanes] = p_mid[:unit]
    product_ref[2 * lanes : 3 * lanes] = product[2 * lanes :]
    product_ref[3 * lanes : 3 * lanes + unit] = product[lanes + unit : 2 * lanes]
    product_ref[3 * lanes + unit : 4 * lanes] = p_mid[unit:]
    begin(3)
    scatter(1)
    d_flat_ref[...] = mxu(d_qkv_ref[...], w_qkv_ref[...], NT).astype(b16)

    def back_tiles(i):
        begin_row = i // window * across * length + i % window * window
        return [
            half_turn(d_flat_ref[begin_row + k * length : begin_row + k * length + window].astype(f32), 0)
            for k in range(across)
        ]

    for i in range(0, rows, 2):
        one, two = back_tiles(i), back_tiles(i + 1)
        col_back[i // 2] = jnp.where(low_sub, one[-1], half_turn(two[-1], 0)).astype(b16)
        if i >= rows - cut:
            row_back[i - (rows - cut)] = jnp.concatenate(one, 0).astype(b16)
            row_back[i + 1 - (rows - cut)] = jnp.concatenate(two, 0).astype(b16)
    far = (rows - cut) // 2
    back = [
        start(row_back, row_back_get, back_sems.at[0], (below, wa, ba)),
        start(col_back.at[pl.ds(0, far)], col_back_get, back_sems.at[1], (ha, right, ba)),
        start(col_back.at[pl.ds(far, cut // 2)], diag_back_get, back_sems.at[2], (below, right, ba)),
    ]
    cross(3)
    spread_column(0)
    for k, row in enumerate(fold_bias([d_bias_ref[g] for g in range(groups)], length, window, span)):
        small[k : k + 1, :] = row
    tiny = start(small, small_core, tiny_sems.at[0], partner)

    def put_row(i, turned, edge, odd):
        ahead = [half_turn(edge, 0) if odd else edge] + turned
        out = [jnp.where(low_sub, ahead[k], ahead[k + 1]) for k in range(across)]
        d_tok_ref[i] = (jnp.concatenate(out, 0) + cot[i].astype(f32)).astype(b16)

    scatter(2)
    back[1].wait()
    for i in range(rows - cut):
        put_row(i + cut, back_tiles(i), col_back_get[i // 2].astype(f32), i % 2 == 1)
    spread_column(1)
    tiny.wait()
    small_half = small_a.shape[0]
    my_rows = pl.ds(pl.multiple_of(core * small_half, 8), small_half)
    small_a[...] = small[my_rows, :] + small_core[my_rows, :]
    tiny = start(small_a, small_image, tiny_sems.at[1], image)
    relay(0)
    back[0].wait()
    back[2].wait()
    for i in range(cut):
        whole_row = row_back_get[i].astype(f32)
        turned = [whole_row[k * window : (k + 1) * window] for k in range(across)]
        put_row(i, turned, diag_back_get[i // 2].astype(f32), i % 2 == 1)
    scatter(3)
    tiny.wait()
    small_b[...] = small_a[...] + small_image[...]
    tiny = start(small_b, small_side, tiny_sems.at[2], side)
    spread_column(2)
    mirror(0)
    relay(1)
    tiny.wait()
    small_c[...] = small_b[...] + small_side[...]
    for step in range(1, chips):
        far_chip = lax.rem(ha // 2 + step, chips)
        start(small_c, small_near.at[step - 1], tiny_sems.at[3], (2 * far_chip + core, wa, ba))
    tinies = [all_of(small_near, small_near, tiny_sems.at[3], partner)]
    finish(0)
    gather(3)
    relay(2)
    mirror(1)
    for copy in tinies:
        copy.wait()
    total = small_c[...]
    for step in range(1, chips):
        total = total + small_near[step - 1]
    small_total[my_rows, :] = total
    tiny = start(small_total.at[my_rows], small_total.at[my_rows], tiny_sems.at[4], partner)
    finish(1)
    mirror(2)
    tiny.wait()
    total = small_total[...]
    table_out[...] = (total[: head_rows] * (BIAS_RANGE * sigma * (1.0 - sigma)))[:heads, :entries]
    gain_row = jnp.concatenate([total[heads : heads + 1, :], total[heads + 1 : heads + 2, : depth - span]], 1)
    gain_out[...] = gain_row.reshape(depth)
    sums = jnp.concatenate([total[heads + 1 : heads + 2, depth - span :], total[heads + 2 : heads + 3, :]], 1)
    sums = mxu_fine(jnp.broadcast_to(sums, (8, depth)), same_block(depth, 128, head_dim, 1), NN)[:1]
    at = lax.broadcasted_iota(jnp.int32, (1, 128), 1)
    logits = jnp.zeros((1, 128), f32)
    for h in range(heads):
        logits = jnp.where(at == h, scale_ref[h], logits)
    scale_out[...] = jnp.where(logits < SCALE_CAP, sums, 0.0).reshape(128)[:heads]
    mirror(3)
    finish(2)
    finish(3)


def finish_kernel(tok_ref, grads_ref, table_ref, scale_ref, gain_ref, tok, wq, wp, table, scale, gain, sems):
    cut = wq.shape[0]
    pairs = (
        (grads_ref.at[pl.ds(0, cut)], wq), (grads_ref.at[pl.ds(cut, wp.shape[0])], wp), (tok_ref, tok),
        (table_ref, table), (scale_ref, scale), (gain_ref, gain),
    )
    copies = [pltpu.make_async_copy(src, dst, sems.at[k]) for k, (src, dst) in enumerate(pairs)]
    for copy in copies:
        copy.start()
    for copy in copies:
        copy.wait()


def whole_grads(tokens, cotangent, w_qkv, w_proj, table_logits, logit_scale, gain, height, width, window):
    size_h, size_w = lax.axis_size("ha"), lax.axis_size("wa")
    peers = size_h // 2 * size_w
    f32, b16 = jnp.float32, jnp.bfloat16
    images, rows, cols, depth = tokens.shape
    heads = logit_scale.shape[0]
    entries = table_logits.shape[1]
    groups = heads // GROUP
    lanes = depth // groups
    length = window * window
    wide = GROUP * length
    total = rows * cols
    count = total // length
    cut = window // 2
    span = 256
    head_rows = -(-heads // 16) * 16
    half = depth // 2
    chips = size_h // 2
    dma, vmem = pltpu.SemaphoreType.DMA, pltpu.VMEM
    chunk_scratch = []
    for w in (lanes // 2, lanes // 2, lanes, lanes):
        r = w // peers
        chunk_scratch += [
            vmem((2 * w, depth), b16), vmem((2 * w, depth), f32), vmem((2 * w, depth), b16),
            vmem((3, w // 2, depth), b16), vmem((3, w // 2, depth), b16),
            vmem((chips, r, depth), b16), vmem((chips - 1, r, depth), b16),
            vmem((peers, r, depth), b16), vmem((peers, r, depth), b16),
            dma((2,)), dma((2,)), dma((2,)), dma((2,)), dma((2,)), dma((2,)),
        ]
    small, part = (16, span), (8, span)
    anywhere = pl.BlockSpec(memory_space=pltpu.HBM)
    pinned = [
        pltpu.with_memory_space_constraint(x, pltpu.HBM)
        for x in (tokens, cotangent, w_qkv, w_proj, table_logits, gain)
    ]
    outs = pl.pallas_call(
        functools.partial(whole_kernel, (size_h, size_w), height, width, window),
        out_shape=[
            jax.ShapeDtypeStruct((rows, cols, depth), b16),
            jax.ShapeDtypeStruct((2 * depth, depth), f32),
            jax.ShapeDtypeStruct((heads, entries), f32),
            jax.ShapeDtypeStruct((heads,), f32),
            jax.ShapeDtypeStruct((depth,), f32),
        ],
        in_specs=[anywhere] * 6 + [pl.BlockSpec(memory_space=pltpu.SMEM)],
        out_specs=[VMEM] * 5,
        scratch_shapes=[
            vmem((rows, cols, depth), b16), vmem((rows, cols, depth), b16),
            vmem((depth, 3 * depth), b16), vmem((depth, depth), b16),
            vmem((heads, entries), f32), vmem((depth,), f32), vmem((head_rows, span), f32), dma((6,)),
            vmem((2, rows // 2, window, depth), b16), vmem((2, cut, cols, depth), b16),
            vmem((2, rows // 2, window, depth), b16), vmem((2, cut // 2, window, depth), b16), dma((2, 3, 2)),
            vmem((total, depth), b16), vmem((total, depth), b16), vmem((total, depth), b16), vmem((total, depth), b16),
            vmem((total, 3 * depth), b16), vmem((total, depth), b16), vmem((total, depth), b16),
            vmem((total, 3 * depth), b16), vmem((count, groups, length, wide), f32), vmem((groups, total, wide), f32),
            vmem((count, groups, 1, wide), f32), vmem((4, groups, length, wide), f32),
            vmem((total, lanes), f32), vmem((total, lanes), f32), vmem((2, groups, total, lanes), f32),
            vmem((groups, length, wide), f32), vmem((lanes, depth), f32), vmem((lanes, depth), f32),
            vmem((4 * lanes, depth), f32),
            vmem((cut, cols, depth), b16), vmem((rows // 2, window, depth), b16), vmem((cut, cols, depth), b16),
            vmem(((rows - cut) // 2, window, depth), b16), vmem((cut // 2, window, depth), b16), dma((3, 2)),
            vmem(small, f32), vmem(small, f32), vmem(part, f32), vmem(part, f32), vmem(part, f32), vmem(part, f32),
            vmem(part, f32), vmem((chips - 1, *part), f32), vmem(small, f32), dma((5, 2)),
            *chunk_scratch,
        ],
        compiler_params=pltpu.CompilerParams(
            collective_id=0, has_side_effects=True, vmem_limit_bytes=VMEM_LIMIT
        ),
        name="whole_grads",
    )(*pinned, logit_scale)
    d_tok, half_qkv, half_proj, d_table, d_scale, d_gain = pl.pallas_call(
        finish_kernel,
        out_shape=[
            jax.ShapeDtypeStruct((rows, cols, depth), b16),
            jax.ShapeDtypeStruct((3 * depth // 2, depth), f32),
            jax.ShapeDtypeStruct((depth // 2, depth), f32),
            jax.ShapeDtypeStruct((heads, entries), f32),
            jax.ShapeDtypeStruct((heads,), f32),
            jax.ShapeDtypeStruct((depth,), f32),
        ],
        in_specs=[VMEM] * 5,
        out_specs=[anywhere] * 6,
        scratch_shapes=[dma((6,))],
        compiler_params=pltpu.CompilerParams(vmem_limit_bytes=FINISH_LIMIT),
        name="finish",
    )(*outs)
    return d_tok[None], half_qkv.T, half_proj.T, d_table, d_scale, d_gain


def can_join(tokens, logit_scale):
    size_h, size_w, size_b = (lax.axis_size(name) for name in ("ha", "wa", "ba"))
    images, rows, cols, depth = tokens.shape
    peers = size_h // 2 * size_w
    return (
        images == 1 and size_b == 2 and size_w == 2 and size_h % 2 == 0 and size_h > 2
        and logit_scale.shape[0] == 3 * GROUP and depth == 3 * 128 and WIN == 8
        and rows % WIN == 0 and cols % (2 * WIN) == 0 and rows * cols // 64 % (2 * BWD) == 0 and rows > WIN
        and 64 % peers == 0 and 64 // peers % 8 == 0
    )


def shift_in(tokens, cotangent, shift):
    stacked = jnp.stack([tokens, cotangent])
    below = from_behind(stacked[:, :, :shift], "ha", -1)
    tall = jnp.concatenate([stacked[:, :, shift:], below], 2)
    beside = from_behind(tall[:, :, :, :shift], "wa", -1)
    moved = jnp.concatenate([tall[:, :, :, shift:], beside], 3)
    return (moved[0], moved[1])


def shift_out(grads, shift):
    rows = grads.shape[1]
    cols = grads.shape[2]
    right = from_behind(grads[:, :, cols - shift :], "wa", 1)
    wide = jnp.concatenate([right, grads[:, :, : cols - shift]], 2)
    lower = from_behind(wide[:, rows - shift :], "ha", 1)
    return jnp.concatenate([lower, wide[:, : rows - shift]], 1)


def shards(tokens, cotangent, w_qkv, w_proj, table_logits, logit_scale, gain):
    rows = tokens.shape[1]
    cols = tokens.shape[2]
    shift = WIN // 2
    height = rows * lax.axis_size("ha")
    width = cols * lax.axis_size("wa")
    row_base = lax.axis_index("ha") * rows
    col_base = lax.axis_index("wa") * cols
    if can_join(tokens, logit_scale):
        return whole_grads(
            tokens, cotangent, w_qkv, w_proj, table_logits, logit_scale, gain, height, width, WIN
        )
    params = (w_qkv, w_proj, table_logits, logit_scale, gain)
    moved, moved_grad = shift_in(tokens, cotangent, shift)
    d_moved, parts = local_grads(moved, moved_grad, row_base, col_base, height, width, WIN, params)
    back = shift_out(d_moved, shift)
    d_tokens = (cotangent.astype(jnp.float32) + back.astype(jnp.float32)).astype(jnp.bfloat16)
    d_wqkv, d_wproj, d_table, d_scale, d_gain = parts
    half_qkv, half_proj = (
        lax.psum_scatter(d_wqkv.astype(jnp.bfloat16), "ba", scatter_dimension=1, tiled=True).astype(jnp.float32),
        lax.psum_scatter(d_wproj.astype(jnp.bfloat16), "ba", scatter_dimension=1, tiled=True).astype(jnp.float32),
    )
    half_qkv, half_proj = lax.psum((half_qkv, half_proj), ("ha", "wa"))
    d_table, d_scale, d_gain = lax.psum((d_table, d_scale, d_gain), ("ha", "wa", "ba"))
    return (d_tokens, half_qkv, half_proj, d_table, d_scale, d_gain)


def solution(mesh):
    return jax.shard_map(
        shards,
        mesh=mesh,
        in_specs=(P("ba", "ha", "wa", None), P("ba", "ha", "wa", None), P(), P(), P(), P(), P()),
        out_specs=(P("ba", "ha", "wa", None), P(None, "ba"), P(None, "ba"), P(), P(), P()),
        check_vma=False,
    )
```

```python
import math

import functools

import jax
import jax.numpy as jnp
import numpy as np
from jax import lax
from jax.experimental import pallas as pl
from jax.experimental.pallas import tpu as pltpu
from jax.sharding import PartitionSpec as P

WIN = 8


EPS_NORM = 1e-05
MASK_FILL = -100.0
SCALE_CAP = math.log(100.0)
BIAS_RANGE = 16.0


def from_behind(block, axis, distance):
    devices = range(lax.axis_size(axis))
    route = [((i - distance) % len(devices), i) for i in devices]
    return lax.ppermute(block, axis, route)


def to_windows(block, window):
    images, height, width, depth = block.shape
    tiles = block.reshape(images, height // window, window, width // window, window, depth)
    tiles = tiles.transpose(0, 1, 3, 2, 4, 5)
    return tiles.reshape(images, height // window * (width // window), window * window, depth)


def from_windows(tiles, images, height, width, window):
    depth = tiles.shape[-1]
    grid = tiles.reshape(images, height // window, width // window, window, window, depth)
    return grid.transpose(0, 1, 3, 2, 4, 5).reshape(images, height, width, depth)


def region_of(coords, extent, window):
    return (coords >= extent - window).astype(jnp.int32) + (coords >= extent - window // 2).astype(
        jnp.int32
    )

GROUP = 4
FWD = 2
BWD = 4
LONG_FWD = 4
LONG_BWD = 8
LOG2E = math.log2(math.e)
VMEM_LIMIT = 40 * 2**20
FINISH_LIMIT = 4 * 2**20
MESH = pl.DeviceIdType.MESH
VMEM = pl.BlockSpec(memory_space=pltpu.VMEM)
NN = (((1,), (0,)), ((), ()))
NT = (((1,), (1,)), ((), ()))
TN = (((0,), (0,)), ((), ()))


def mxu(left, right, dims):
    return lax.dot_general(left, right, dims, preferred_element_type=jnp.float32)


def split(value):
    high = value.astype(jnp.bfloat16)
    return high, (value - high.astype(jnp.float32)).astype(jnp.bfloat16)


def mxu_fine(left, right, dims):
    high, low = split(left)
    return mxu(high, right, dims) + mxu(low, right, dims)


def same_block(rows, cols, row_size, col_size):
    row = lax.broadcasted_iota(jnp.int32, (rows, cols), 0) // row_size
    col = lax.broadcasted_iota(jnp.int32, (rows, cols), 1) // col_size
    return (row == col).astype(jnp.bfloat16)


def tile_heads(value, width):
    lane = lax.broadcasted_iota(jnp.int32, (1, value.shape[1]), 1) % (GROUP * width) // width
    rows = []
    for head in range(GROUP):
        rows.append(value * (lane == head).astype(jnp.bfloat16))
    return jnp.concatenate(rows, 0)


def gather_heads(value, width, length):
    lane = lax.broadcasted_iota(jnp.int32, (length, value.shape[1]), 1) // width
    total = value[:length]
    for head in range(1, GROUP):
        total = jnp.where(lane == head, value[head * length : (head + 1) * length], total)
    return total


def local_kernel(
    grid_cols, height, width, window,
    flat_ref, grad_ref, w_qkv_ref, w_proj_ref, bias_ref, scale_ref, gain_ref,
    d_flat_ref, d_wqkv_ref, d_wproj_ref, d_bias_ref, d_cos_ref, d_gain_ref,
    qkv_ref, att_ref, d_att_ref, d_qkv_ref, probs_ref, kinv_ref, qrow_ref, masked_ref, raw_q_ref, raw_k_ref,
    norm_ref,
):
    tokens, depth = flat_ref.shape
    f32, b16 = jnp.float32, jnp.bfloat16
    length = window * window
    count = tokens // length
    groups = bias_ref.shape[0]
    lanes = depth // groups
    heads = groups * GROUP
    head_dim = lanes // GROUP
    wide = GROUP * length
    row_base = lax.axis_index("ha") * (count // grid_cols * window)
    col_base = lax.axis_index("wa") * (grid_cols * window)

    qkv_ref[...] = mxu(flat_ref[...], w_qkv_ref[...], NN).astype(b16)
    lane_ones = same_block(lanes, wide, head_dim, length)
    lane_lane = same_block(lanes, lanes, head_dim, head_dim)

    head_rows = scale_ref.shape[0]
    pick = same_block(head_rows, depth, 1, head_dim)
    high, low = split(jnp.square(qkv_ref[:, :depth].astype(f32)))
    q_sums = mxu(pick, high, NT) + mxu(pick, low, NT)
    q_rows = lax.rsqrt(q_sums + 1.0) * scale_ref[:, :1]
    half = lax.broadcasted_iota(jnp.int32, (1, 2 * length), 1) < length
    for j in range(count // 2):
        base = q_rows[:, j * 2 * length : (j + 1) * 2 * length]
        turned = pltpu.roll(base, length, 1)
        for g in range(groups):
            for p in range(GROUP // 2):
                one, two = g * GROUP + 2 * p, g * GROUP + 2 * p + 1
                place = slice(p * 2 * length, (p + 1) * 2 * length)
                qrow_ref[2 * j, g, :, place] = jnp.where(half, base[one : one + 1], turned[two : two + 1])
                qrow_ref[2 * j + 1, g, :, place] = jnp.where(half, turned[one : one + 1], base[two : two + 1])
    for g in range(groups):
        query = qkv_ref[:, g * lanes : (g + 1) * lanes].astype(f32)
        key = qkv_ref[:, depth + g * lanes : depth + (g + 1) * lanes].astype(f32)
        high, low = split(jnp.square(key))
        kinv_ref[g] = lax.rsqrt(mxu(high, lane_ones, NN) + mxu(low, lane_ones, NN) + 1.0)
        norm_ref[1, g] = 1.0 / (mxu(high, lane_lane, NN) + mxu(low, lane_lane, NN) + 1.0)
        high, low = split(jnp.square(query))
        norm_ref[0, g] = 1.0 / (mxu(high, lane_lane, NN) + mxu(low, lane_lane, NN) + 1.0)

    mine = lax.broadcasted_iota(jnp.int32, (length, wide), 0)
    other = lax.broadcasted_iota(jnp.int32, (length, wide), 1) % length
    cut = window // 2
    row_off = (mine // window // cut) != (other // window // cut)
    col_off = (mine % window // cut) != (other % window // cut)
    for g in range(groups):
        bias = bias_ref[g] * LOG2E
        masked_ref[0, g] = bias
        masked_ref[1, g] = jnp.where(col_off, bias + MASK_FILL * LOG2E, bias)
        masked_ref[2, g] = jnp.where(row_off, bias + MASK_FILL * LOG2E, bias)
        masked_ref[3, g] = jnp.where(row_off | col_off, bias + MASK_FILL * LOG2E, bias)

    def load(ref, w, g, part):
        return ref[
            pl.ds(pl.multiple_of(w * length, length), length),
            part * depth + g * lanes : part * depth + (g + 1) * lanes,
        ]

    def forward(step, carry):
        units = [(step * FWD + k, g) for k in range(FWD) for g in range(groups)]
        scores = []
        for w, g in units:
            query, key = load(qkv_ref, w, g, 0), load(qkv_ref, w, g, 1)
            raw = mxu(key, tile_heads(query, head_dim), NT)
            last_row = (row_base + w // grid_cols * window) // (height - window)
            last_col = (col_base + w % grid_cols * window) // (width - window)
            kinv = kinv_ref[g, pl.ds(pl.multiple_of(w * length, length), length), :]
            scores.append(raw * kinv * (qrow_ref[w, g] * LOG2E) + masked_ref[last_row * 2 + last_col, g])
        for (w, g), score in zip(units, scores):
            expo = jnp.exp2(score - jnp.max(score, 0, keepdims=True))
            probs = expo * (1.0 / jnp.sum(expo, 0, keepdims=True))
            probs_ref[w, g] = probs
            att = gather_heads(mxu(probs.astype(b16), load(qkv_ref, w, g, 2), TN), head_dim, length)
            att_ref[
                pl.ds(pl.multiple_of(w * length, length), length), g * lanes : (g + 1) * lanes
            ] = att.astype(b16)
        return carry

    lax.fori_loop(0, count // FWD, forward, 0)

    proj = mxu(att_ref[...], w_proj_ref[...], NN)
    centre = proj - jnp.mean(proj, -1, keepdims=True)
    inv_std = lax.rsqrt(jnp.mean(centre * centre, -1, keepdims=True) + EPS_NORM)
    normed = centre * inv_std
    upstream = grad_ref[...].astype(f32)
    d_gain_ref[...] = jnp.sum(upstream * normed, 0, keepdims=True)
    scaled = upstream * gain_ref[...]
    d_proj = inv_std * (
        scaled
        - jnp.mean(scaled, -1, keepdims=True)
        - normed * jnp.mean(scaled * normed, -1, keepdims=True)
    )
    d_proj = d_proj.astype(b16)
    d_wproj_ref[...] = mxu(att_ref[...], d_proj, TN)
    d_att_ref[...] = mxu(d_proj, w_proj_ref[...], NT).astype(b16)
    d_bias_ref[...] = jnp.zeros_like(d_bias_ref)

    for g in range(groups):

        def backward(step, carry):
            units = [step * BWD + k for k in range(BWD)]
            grads = []
            for w in units:
                d_tall = tile_heads(load(d_att_ref, w, g, 0), head_dim)
                d_probs = mxu(load(qkv_ref, w, g, 2), d_tall, NT)
                d_value = mxu(probs_ref[w, g].astype(b16), d_tall, NN)
                d_qkv_ref[
                    pl.ds(pl.multiple_of(w * length, length), length),
                    2 * depth + g * lanes : 2 * depth + (g + 1) * lanes,
                ] = d_value.astype(b16)
                grads.append(d_probs)
            total = d_bias_ref[g]
            for w, d_probs in zip(units, grads):
                rows = pl.ds(pl.multiple_of(w * length, length), length)
                probs = probs_ref[w, g]
                d_scores = probs * (d_probs - jnp.sum(d_probs * probs, 0, keepdims=True))
                total = total + d_scores
                high, low = split(d_scores * kinv_ref[g, rows, :] * qrow_ref[w, g])
                both = jnp.concatenate([high, low], 0)
                query, key = load(qkv_ref, w, g, 0), load(qkv_ref, w, g, 1)
                pair = mxu(both, tile_heads(query, head_dim), NN)
                raw_k_ref[rows, :] = pair[:length] + pair[length:]
                tall = mxu(both, jnp.concatenate([key, key], 0), TN)
                raw_q_ref[rows, :] = gather_heads(tall, head_dim, length)
            d_bias_ref[g] = total
            return carry

        lax.fori_loop(0, count // BWD, backward, 0)
        for part, ref in enumerate((raw_q_ref, raw_k_ref)):
            place = slice(part * depth + g * lanes, part * depth + (g + 1) * lanes)
            value, grad = qkv_ref[:, place].astype(f32), ref[...]
            along = value * grad
            if part == 0:
                d_cos_ref[g] = jnp.sum(along, 0, keepdims=True)
            d_qkv_ref[:, place] = (
                grad - value * norm_ref[part, g] * mxu_fine(along, lane_lane, NN)
            ).astype(b16)
    d_wqkv_ref[...] = mxu(flat_ref[...], d_qkv_ref[...], TN)
    d_flat_ref[...] = mxu(d_qkv_ref[...], w_qkv_ref[...], NT).astype(b16)


def offset_onehot(window):
    places = np.arange(window * window)
    row_of, col_of = places // window, places % window
    offset = (row_of[:, None] - row_of[None, :] + window - 1) * (2 * window - 1) + (
        col_of[:, None] - col_of[None, :] + window - 1
    )
    return jnp.asarray(offset.reshape(-1), jnp.int32)


def three_parts(value):
    high = lax.reduce_precision(value, 8, 7)
    middle = lax.reduce_precision(value - high, 8, 7)
    return jnp.concatenate([high, middle, value - high - middle], 0).astype(jnp.bfloat16)


def local_grads(block, grad_block, row_base, col_base, height, width, window, params):
    w_qkv, w_proj, table_logits, logit_scale, gain = params
    images, rows, cols, depth = block.shape
    heads = logit_scale.shape[0]
    length = window * window
    groups = heads // GROUP
    wide = GROUP * length
    flat = to_windows(block, window).reshape(-1, depth)
    grad_flat = to_windows(grad_block, window).reshape(-1, depth)
    tokens = flat.shape[0]
    count = tokens // length
    scale = jnp.exp(jnp.minimum(logit_scale, SCALE_CAP))
    scale_rows = jnp.pad(scale, (0, -heads % 16)).reshape(-1, 1) * jnp.ones((1, 128), jnp.float32)
    sigma = jax.nn.sigmoid(table_logits)
    entries = table_logits.shape[1]
    hot = offset_onehot(window)[None, :] == jnp.arange(entries, dtype=jnp.int32)[:, None]
    hot = hot.astype(jnp.bfloat16)
    parts = jnp.dot(three_parts(sigma * BIAS_RANGE), hot, preferred_element_type=jnp.float32)
    rel_bias = jnp.sum(parts.reshape(3, heads, -1), 0).reshape(groups, GROUP, length, length)
    rel_bias = rel_bias.transpose(0, 3, 1, 2).reshape(groups, length, wide)
    f32, b16 = jnp.float32, jnp.bfloat16
    d_flat, d_wqkv, d_wproj, d_bias, d_cos, d_gain = pl.pallas_call(
        functools.partial(local_kernel, cols // window, height, width, window),
        out_shape=[
            jax.ShapeDtypeStruct((tokens, depth), b16),
            jax.ShapeDtypeStruct((depth, 3 * depth), f32),
            jax.ShapeDtypeStruct((depth, depth), f32),
            jax.ShapeDtypeStruct((groups, length, wide), f32),
            jax.ShapeDtypeStruct((groups, 1, depth // groups), f32),
            jax.ShapeDtypeStruct((1, depth), f32),
        ],
        in_specs=[VMEM] * 7,
        out_specs=[VMEM] * 6,
        scratch_shapes=[
            pltpu.VMEM((tokens, 3 * depth), b16),
            pltpu.VMEM((tokens, depth), b16),
            pltpu.VMEM((tokens, depth), b16),
            pltpu.VMEM((tokens, 3 * depth), b16),
            pltpu.VMEM((count, groups, length, wide), f32),
            pltpu.VMEM((groups, tokens, wide), f32),
            pltpu.VMEM((count, groups, 1, wide), f32),
            pltpu.VMEM((4, groups, length, wide), f32),
            pltpu.VMEM((tokens, depth // groups), f32),
            pltpu.VMEM((tokens, depth // groups), f32),
            pltpu.VMEM((2, groups, tokens, depth // groups), f32),
        ],
        compiler_params=pltpu.CompilerParams(vmem_limit_bytes=48 * 2**20),
        cost_estimate=pl.CostEstimate(
            flops=4_000_000_000, bytes_accessed=8_000_000, transcendentals=400_000
        ),
        name="local_grads",
    )(flat, grad_flat, w_qkv, w_proj, rel_bias, scale_rows, gain.reshape(1, depth))
    heads_bias = d_bias.reshape(groups, length, GROUP, length).transpose(0, 2, 3, 1)
    heads_bias = heads_bias.reshape(heads, length * length)
    sums = lax.dot_general(three_parts(heads_bias), hot, NT, preferred_element_type=jnp.float32)
    d_table = jnp.sum(sums.reshape(3, heads, entries), 0) * (BIAS_RANGE * sigma * (1.0 - sigma))
    live = (logit_scale < SCALE_CAP).astype(jnp.float32)
    d_scale = jnp.sum(d_cos.reshape(heads, depth // heads), 1) * live
    d_block = from_windows(d_flat.reshape(images, count, length, depth), images, rows, cols, window)
    return (d_block, (d_wqkv, d_wproj, d_table, d_scale, d_gain.reshape(depth)))


def half_turn(value, axis):
    return pltpu.roll(value, value.shape[axis] // 2, axis)


def exp_fine(value):
    whole = jnp.floor(value * LOG2E + 0.5)
    rest = value - whole * 0.693359375 + whole * 2.12194440e-4
    total = jnp.ones_like(rest)
    for k in range(8, 0, -1):
        total = 1.0 + total * rest * (1.0 / k)
    return total * jnp.exp2(whole)


def inverse(value):
    guess = 1.0 / value
    return guess * (2.0 - value * guess)


def place_of(index, window):
    return index // window * (2 * window - 1) + index % window


def expand_bias(table, length, window, groups, out_ref):
    span = table.shape[1]
    f32, b16 = jnp.float32, jnp.bfloat16
    heads = groups * GROUP
    base = jnp.concatenate([jnp.broadcast_to(table[h : h + 1], (window, span)) for h in range(heads)], 0)
    sub = lax.broadcasted_iota(jnp.int32, base.shape, 0) % window
    bit = 1
    while bit < window:
        base = jnp.where(sub // bit % 2 == 1, pltpu.roll(base, bit, 1), base)
        bit *= 2
    top = place_of(length - 1, window)
    turned = [
        pltpu.roll(base, (span - top + (2 * window - 1) * r) % span, 1)[:, : span // 2] for r in range(window)
    ]
    wide = GROUP * length
    row = lax.broadcasted_iota(jnp.int32, (span, wide), 0) % (span // 2)
    col = lax.broadcasted_iota(jnp.int32, (span, wide), 1)
    hit = row == place_of(col % length, window)
    for g in range(groups):
        total = jnp.zeros((length, wide), f32)
        for k in range(GROUP):
            h = g * GROUP + k
            block = jnp.concatenate([t[h * window : (h + 1) * window] for t in turned], 0)
            pair = jnp.concatenate(split(block), 1)
            total = total + mxu(pair, (hit & (col // length == k)).astype(b16), NN)
        out_ref[0, g] = total


def fold_bias(grads, length, window, span):
    f32, b16 = jnp.float32, jnp.bfloat16
    wide = GROUP * length
    row = lax.broadcasted_iota(jnp.int32, (wide, span // 2), 0)
    col = lax.broadcasted_iota(jnp.int32, (wide, span // 2), 1)
    hit = col == place_of(row % length, window)
    both = jnp.concatenate([half for grad in grads for half in split(grad)], 0)
    by_head = [None] * (len(grads) * GROUP)
    for k in range(GROUP):
        pairs = mxu(both, (hit & (row // length == k)).astype(b16), NN)
        for g in range(len(grads)):
            pair = pairs[2 * g * length : (2 * g + 2) * length]
            block = pair[:length] + pair[length:]
            by_head[g * GROUP + k] = jnp.concatenate([block, jnp.zeros_like(block)], 1)
    parts = [
        jnp.concatenate([block[r * window : (r + 1) * window] for block in by_head], 0) for r in range(window)
    ]
    step = 2 * window - 1
    while len(parts) > 1:
        parts = [pltpu.roll(parts[i], step, 1) + parts[i + 1] for i in range(0, len(parts), 2)]
        step *= 2
    total = parts[0]
    sub = window - 1 - lax.broadcasted_iota(jnp.int32, total.shape, 0) % window
    bit = 1
    while bit < window:
        total = jnp.where(sub // bit % 2 == 1, pltpu.roll(total, bit, 1), total)
        bit *= 2
    return [jnp.sum(total[k * window : (k + 1) * window], 0, keepdims=True) for k in range(len(by_head))]


def whole_kernel(
    shape, height, width, window,
    tokens_ref, cot_ref, w_qkv_hbm, w_proj_hbm, table_hbm, gain_hbm, scale_hbm,
    d_tok_ref, grads_out, table_out, scale_out, gain_out,
    tok, cot, w_qkv_ref, w_proj_ref, table_in, gain_ref, scale_ref, table_ref, local_sems,
    col_send, row_get, col_get, diag_get, halo_sems,
    flat_ref, grad_ref, d_flat_ref, d_proj_ref,
    qkv_ref, att_ref, d_att_ref, d_qkv_ref, probs_ref, kinv_ref, qrow_ref, masked_ref, raw_q_ref, raw_k_ref,
    norm_ref, d_bias_ref, p_mid, k_first, product_ref,
    row_back, col_back, row_back_get, col_back_get, diag_back_get, back_sems,
    small, small_core, small_a, small_image, small_b, small_side, small_c, small_near, small_total, tiny_sems,
    *chunk_refs,
):
    size_h, size_w = shape
    chips = size_h // 2
    peers = chips * size_w
    ha, wa, ba = lax.axis_index("ha"), lax.axis_index("wa"), lax.axis_index("ba")
    core = ha % 2
    me = wa * chips + ha // 2
    partner = (ha + 1 - 2 * core, wa, ba)
    image, side, corner = (ha, wa, 1 - ba), (ha, 1 - wa, ba), (ha, 1 - wa, 1 - ba)
    above, below = lax.rem(ha + size_h - 1, size_h), lax.rem(ha + 1, size_h)
    left, right = lax.rem(wa + size_w - 1, size_w), lax.rem(wa + 1, size_w)
    f32, b16 = jnp.float32, jnp.bfloat16

    def peer(step):
        other = lax.rem(me + step, peers)
        return other, (other % chips * 2 + core, other // chips, ba)

    loads = []
    for k, (src, dst) in enumerate(
        (
            (tokens_ref.at[0], tok), (cot_ref.at[0], cot), (w_qkv_hbm, w_qkv_ref), (w_proj_hbm, w_proj_ref),
            (table_hbm, table_in), (gain_hbm, gain_ref), (scale_hbm, scale_ref),
        )
    ):
        copy = pltpu.make_async_copy(src, dst, local_sems.at[k])
        copy.start()
        loads.append(copy)
    targets = [
        (above, wa, ba), (below, wa, ba), (ha, left, ba), (ha, right, ba), (above, left, ba), (below, right, ba),
        partner, image, corner,
    ] + [peer(step)[1] for step in range(1, peers)]
    barrier = pltpu.get_barrier_semaphore()
    for device in targets:
        pl.semaphore_signal(barrier, inc=1, device_id=device, device_id_type=MESH)

    def start(src, dst, sems, device):
        copy = pltpu.make_async_remote_copy(
            src_ref=src, dst_ref=dst, send_sem=sems.at[0], recv_sem=sems.at[1],
            device_id=device, device_id_type=MESH,
        )
        copy.start()
        return copy

    def all_of(src, dst, sems, device):
        return pltpu.make_async_remote_copy(
            src_ref=src, dst_ref=dst, send_sem=sems.at[0], recv_sem=sems.at[1],
            device_id=device, device_id_type=MESH,
        )

    rows, cols, depth = tok.shape
    cut = window // 2
    length = window * window
    across = cols // window
    count = rows // window * across
    fwd, bwd = math.gcd(across, LONG_FWD), math.gcd(count, LONG_BWD)
    tokens = count * length
    groups = qrow_ref.shape[1]
    lanes = depth // groups
    head_dim = lanes // GROUP
    wide = GROUP * length
    low_sub = lax.broadcasted_iota(jnp.int32, (window, depth), 0) < cut

    def pack_columns(a, ref):
        loads[a].wait()
        for j in range(rows // 2):
            first = ref[2 * j, :window, :].astype(f32)
            second = ref[2 * j + 1, :window, :].astype(f32)
            col_send[a, j] = jnp.where(low_sub, first, half_turn(second, 0)).astype(b16)

    halos = {}

    def send_halo(a, ref):
        halos[a, 0] = start(col_send.at[a], col_get.at[a], halo_sems.at[a, 1], (ha, left, ba))
        halos[a, 1] = start(ref.at[pl.ds(0, cut)], row_get.at[a], halo_sems.at[a, 0], (above, wa, ba))
        halos[a, 2] = start(
            col_send.at[a, pl.ds(0, cut // 2)], diag_get.at[a], halo_sems.at[a, 2], (above, left, ba)
        )

    pack_columns(0, tok)
    pl.semaphore_wait(barrier, len(targets))
    send_halo(0, tok)
    pack_columns(1, cot)
    send_halo(1, cot)

    for k in range(4, 7):
        loads[k].wait()
    heads = groups * GROUP
    entries = table_in.shape[1]
    table_ref[...] = jnp.zeros_like(table_ref)
    table_ref[:heads, :entries] = table_in[...]
    sigma = inverse(1.0 + exp_fine(-table_ref[...]))
    head_rows, span = table_ref.shape
    spot = lax.broadcasted_iota(jnp.int32, (head_rows, 128), 0)
    logits = jnp.zeros((head_rows, 128), f32)
    for h in range(heads):
        logits = jnp.where(spot == h, scale_ref[h], logits)
    scale = exp_fine(jnp.minimum(logits, SCALE_CAP))
    expand_bias(sigma * (BIAS_RANGE * LOG2E), length, window, groups, masked_ref)
    mine = lax.broadcasted_iota(jnp.int32, (length, wide), 0)
    other = lax.broadcasted_iota(jnp.int32, (length, wide), 1) % length
    row_off = (mine // window // cut) != (other // window // cut)
    col_off = (mine % window // cut) != (other % window // cut)
    for g in range(groups):
        bias = masked_ref[0, g]
        masked_ref[1, g] = jnp.where(col_off, bias + MASK_FILL * LOG2E, bias)
        masked_ref[2, g] = jnp.where(row_off, bias + MASK_FILL * LOG2E, bias)
        masked_ref[3, g] = jnp.where(row_off | col_off, bias + MASK_FILL * LOG2E, bias)
    small[...] = jnp.zeros_like(small)

    def gather_rows(a, ref, out_ref, from_row, to_row):
        def shifted(i):
            if i + cut < rows:
                row, edge = ref[i + cut], col_get[a, (i + cut) // 2]
            else:
                row, edge = row_get[a, i + cut - rows], diag_get[a, (i + cut - rows) // 2]
            row, edge = row.astype(f32), edge.astype(f32)
            turned = [half_turn(row[k * window : (k + 1) * window], 0) for k in range(across)]
            turned.append(half_turn(edge, 0) if i % 2 == 0 else edge)
            return [jnp.where(low_sub, turned[k], turned[k + 1]) for k in range(across)]

        for i in range(from_row, to_row, 2):
            one, two = shifted(i), shifted(i + 1)
            for k in range(across):
                begin = (i // window * across + k) * length + i % window * window
                out_ref[begin : begin + 2 * window] = jnp.concatenate([one[k], two[k]], 0).astype(b16)

    row_base, col_base = ha * rows, wa * cols
    lane_ones = same_block(lanes, wide, head_dim, length)
    lane_lane = same_block(lanes, lanes, head_dim, head_dim)
    pick = same_block(head_rows, depth, 1, head_dim)
    half = lax.broadcasted_iota(jnp.int32, (1, 2 * length), 1) < length

    def project(begin_window, end_window):
        part_rows = slice(begin_window * length, end_window * length)
        qkv_ref[part_rows] = mxu(flat_ref[part_rows], w_qkv_ref[...], NN).astype(b16)
        high, low = split(jnp.square(qkv_ref[part_rows, :depth].astype(f32)))
        q_sums = mxu(pick, high, NT) + mxu(pick, low, NT)
        q_rows = lax.rsqrt(q_sums + 1.0) * scale[:, :1]
        for j in range(begin_window // 2, end_window // 2):
            shifted_j = 2 * j - begin_window
            base = q_rows[:, shifted_j * length : (shifted_j + 2) * length]
            turned = half_turn(base, 1)
            for g in range(groups):
                for p in range(GROUP // 2):
                    one, two = g * GROUP + 2 * p, g * GROUP + 2 * p + 1
                    place = slice(p * 2 * length, (p + 1) * 2 * length)
                    qrow_ref[2 * j, g, :, place] = jnp.where(half, base[one : one + 1], turned[two : two + 1])
                    qrow_ref[2 * j + 1, g, :, place] = jnp.where(half, turned[one : one + 1], base[two : two + 1])
        for g in range(groups):
            key = qkv_ref[part_rows, depth + g * lanes : depth + (g + 1) * lanes].astype(f32)
            high, low = split(jnp.square(key))
            kinv_ref[g, part_rows] = lax.rsqrt(mxu(high, lane_ones, NN) + mxu(low, lane_ones, NN) + 1.0)

    def norms(begin_window, end_window):
        part_rows = slice(begin_window * length, end_window * length)
        for g in range(groups):
            for part in range(2):
                place = slice(part * depth + g * lanes, part * depth + (g + 1) * lanes)
                high, low = split(jnp.square(qkv_ref[part_rows, place].astype(f32)))
                inv = lax.rsqrt(mxu(high, lane_lane, NN) + mxu(low, lane_lane, NN) + 1.0)
                norm_ref[part, g, part_rows] = inv * inv

    def load(ref, w, g, part):
        return ref[
            pl.ds(pl.multiple_of(w * length, length), length),
            part * depth + g * lanes : part * depth + (g + 1) * lanes,
        ]

    def forward(step, carry):
        units = [(step * fwd + k, g) for k in range(fwd) for g in range(groups)]
        scores = []
        for w, g in units:
            query, key = load(qkv_ref, w, g, 0), load(qkv_ref, w, g, 1)
            raw = mxu(key, tile_heads(query, head_dim), NT)
            last_row = (row_base + w // across * window) // (height - window)
            last_col = (col_base + w % across * window) // (width - window)
            kinv = kinv_ref[g, pl.ds(pl.multiple_of(w * length, length), length), :]
            scores.append(raw * kinv * (qrow_ref[w, g] * LOG2E) + masked_ref[last_row * 2 + last_col, g])
        for (w, g), score in zip(units, scores):
            expo = jnp.exp2(score - jnp.max(score, 0, keepdims=True))
            probs = expo * (1.0 / jnp.sum(expo, 0, keepdims=True))
            probs_ref[w, g] = probs
            att = gather_heads(mxu(probs.astype(b16), load(qkv_ref, w, g, 2), TN), head_dim, length)
            att_ref[
                pl.ds(pl.multiple_of(w * length, length), length), g * lanes : (g + 1) * lanes
            ] = att.astype(b16)
        return carry

    def norm_gradient(begin_window, end_window):
        part_rows = slice(begin_window * length, end_window * length)
        proj = mxu(att_ref[part_rows], w_proj_ref[...], NN)
        centre = proj - jnp.mean(proj, -1, keepdims=True)
        inv_std = lax.rsqrt(jnp.mean(centre * centre, -1, keepdims=True) + EPS_NORM)
        normed = centre * inv_std
        upstream = grad_ref[part_rows].astype(f32)
        d_gain = jnp.sum(upstream * normed, 0, keepdims=True)
        scaled = upstream * gain_ref[...].reshape(1, depth)
        d_proj = inv_std * (
            scaled
            - jnp.mean(scaled, -1, keepdims=True)
            - normed * jnp.mean(scaled * normed, -1, keepdims=True)
        )
        d_proj = d_proj.astype(b16)
        d_proj_ref[part_rows] = d_proj
        d_att_ref[part_rows] = mxu(d_proj, w_proj_ref[...], NT).astype(b16)
        return d_gain

    early = count - across
    halos[0, 0].wait()
    gather_rows(0, tok, flat_ref, 0, rows - window)
    loads[2].wait()
    project(0, early)
    lax.fori_loop(0, early // fwd, forward, 0)
    norms(0, early)
    halos[1, 0].wait()
    gather_rows(1, cot, grad_ref, 0, rows - window)
    loads[3].wait()
    d_gain = norm_gradient(0, early)
    halos[0, 1].wait()
    halos[0, 2].wait()
    gather_rows(0, tok, flat_ref, rows - window, rows)
    project(early, count)
    lax.fori_loop(early // fwd, count // fwd, forward, 0)
    halos[1, 1].wait()
    halos[1, 2].wait()
    gather_rows(1, cot, grad_ref, rows - window, rows)
    d_gain = d_gain + norm_gradient(early, count)
    small[heads : heads + 1, :] = d_gain[:, :span]
    small[heads + 1 : heads + 2, : depth - span] = d_gain[:, span:]
    per = len(chunk_refs) // 4
    chunks = [chunk_refs[c * per : (c + 1) * per] for c in range(4)]
    flying = {}

    def begin(c):
        core_send, core_mine, core_get = chunks[c][:3]
        w = core_send.shape[0] // 2
        for side_of in range(2):
            here = slice(side_of * w, (side_of + 1) * w)
            base = 2 * side_of * w
            theirs = pl.ds(pl.multiple_of(base + (1 - core) * w, 32), w)
            core_send[here] = product_ref[theirs, :].astype(b16)
        flying[c] = start(core_send, core_get, chunks[c][9], partner)
        for side_of in range(2):
            here = slice(side_of * w, (side_of + 1) * w)
            core_mine[here] = product_ref[pl.ds(pl.multiple_of(2 * side_of * w + core * w, 32), w), :]

    def cross(c):
        core_send, core_mine, core_get, plane_send, plane_get = chunks[c][:5]
        flying[c].wait()
        core_mine[...] = core_mine[...] + core_get[...].astype(f32)
        w = plane_send.shape[1]
        for k, (b, y, device) in enumerate(((1 - ba, wa, image), (ba, 1 - wa, side), (1 - ba, 1 - wa, corner))):
            place = pl.ds(pl.multiple_of((2 * b + y) * w, 32), w)
            plane_send[k] = core_mine[place, :].astype(b16)
            start(plane_send.at[k], plane_get.at[k], chunks[c][10], device)
        flying[c] = [all_of(plane_send, plane_get, chunks[c][10], image)]

    def scatter(c):
        core_mine, plane_get, near_send, near_get = chunks[c][1], chunks[c][4], chunks[c][5], chunks[c][6]
        for copy in flying[c]:
            copy.wait()
        w = plane_get.shape[1]
        total = core_mine[pl.ds(pl.multiple_of((2 * ba + wa) * w, 32), w), :]
        for k in range(3):
            total = total + plane_get[k].astype(f32)
        r = near_send.shape[1]
        for j in range(chips):
            near_send[j] = total[j * r : (j + 1) * r].astype(b16)
        for step in range(1, chips):
            far_chip = lax.rem(ha // 2 + step, chips)
            start(near_send.at[far_chip], near_get.at[step - 1], chunks[c][11], (2 * far_chip + core, wa, ba))
        flying[c] = [all_of(near_send.at[pl.ds(0, chips - 1)], near_get, chunks[c][11], partner)]

    def gather(c):
        near_send, near_get, whole = chunks[c][5:8]
        for copy in flying[c]:
            copy.wait()
        total = near_send[ha // 2].astype(f32)
        for step in range(1, chips):
            total = total + near_get[step - 1].astype(f32)
        whole[me] = total.astype(b16)
        for step in range(1, peers):
            start(whole.at[me], whole.at[me], chunks[c][12], peer(step)[1])
        several = whole.at[pl.ds(0, peers - 1)]
        flying[c] = [all_of(several, several, chunks[c][12], partner)]

    def spread_column(c):
        near_send, near_get, whole = chunks[c][5:8]
        for copy in flying[c]:
            copy.wait()
        total = near_send[ha // 2].astype(f32)
        for step in range(1, chips):
            total = total + near_get[step - 1].astype(f32)
        whole[me] = total.astype(b16)
        for step in range(1, chips):
            far_chip = lax.rem(ha // 2 + step, chips)
            start(whole.at[me], whole.at[me], chunks[c][12], (2 * far_chip + core, wa, ba))
        several = whole.at[pl.ds(0, chips - 1)]
        flying[c] = [all_of(several, several, chunks[c][12], partner)]

    def relay(c):
        whole = chunks[c][7]
        for copy in flying[c]:
            copy.wait()
        held = pl.ds(wa * chips, chips)
        flying[c] = [start(whole.at[held], whole.at[held], chunks[c][14], side)]

    def mirror(c):
        whole, core_all = chunks[c][7:9]
        for copy in flying[c]:
            copy.wait()
        flying[c] = start(whole, core_all, chunks[c][13], partner)

    def finish(c):
        put(c, chunks[c][7], core)
        flying[c].wait()
        put(c, chunks[c][8], 1 - core)

    unit = lanes // 2
    proj_at = 3 * depth // 2

    targets_of = [
        [(proj_at + k * unit, proj_at + (1 + k) * unit) for k in range(2)],
        [(k * unit, (3 + k) * unit) for k in range(2)],
        [((4 + k) * unit, (1 + k if k < 2 else 5 + k) * unit) for k in range(4)],
        [(2 * unit, 5 * unit), (3 * unit, 6 * unit), (8 * unit, 0), (proj_at + 2 * unit, proj_at)],
    ]

    def put(c, source, which):
        r = source.shape[1]
        blocks = peers * r // unit
        for k in range(blocks):
            zero, one = targets_of[c][k], targets_of[c][blocks + k]
            row = jnp.where(
                which == 0, jnp.where(ba == 0, zero[0], zero[1]), jnp.where(ba == 0, one[0], one[1])
            )
            for j in range(unit // r):
                grads_out[pl.ds(pl.multiple_of(row + j * r, 8), r), :] = source[k * (unit // r) + j].astype(f32)

    product = mxu(d_proj_ref[...], att_ref[...], TN)
    product_ref[:lanes] = product[:lanes]
    p_mid[...] = product[lanes : 2 * lanes]
    product_ref[lanes : 2 * lanes] = product[2 * lanes :]
    begin(0)

    def backward_group(g):
        def backward(step, total):
            units = [step * bwd + k for k in range(bwd)]
            grads = []
            for w in units:
                d_tall = tile_heads(load(d_att_ref, w, g, 0), head_dim)
                d_probs = mxu(load(qkv_ref, w, g, 2), d_tall, NT)
                d_value = mxu(probs_ref[w, g].astype(b16), d_tall, NN)
                d_qkv_ref[
                    pl.ds(pl.multiple_of(w * length, length), length),
                    2 * depth + g * lanes : 2 * depth + (g + 1) * lanes,
                ] = d_value.astype(b16)
                grads.append(d_probs)
            summed = d_bias_ref[g]
            for w, d_probs in zip(units, grads):
                place = pl.ds(pl.multiple_of(w * length, length), length)
                probs = probs_ref[w, g]
                d_scores = probs * (d_probs - jnp.sum(d_probs * probs, 0, keepdims=True))
                summed = summed + d_scores
                high, low = split(d_scores * kinv_ref[g, place, :] * qrow_ref[w, g])
                both = jnp.concatenate([high, low], 0)
                query, key = load(qkv_ref, w, g, 0), load(qkv_ref, w, g, 1)
                pair = mxu(both, tile_heads(query, head_dim), NN)
                raw_k_ref[place, :] = pair[:length] + pair[length:]
                tall = mxu(both, jnp.concatenate([key, key], 0), TN)
                raw_q_ref[place, :] = gather_heads(tall, head_dim, length)
            d_bias_ref[g] = summed
            return total

        d_bias_ref[g] = jnp.zeros((length, wide), f32)
        lax.fori_loop(0, count // bwd, backward, 0)
        for part, ref in enumerate((raw_q_ref, raw_k_ref)):
            place = slice(part * depth + g * lanes, part * depth + (g + 1) * lanes)
            value, grad = qkv_ref[:, place].astype(f32), ref[...]
            along = value * grad
            if part == 0:
                spot = depth - span + g * lanes
                small[
                    heads + 1 + spot // span : heads + 2 + spot // span, spot % span : spot % span + lanes
                ] = jnp.sum(along, 0, keepdims=True)
            d_qkv_ref[:, place] = (
                grad - value * norm_ref[part, g] * mxu_fine(along, lane_lane, NN)
            ).astype(b16)

    def dense(g):
        joined = jnp.concatenate(
            [d_qkv_ref[:, part * depth + g * lanes : part * depth + (g + 1) * lanes] for part in range(3)], 1
        )
        return mxu(joined, flat_ref[...], TN)

    norms(early, count)
    backward_group(0)
    product = dense(0)
    product_ref[:lanes] = product[:lanes]
    product_ref[lanes : 2 * lanes] = product[2 * lanes :]
    k_first[...] = product[lanes : 2 * lanes]
    begin(1)
    cross(0)
    backward_group(2)
    cross(1)
    product = dense(2)
    product_ref[:lanes] = product[:lanes]
    product_ref[lanes : 2 * lanes] = k_first[...]
    product_ref[2 * lanes : 4 * lanes] = product[lanes:]
    begin(2)
    scatter(0)
    backward_group(1)
    cross(2)
    product = dense(1)
    product_ref[:lanes] = product[:lanes]
    product_ref[lanes : lanes + unit] = product[lanes : lanes + unit]
    product_ref[lanes + unit : 2 * lanes] = p_mid[:unit]
    product_ref[2 * lanes : 3 * lanes] = product[2 * lanes :]
    product_ref[3 * lanes : 3 * lanes + unit] = product[lanes + unit : 2 * lanes]
    product_ref[3 * lanes + unit : 4 * lanes] = p_mid[unit:]
    begin(3)
    scatter(1)
    d_flat_ref[...] = mxu(d_qkv_ref[...], w_qkv_ref[...], NT).astype(b16)

    def back_tiles(i):
        begin_row = i // window * across * length + i % window * window
        return [
            half_turn(d_flat_ref[begin_row + k * length : begin_row + k * length + window].astype(f32), 0)
            for k in range(across)
        ]

    for i in range(0, rows, 2):
        one, two = back_tiles(i), back_tiles(i + 1)
        col_back[i // 2] = jnp.where(low_sub, one[-1], half_turn(two[-1], 0)).astype(b16)
        if i >= rows - cut:
            row_back[i - (rows - cut)] = jnp.concatenate(one, 0).astype(b16)
            row_back[i + 1 - (rows - cut)] = jnp.concatenate(two, 0).astype(b16)
    far = (rows - cut) // 2
    back = [
        start(row_back, row_back_get, back_sems.at[0], (below, wa, ba)),
        start(col_back.at[pl.ds(0, far)], col_back_get, back_sems.at[1], (ha, right, ba)),
        start(col_back.at[pl.ds(far, cut // 2)], diag_back_get, back_sems.at[2], (below, right, ba)),
    ]
    cross(3)
    spread_column(0)
    for k, row in enumerate(fold_bias([d_bias_ref[g] for g in range(groups)], length, window, span)):
        small[k : k + 1, :] = row
    tiny = start(small, small_core, tiny_sems.at[0], partner)

    def put_row(i, turned, edge, odd):
        ahead = [half_turn(edge, 0) if odd else edge] + turned
        out = [jnp.where(low_sub, ahead[k], ahead[k + 1]) for k in range(across)]
        d_tok_ref[i] = (jnp.concatenate(out, 0) + cot[i].astype(f32)).astype(b16)

    scatter(2)
    back[1].wait()
    for i in range(rows - cut):
        put_row(i + cut, back_tiles(i), col_back_get[i // 2].astype(f32), i % 2 == 1)
    spread_column(1)
    tiny.wait()
    small_half = small_a.shape[0]
    my_rows = pl.ds(pl.multiple_of(core * small_half, 8), small_half)
    small_a[...] = small[my_rows, :] + small_core[my_rows, :]
    tiny = start(small_a, small_image, tiny_sems.at[1], image)
    relay(0)
    back[0].wait()
    back[2].wait()
    for i in range(cut):
        whole_row = row_back_get[i].astype(f32)
        turned = [whole_row[k * window : (k + 1) * window] for k in range(across)]
        put_row(i, turned, diag_back_get[i // 2].astype(f32), i % 2 == 1)
    scatter(3)
    tiny.wait()
    small_b[...] = small_a[...] + small_image[...]
    tiny = start(small_b, small_side, tiny_sems.at[2], side)
    spread_column(2)
    mirror(0)
    relay(1)
    tiny.wait()
    small_c[...] = small_b[...] + small_side[...]
    for step in range(1, chips):
        far_chip = lax.rem(ha // 2 + step, chips)
        start(small_c, small_near.at[step - 1], tiny_sems.at[3], (2 * far_chip + core, wa, ba))
    tinies = [all_of(small_near, small_near, tiny_sems.at[3], partner)]
    finish(0)
    gather(3)
    relay(2)
    mirror(1)
    for copy in tinies:
        copy.wait()
    total = small_c[...]
    for step in range(1, chips):
        total = total + small_near[step - 1]
    small_total[my_rows, :] = total
    tiny = start(small_total.at[my_rows], small_total.at[my_rows], tiny_sems.at[4], partner)
    finish(1)
    mirror(2)
    tiny.wait()
    total = small_total[...]
    table_out[...] = (total[: head_rows] * (BIAS_RANGE * sigma * (1.0 - sigma)))[:heads, :entries]
    gain_row = jnp.concatenate([total[heads : heads + 1, :], total[heads + 1 : heads + 2, : depth - span]], 1)
    gain_out[...] = gain_row.reshape(depth)
    sums = jnp.concatenate([total[heads + 1 : heads + 2, depth - span :], total[heads + 2 : heads + 3, :]], 1)
    sums = mxu_fine(jnp.broadcast_to(sums, (8, depth)), same_block(depth, 128, head_dim, 1), NN)[:1]
    at = lax.broadcasted_iota(jnp.int32, (1, 128), 1)
    logits = jnp.zeros((1, 128), f32)
    for h in range(heads):
        logits = jnp.where(at == h, scale_ref[h], logits)
    scale_out[...] = jnp.where(logits < SCALE_CAP, sums, 0.0).reshape(128)[:heads]
    mirror(3)
    finish(2)
    finish(3)


def finish_kernel(tok_ref, grads_ref, table_ref, scale_ref, gain_ref, tok, wq, wp, table, scale, gain, sems):
    cut = wq.shape[0]
    pairs = (
        (grads_ref.at[pl.ds(0, cut)], wq), (grads_ref.at[pl.ds(cut, wp.shape[0])], wp), (tok_ref, tok),
        (table_ref, table), (scale_ref, scale), (gain_ref, gain),
    )
    copies = [pltpu.make_async_copy(src, dst, sems.at[k]) for k, (src, dst) in enumerate(pairs)]
    for copy in copies:
        copy.start()
    for copy in copies:
        copy.wait()


def whole_grads(tokens, cotangent, w_qkv, w_proj, table_logits, logit_scale, gain, height, width, window):
    size_h, size_w = lax.axis_size("ha"), lax.axis_size("wa")
    peers = size_h // 2 * size_w
    f32, b16 = jnp.float32, jnp.bfloat16
    images, rows, cols, depth = tokens.shape
    heads = logit_scale.shape[0]
    entries = table_logits.shape[1]
    groups = heads // GROUP
    lanes = depth // groups
    length = window * window
    wide = GROUP * length
    total = rows * cols
    count = total // length
    cut = window // 2
    span = 256
    head_rows = -(-heads // 16) * 16
    half = depth // 2
    chips = size_h // 2
    dma, vmem = pltpu.SemaphoreType.DMA, pltpu.VMEM
    chunk_scratch = []
    for w in (lanes // 2, lanes // 2, lanes, lanes):
        r = w // peers
        chunk_scratch += [
            vmem((2 * w, depth), b16), vmem((2 * w, depth), f32), vmem((2 * w, depth), b16),
            vmem((3, w // 2, depth), b16), vmem((3, w // 2, depth), b16),
            vmem((chips, r, depth), b16), vmem((chips - 1, r, depth), b16),
            vmem((peers, r, depth), b16), vmem((peers, r, depth), b16),
            dma((2,)), dma((2,)), dma((2,)), dma((2,)), dma((2,)), dma((2,)),
        ]
    small, part = (16, span), (8, span)
    anywhere = pl.BlockSpec(memory_space=pltpu.HBM)
    pinned = [
        pltpu.with_memory_space_constraint(x, pltpu.HBM)
        for x in (tokens, cotangent, w_qkv, w_proj, table_logits, gain, logit_scale)
    ]
    outs = pl.pallas_call(
        functools.partial(whole_kernel, (size_h, size_w), height, width, window),
        out_shape=[
            jax.ShapeDtypeStruct((rows, cols, depth), b16),
            jax.ShapeDtypeStruct((2 * depth, depth), f32),
            jax.ShapeDtypeStruct((heads, entries), f32),
            jax.ShapeDtypeStruct((heads,), f32),
            jax.ShapeDtypeStruct((depth,), f32),
        ],
        in_specs=[anywhere] * 7,
        out_specs=[VMEM] * 5,
        scratch_shapes=[
            vmem((rows, cols, depth), b16), vmem((rows, cols, depth), b16),
            vmem((depth, 3 * depth), b16), vmem((depth, depth), b16),
            vmem((heads, entries), f32), vmem((depth,), f32), pltpu.SMEM((heads,), f32),
            vmem((head_rows, span), f32), dma((7,)),
            vmem((2, rows // 2, window, depth), b16), vmem((2, cut, cols, depth), b16),
            vmem((2, rows // 2, window, depth), b16), vmem((2, cut // 2, window, depth), b16), dma((2, 3, 2)),
            vmem((total, depth), b16), vmem((total, depth), b16), vmem((total, depth), b16), vmem((total, depth), b16),
            vmem((total, 3 * depth), b16), vmem((total, depth), b16), vmem((total, depth), b16),
            vmem((total, 3 * depth), b16), vmem((count, groups, length, wide), f32), vmem((groups, total, wide), f32),
            vmem((count, groups, 1, wide), f32), vmem((4, groups, length, wide), f32),
            vmem((total, lanes), f32), vmem((total, lanes), f32), vmem((2, groups, total, lanes), f32),
            vmem((groups, length, wide), f32), vmem((lanes, depth), f32), vmem((lanes, depth), f32),
            vmem((4 * lanes, depth), f32),
            vmem((cut, cols, depth), b16), vmem((rows // 2, window, depth), b16), vmem((cut, cols, depth), b16),
            vmem(((rows - cut) // 2, window, depth), b16), vmem((cut // 2, window, depth), b16), dma((3, 2)),
            vmem(small, f32), vmem(small, f32), vmem(part, f32), vmem(part, f32), vmem(part, f32), vmem(part, f32),
            vmem(part, f32), vmem((chips - 1, *part), f32), vmem(small, f32), dma((5, 2)),
            *chunk_scratch,
        ],
        compiler_params=pltpu.CompilerParams(
            collective_id=0, has_side_effects=True, vmem_limit_bytes=VMEM_LIMIT
        ),
        name="whole_grads",
    )(*pinned)
    d_tok, half_qkv, half_proj, d_table, d_scale, d_gain = pl.pallas_call(
        finish_kernel,
        out_shape=[
            jax.ShapeDtypeStruct((rows, cols, depth), b16),
            jax.ShapeDtypeStruct((3 * depth // 2, depth), f32),
            jax.ShapeDtypeStruct((depth // 2, depth), f32),
            jax.ShapeDtypeStruct((heads, entries), f32),
            jax.ShapeDtypeStruct((heads,), f32),
            jax.ShapeDtypeStruct((depth,), f32),
        ],
        in_specs=[VMEM] * 5,
        out_specs=[anywhere] * 6,
        scratch_shapes=[dma((6,))],
        compiler_params=pltpu.CompilerParams(vmem_limit_bytes=FINISH_LIMIT),
        name="finish",
    )(*outs)
    return d_tok[None], half_qkv.T, half_proj.T, d_table, d_scale, d_gain


def can_join(tokens, logit_scale):
    size_h, size_w, size_b = (lax.axis_size(name) for name in ("ha", "wa", "ba"))
    images, rows, cols, depth = tokens.shape
    peers = size_h // 2 * size_w
    return (
        images == 1 and size_b == 2 and size_w == 2 and size_h % 2 == 0 and size_h > 2
        and logit_scale.shape[0] == 3 * GROUP and depth == 3 * 128 and WIN == 8
        and rows % WIN == 0 and cols % (2 * WIN) == 0 and rows > WIN
        and 64 % peers == 0 and 64 // peers % 8 == 0
    )


def shift_in(tokens, cotangent, shift):
    stacked = jnp.stack([tokens, cotangent])
    below = from_behind(stacked[:, :, :shift], "ha", -1)
    tall = jnp.concatenate([stacked[:, :, shift:], below], 2)
    beside = from_behind(tall[:, :, :, :shift], "wa", -1)
    moved = jnp.concatenate([tall[:, :, :, shift:], beside], 3)
    return (moved[0], moved[1])


def shift_out(grads, shift):
    rows = grads.shape[1]
    cols = grads.shape[2]
    right = from_behind(grads[:, :, cols - shift :], "wa", 1)
    wide = jnp.concatenate([right, grads[:, :, : cols - shift]], 2)
    lower = from_behind(wide[:, rows - shift :], "ha", 1)
    return jnp.concatenate([lower, wide[:, : rows - shift]], 1)


def shards(tokens, cotangent, w_qkv, w_proj, table_logits, logit_scale, gain):
    rows = tokens.shape[1]
    cols = tokens.shape[2]
    shift = WIN // 2
    height = rows * lax.axis_size("ha")
    width = cols * lax.axis_size("wa")
    row_base = lax.axis_index("ha") * rows
    col_base = lax.axis_index("wa") * cols
    if can_join(tokens, logit_scale):
        return whole_grads(
            tokens, cotangent, w_qkv, w_proj, table_logits, logit_scale, gain, height, width, WIN
        )
    params = (w_qkv, w_proj, table_logits, logit_scale, gain)
    moved, moved_grad = shift_in(tokens, cotangent, shift)
    d_moved, parts = local_grads(moved, moved_grad, row_base, col_base, height, width, WIN, params)
    back = shift_out(d_moved, shift)
    d_tokens = (cotangent.astype(jnp.float32) + back.astype(jnp.float32)).astype(jnp.bfloat16)
    d_wqkv, d_wproj, d_table, d_scale, d_gain = parts
    half_qkv, half_proj = (
        lax.psum_scatter(d_wqkv.astype(jnp.bfloat16), "ba", scatter_dimension=1, tiled=True).astype(jnp.float32),
        lax.psum_scatter(d_wproj.astype(jnp.bfloat16), "ba", scatter_dimension=1, tiled=True).astype(jnp.float32),
    )
    half_qkv, half_proj = lax.psum((half_qkv, half_proj), ("ha", "wa"))
    d_table, d_scale, d_gain = lax.psum((d_table, d_scale, d_gain), ("ha", "wa", "ba"))
    return (d_tokens, half_qkv, half_proj, d_table, d_scale, d_gain)


def solution(mesh):
    return jax.shard_map(
        shards,
        mesh=mesh,
        in_specs=(P("ba", "ha", "wa", None), P("ba", "ha", "wa", None), P(), P(), P(), P(), P()),
        out_specs=(P("ba", "ha", "wa", None), P(None, "ba"), P(None, "ba"), P(), P(), P()),
        check_vma=False,
    )
```

```python
import math

import functools

import jax
import jax.numpy as jnp
import numpy as np
from jax import lax
from jax.experimental import pallas as pl
from jax.experimental.pallas import tpu as pltpu
from jax.sharding import PartitionSpec as P

WIN = 8


EPS_NORM = 1e-05
MASK_FILL = -100.0
SCALE_CAP = math.log(100.0)
BIAS_RANGE = 16.0


def from_behind(block, axis, distance):
    devices = range(lax.axis_size(axis))
    route = [((i - distance) % len(devices), i) for i in devices]
    return lax.ppermute(block, axis, route)


def to_windows(block, window):
    images, height, width, depth = block.shape
    tiles = block.reshape(images, height // window, window, width // window, window, depth)
    tiles = tiles.transpose(0, 1, 3, 2, 4, 5)
    return tiles.reshape(images, height // window * (width // window), window * window, depth)


def from_windows(tiles, images, height, width, window):
    depth = tiles.shape[-1]
    grid = tiles.reshape(images, height // window, width // window, window, window, depth)
    return grid.transpose(0, 1, 3, 2, 4, 5).reshape(images, height, width, depth)


def region_of(coords, extent, window):
    return (coords >= extent - window).astype(jnp.int32) + (coords >= extent - window // 2).astype(
        jnp.int32
    )

GROUP = 4
FWD = 2
BWD = 4
LONG_FWD = 4
LONG_BWD = 8
LOG2E = math.log2(math.e)
VMEM_LIMIT = 40 * 2**20
FINISH_LIMIT = 4 * 2**20
MESH = pl.DeviceIdType.MESH
VMEM = pl.BlockSpec(memory_space=pltpu.VMEM)
NN = (((1,), (0,)), ((), ()))
NT = (((1,), (1,)), ((), ()))
TN = (((0,), (0,)), ((), ()))


def mxu(left, right, dims):
    return lax.dot_general(left, right, dims, preferred_element_type=jnp.float32)


def split(value):
    high = value.astype(jnp.bfloat16)
    return high, (value - high.astype(jnp.float32)).astype(jnp.bfloat16)


def mxu_fine(left, right, dims):
    high, low = split(left)
    return mxu(high, right, dims) + mxu(low, right, dims)


def same_block(rows, cols, row_size, col_size):
    row = lax.broadcasted_iota(jnp.int32, (rows, cols), 0) // row_size
    col = lax.broadcasted_iota(jnp.int32, (rows, cols), 1) // col_size
    return (row == col).astype(jnp.bfloat16)


def tile_heads(value, width):
    lane = lax.broadcasted_iota(jnp.int32, (1, value.shape[1]), 1) % (GROUP * width) // width
    rows = []
    for head in range(GROUP):
        rows.append(value * (lane == head).astype(jnp.bfloat16))
    return jnp.concatenate(rows, 0)


def gather_heads(value, width, length):
    lane = lax.broadcasted_iota(jnp.int32, (length, value.shape[1]), 1) // width
    total = value[:length]
    for head in range(1, GROUP):
        total = jnp.where(lane == head, value[head * length : (head + 1) * length], total)
    return total


def local_kernel(
    grid_cols, height, width, window,
    flat_ref, grad_ref, w_qkv_ref, w_proj_ref, bias_ref, scale_ref, gain_ref,
    d_flat_ref, d_wqkv_ref, d_wproj_ref, d_bias_ref, d_cos_ref, d_gain_ref,
    qkv_ref, att_ref, d_att_ref, d_qkv_ref, probs_ref, kinv_ref, qrow_ref, masked_ref, raw_q_ref, raw_k_ref,
    norm_ref,
):
    tokens, depth = flat_ref.shape
    f32, b16 = jnp.float32, jnp.bfloat16
    length = window * window
    count = tokens // length
    groups = bias_ref.shape[0]
    lanes = depth // groups
    heads = groups * GROUP
    head_dim = lanes // GROUP
    wide = GROUP * length
    row_base = lax.axis_index("ha") * (count // grid_cols * window)
    col_base = lax.axis_index("wa") * (grid_cols * window)

    qkv_ref[...] = mxu(flat_ref[...], w_qkv_ref[...], NN).astype(b16)
    lane_ones = same_block(lanes, wide, head_dim, length)
    lane_lane = same_block(lanes, lanes, head_dim, head_dim)

    head_rows = scale_ref.shape[0]
    pick = same_block(head_rows, depth, 1, head_dim)
    high, low = split(jnp.square(qkv_ref[:, :depth].astype(f32)))
    q_sums = mxu(pick, high, NT) + mxu(pick, low, NT)
    q_rows = lax.rsqrt(q_sums + 1.0) * scale_ref[:, :1]
    half = lax.broadcasted_iota(jnp.int32, (1, 2 * length), 1) < length
    for j in range(count // 2):
        base = q_rows[:, j * 2 * length : (j + 1) * 2 * length]
        turned = pltpu.roll(base, length, 1)
        for g in range(groups):
            for p in range(GROUP // 2):
                one, two = g * GROUP + 2 * p, g * GROUP + 2 * p + 1
                place = slice(p * 2 * length, (p + 1) * 2 * length)
                qrow_ref[2 * j, g, :, place] = jnp.where(half, base[one : one + 1], turned[two : two + 1])
                qrow_ref[2 * j + 1, g, :, place] = jnp.where(half, turned[one : one + 1], base[two : two + 1])
    for g in range(groups):
        query = qkv_ref[:, g * lanes : (g + 1) * lanes].astype(f32)
        key = qkv_ref[:, depth + g * lanes : depth + (g + 1) * lanes].astype(f32)
        high, low = split(jnp.square(key))
        kinv_ref[g] = lax.rsqrt(mxu(high, lane_ones, NN) + mxu(low, lane_ones, NN) + 1.0)
        norm_ref[1, g] = 1.0 / (mxu(high, lane_lane, NN) + mxu(low, lane_lane, NN) + 1.0)
        high, low = split(jnp.square(query))
        norm_ref[0, g] = 1.0 / (mxu(high, lane_lane, NN) + mxu(low, lane_lane, NN) + 1.0)

    mine = lax.broadcasted_iota(jnp.int32, (length, wide), 0)
    other = lax.broadcasted_iota(jnp.int32, (length, wide), 1) % length
    cut = window // 2
    row_off = (mine // window // cut) != (other // window // cut)
    col_off = (mine % window // cut) != (other % window // cut)
    for g in range(groups):
        bias = bias_ref[g] * LOG2E
        masked_ref[0, g] = bias
        masked_ref[1, g] = jnp.where(col_off, bias + MASK_FILL * LOG2E, bias)
        masked_ref[2, g] = jnp.where(row_off, bias + MASK_FILL * LOG2E, bias)
        masked_ref[3, g] = jnp.where(row_off | col_off, bias + MASK_FILL * LOG2E, bias)

    def load(ref, w, g, part):
        return ref[
            pl.ds(pl.multiple_of(w * length, length), length),
            part * depth + g * lanes : part * depth + (g + 1) * lanes,
        ]

    def forward(step, carry):
        units = [(step * FWD + k, g) for k in range(FWD) for g in range(groups)]
        scores = []
        for w, g in units:
            query, key = load(qkv_ref, w, g, 0), load(qkv_ref, w, g, 1)
            raw = mxu(key, tile_heads(query, head_dim), NT)
            last_row = (row_base + w // grid_cols * window) // (height - window)
            last_col = (col_base + w % grid_cols * window) // (width - window)
            kinv = kinv_ref[g, pl.ds(pl.multiple_of(w * length, length), length), :]
            scores.append(raw * kinv * (qrow_ref[w, g] * LOG2E) + masked_ref[last_row * 2 + last_col, g])
        for (w, g), score in zip(units, scores):
            expo = jnp.exp2(score - jnp.max(score, 0, keepdims=True))
            probs = expo * (1.0 / jnp.sum(expo, 0, keepdims=True))
            probs_ref[w, g] = probs
            att = gather_heads(mxu(probs.astype(b16), load(qkv_ref, w, g, 2), TN), head_dim, length)
            att_ref[
                pl.ds(pl.multiple_of(w * length, length), length), g * lanes : (g + 1) * lanes
            ] = att.astype(b16)
        return carry

    lax.fori_loop(0, count // FWD, forward, 0)

    proj = mxu(att_ref[...], w_proj_ref[...], NN)
    centre = proj - jnp.mean(proj, -1, keepdims=True)
    inv_std = lax.rsqrt(jnp.mean(centre * centre, -1, keepdims=True) + EPS_NORM)
    normed = centre * inv_std
    upstream = grad_ref[...].astype(f32)
    d_gain_ref[...] = jnp.sum(upstream * normed, 0, keepdims=True)
    scaled = upstream * gain_ref[...]
    d_proj = inv_std * (
        scaled
        - jnp.mean(scaled, -1, keepdims=True)
        - normed * jnp.mean(scaled * normed, -1, keepdims=True)
    )
    d_proj = d_proj.astype(b16)
    d_wproj_ref[...] = mxu(att_ref[...], d_proj, TN)
    d_att_ref[...] = mxu(d_proj, w_proj_ref[...], NT).astype(b16)
    d_bias_ref[...] = jnp.zeros_like(d_bias_ref)

    for g in range(groups):

        def backward(step, carry):
            units = [step * BWD + k for k in range(BWD)]
            grads = []
            for w in units:
                d_tall = tile_heads(load(d_att_ref, w, g, 0), head_dim)
                d_probs = mxu(load(qkv_ref, w, g, 2), d_tall, NT)
                d_value = mxu(probs_ref[w, g].astype(b16), d_tall, NN)
                d_qkv_ref[
                    pl.ds(pl.multiple_of(w * length, length), length),
                    2 * depth + g * lanes : 2 * depth + (g + 1) * lanes,
                ] = d_value.astype(b16)
                grads.append(d_probs)
            total = d_bias_ref[g]
            for w, d_probs in zip(units, grads):
                rows = pl.ds(pl.multiple_of(w * length, length), length)
                probs = probs_ref[w, g]
                d_scores = probs * (d_probs - jnp.sum(d_probs * probs, 0, keepdims=True))
                total = total + d_scores
                high, low = split(d_scores * kinv_ref[g, rows, :] * qrow_ref[w, g])
                both = jnp.concatenate([high, low], 0)
                query, key = load(qkv_ref, w, g, 0), load(qkv_ref, w, g, 1)
                pair = mxu(both, tile_heads(query, head_dim), NN)
                raw_k_ref[rows, :] = pair[:length] + pair[length:]
                tall = mxu(both, jnp.concatenate([key, key], 0), TN)
                raw_q_ref[rows, :] = gather_heads(tall, head_dim, length)
            d_bias_ref[g] = total
            return carry

        lax.fori_loop(0, count // BWD, backward, 0)
        for part, ref in enumerate((raw_q_ref, raw_k_ref)):
            place = slice(part * depth + g * lanes, part * depth + (g + 1) * lanes)
            value, grad = qkv_ref[:, place].astype(f32), ref[...]
            along = value * grad
            if part == 0:
                d_cos_ref[g] = jnp.sum(along, 0, keepdims=True)
            d_qkv_ref[:, place] = (
                grad - value * norm_ref[part, g] * mxu_fine(along, lane_lane, NN)
            ).astype(b16)
    d_wqkv_ref[...] = mxu(flat_ref[...], d_qkv_ref[...], TN)
    d_flat_ref[...] = mxu(d_qkv_ref[...], w_qkv_ref[...], NT).astype(b16)


def offset_onehot(window):
    places = np.arange(window * window)
    row_of, col_of = places // window, places % window
    offset = (row_of[:, None] - row_of[None, :] + window - 1) * (2 * window - 1) + (
        col_of[:, None] - col_of[None, :] + window - 1
    )
    return jnp.asarray(offset.reshape(-1), jnp.int32)


def three_parts(value):
    high = lax.reduce_precision(value, 8, 7)
    middle = lax.reduce_precision(value - high, 8, 7)
    return jnp.concatenate([high, middle, value - high - middle], 0).astype(jnp.bfloat16)


def local_grads(block, grad_block, row_base, col_base, height, width, window, params):
    w_qkv, w_proj, table_logits, logit_scale, gain = params
    images, rows, cols, depth = block.shape
    heads = logit_scale.shape[0]
    length = window * window
    groups = heads // GROUP
    wide = GROUP * length
    flat = to_windows(block, window).reshape(-1, depth)
    grad_flat = to_windows(grad_block, window).reshape(-1, depth)
    tokens = flat.shape[0]
    count = tokens // length
    scale = jnp.exp(jnp.minimum(logit_scale, SCALE_CAP))
    scale_rows = jnp.pad(scale, (0, -heads % 16)).reshape(-1, 1) * jnp.ones((1, 128), jnp.float32)
    sigma = jax.nn.sigmoid(table_logits)
    entries = table_logits.shape[1]
    hot = offset_onehot(window)[None, :] == jnp.arange(entries, dtype=jnp.int32)[:, None]
    hot = hot.astype(jnp.bfloat16)
    parts = jnp.dot(three_parts(sigma * BIAS_RANGE), hot, preferred_element_type=jnp.float32)
    rel_bias = jnp.sum(parts.reshape(3, heads, -1), 0).reshape(groups, GROUP, length, length)
    rel_bias = rel_bias.transpose(0, 3, 1, 2).reshape(groups, length, wide)
    f32, b16 = jnp.float32, jnp.bfloat16
    d_flat, d_wqkv, d_wproj, d_bias, d_cos, d_gain = pl.pallas_call(
        functools.partial(local_kernel, cols // window, height, width, window),
        out_shape=[
            jax.ShapeDtypeStruct((tokens, depth), b16),
            jax.ShapeDtypeStruct((depth, 3 * depth), f32),
            jax.ShapeDtypeStruct((depth, depth), f32),
            jax.ShapeDtypeStruct((groups, length, wide), f32),
            jax.ShapeDtypeStruct((groups, 1, depth // groups), f32),
            jax.ShapeDtypeStruct((1, depth), f32),
        ],
        in_specs=[VMEM] * 7,
        out_specs=[VMEM] * 6,
        scratch_shapes=[
            pltpu.VMEM((tokens, 3 * depth), b16),
            pltpu.VMEM((tokens, depth), b16),
            pltpu.VMEM((tokens, depth), b16),
            pltpu.VMEM((tokens, 3 * depth), b16),
            pltpu.VMEM((count, groups, length, wide), f32),
            pltpu.VMEM((groups, tokens, wide), f32),
            pltpu.VMEM((count, groups, 1, wide), f32),
            pltpu.VMEM((4, groups, length, wide), f32),
            pltpu.VMEM((tokens, depth // groups), f32),
            pltpu.VMEM((tokens, depth // groups), f32),
            pltpu.VMEM((2, groups, tokens, depth // groups), f32),
        ],
        compiler_params=pltpu.CompilerParams(vmem_limit_bytes=48 * 2**20),
        cost_estimate=pl.CostEstimate(
            flops=4_000_000_000, bytes_accessed=8_000_000, transcendentals=400_000
        ),
        name="local_grads",
    )(flat, grad_flat, w_qkv, w_proj, rel_bias, scale_rows, gain.reshape(1, depth))
    heads_bias = d_bias.reshape(groups, length, GROUP, length).transpose(0, 2, 3, 1)
    heads_bias = heads_bias.reshape(heads, length * length)
    sums = lax.dot_general(three_parts(heads_bias), hot, NT, preferred_element_type=jnp.float32)
    d_table = jnp.sum(sums.reshape(3, heads, entries), 0) * (BIAS_RANGE * sigma * (1.0 - sigma))
    live = (logit_scale < SCALE_CAP).astype(jnp.float32)
    d_scale = jnp.sum(d_cos.reshape(heads, depth // heads), 1) * live
    d_block = from_windows(d_flat.reshape(images, count, length, depth), images, rows, cols, window)
    return (d_block, (d_wqkv, d_wproj, d_table, d_scale, d_gain.reshape(depth)))


def half_turn(value, axis):
    return pltpu.roll(value, value.shape[axis] // 2, axis)


def exp_fine(value):
    whole = jnp.floor(value * LOG2E + 0.5)
    rest = value - whole * 0.693359375 + whole * 2.12194440e-4
    total = jnp.ones_like(rest)
    for k in range(8, 0, -1):
        total = 1.0 + total * rest * (1.0 / k)
    return total * jnp.exp2(whole)


def inverse(value):
    guess = 1.0 / value
    return guess * (2.0 - value * guess)


def place_of(index, window):
    return index // window * (2 * window - 1) + index % window


def expand_bias(table, length, window, groups, out_ref):
    span = table.shape[1]
    f32, b16 = jnp.float32, jnp.bfloat16
    heads = groups * GROUP
    base = jnp.concatenate([jnp.broadcast_to(table[h : h + 1], (window, span)) for h in range(heads)], 0)
    sub = lax.broadcasted_iota(jnp.int32, base.shape, 0) % window
    bit = 1
    while bit < window:
        base = jnp.where(sub // bit % 2 == 1, pltpu.roll(base, bit, 1), base)
        bit *= 2
    top = place_of(length - 1, window)
    turned = [
        pltpu.roll(base, (span - top + (2 * window - 1) * r) % span, 1)[:, : span // 2] for r in range(window)
    ]
    wide = GROUP * length
    row = lax.broadcasted_iota(jnp.int32, (span, wide), 0) % (span // 2)
    col = lax.broadcasted_iota(jnp.int32, (span, wide), 1)
    hit = row == place_of(col % length, window)
    for g in range(groups):
        total = jnp.zeros((length, wide), f32)
        for k in range(GROUP):
            h = g * GROUP + k
            block = jnp.concatenate([t[h * window : (h + 1) * window] for t in turned], 0)
            pair = jnp.concatenate(split(block), 1)
            total = total + mxu(pair, (hit & (col // length == k)).astype(b16), NN)
        out_ref[0, g] = total


def fold_bias(grads, length, window, span):
    f32, b16 = jnp.float32, jnp.bfloat16
    wide = GROUP * length
    row = lax.broadcasted_iota(jnp.int32, (wide, span // 2), 0)
    col = lax.broadcasted_iota(jnp.int32, (wide, span // 2), 1)
    hit = col == place_of(row % length, window)
    both = jnp.concatenate([half for grad in grads for half in split(grad)], 0)
    by_head = [None] * (len(grads) * GROUP)
    for k in range(GROUP):
        pairs = mxu(both, (hit & (row // length == k)).astype(b16), NN)
        for g in range(len(grads)):
            pair = pairs[2 * g * length : (2 * g + 2) * length]
            block = pair[:length] + pair[length:]
            by_head[g * GROUP + k] = jnp.concatenate([block, jnp.zeros_like(block)], 1)
    parts = [
        jnp.concatenate([block[r * window : (r + 1) * window] for block in by_head], 0) for r in range(window)
    ]
    step = 2 * window - 1
    while len(parts) > 1:
        parts = [pltpu.roll(parts[i], step, 1) + parts[i + 1] for i in range(0, len(parts), 2)]
        step *= 2
    total = parts[0]
    sub = window - 1 - lax.broadcasted_iota(jnp.int32, total.shape, 0) % window
    bit = 1
    while bit < window:
        total = jnp.where(sub // bit % 2 == 1, pltpu.roll(total, bit, 1), total)
        bit *= 2
    return [jnp.sum(total[k * window : (k + 1) * window], 0, keepdims=True) for k in range(len(by_head))]


def whole_kernel(
    shape, height, width, window,
    tokens_ref, cot_ref, w_qkv_hbm, w_proj_hbm, table_hbm, gain_hbm, scale_hbm,
    d_tok_ref, grads_out, table_out, scale_out, gain_out,
    tok, cot, w_qkv_ref, w_proj_ref, table_in, gain_ref, scale_ref, table_ref, local_sems,
    col_send, row_get, col_get, diag_get, halo_sems,
    flat_ref, grad_ref, d_flat_ref, d_proj_ref,
    qkv_ref, att_ref, d_att_ref, d_qkv_ref, probs_ref, kinv_ref, qrow_ref, masked_ref, raw_q_ref, raw_k_ref,
    norm_ref, d_bias_ref, p_mid, k_first, product_ref,
    row_back, col_back, row_back_get, col_back_get, diag_back_get, back_sems,
    small, small_core, small_a, small_image, small_b, small_side, small_c, small_near, small_total, tiny_sems,
    *chunk_refs,
):
    size_h, size_w = shape
    chips = size_h // 2
    peers = chips * size_w
    ha, wa, ba = lax.axis_index("ha"), lax.axis_index("wa"), lax.axis_index("ba")
    core = ha % 2
    me = wa * chips + ha // 2
    partner = (ha + 1 - 2 * core, wa, ba)
    image, side, corner = (ha, wa, 1 - ba), (ha, 1 - wa, ba), (ha, 1 - wa, 1 - ba)
    above, below = lax.rem(ha + size_h - 1, size_h), lax.rem(ha + 1, size_h)
    left, right = lax.rem(wa + size_w - 1, size_w), lax.rem(wa + 1, size_w)
    f32, b16 = jnp.float32, jnp.bfloat16

    def peer(step):
        other = lax.rem(me + step, peers)
        return other, (other % chips * 2 + core, other // chips, ba)

    loads = []
    for k, (src, dst) in enumerate(
        (
            (tokens_ref.at[0], tok), (cot_ref.at[0], cot), (w_qkv_hbm, w_qkv_ref), (w_proj_hbm, w_proj_ref),
            (table_hbm, table_in), (gain_hbm, gain_ref), (scale_hbm, scale_ref),
        )
    ):
        copy = pltpu.make_async_copy(src, dst, local_sems.at[k])
        copy.start()
        loads.append(copy)
    targets = [
        (above, wa, ba), (below, wa, ba), (ha, left, ba), (ha, right, ba), (above, left, ba), (below, right, ba),
        partner, image, corner,
    ] + [peer(step)[1] for step in range(1, peers)]
    barrier = pltpu.get_barrier_semaphore()
    for device in targets:
        pl.semaphore_signal(barrier, inc=1, device_id=device, device_id_type=MESH)

    def start(src, dst, sems, device):
        copy = pltpu.make_async_remote_copy(
            src_ref=src, dst_ref=dst, send_sem=sems.at[0], recv_sem=sems.at[1],
            device_id=device, device_id_type=MESH,
        )
        copy.start()
        return copy

    def all_of(src, dst, sems, device):
        return pltpu.make_async_remote_copy(
            src_ref=src, dst_ref=dst, send_sem=sems.at[0], recv_sem=sems.at[1],
            device_id=device, device_id_type=MESH,
        )

    rows, cols, depth = tok.shape
    cut = window // 2
    length = window * window
    across = cols // window
    count = rows // window * across
    fwd, bwd = math.gcd(across, LONG_FWD), math.gcd(count, LONG_BWD)
    tokens = count * length
    groups = qrow_ref.shape[1]
    lanes = depth // groups
    head_dim = lanes // GROUP
    wide = GROUP * length
    low_sub = lax.broadcasted_iota(jnp.int32, (window, depth), 0) < cut

    def pack_columns(a, ref):
        loads[a].wait()
        for j in range(rows // 2):
            first = ref[2 * j, :window, :].astype(f32)
            second = ref[2 * j + 1, :window, :].astype(f32)
            col_send[a, j] = jnp.where(low_sub, first, half_turn(second, 0)).astype(b16)

    halos = {}

    def send_halo(a, ref):
        halos[a, 0] = start(col_send.at[a], col_get.at[a], halo_sems.at[a, 1], (ha, left, ba))
        halos[a, 1] = start(ref.at[pl.ds(0, cut)], row_get.at[a], halo_sems.at[a, 0], (above, wa, ba))
        halos[a, 2] = start(
            col_send.at[a, pl.ds(0, cut // 2)], diag_get.at[a], halo_sems.at[a, 2], (above, left, ba)
        )

    pack_columns(0, tok)
    pl.semaphore_wait(barrier, len(targets))
    send_halo(0, tok)
    pack_columns(1, cot)
    send_halo(1, cot)

    for k in range(4, 7):
        loads[k].wait()
    heads = groups * GROUP
    entries = table_in.shape[1]
    table_ref[...] = jnp.zeros_like(table_ref)
    table_ref[:heads, :entries] = table_in[...]
    sigma = inverse(1.0 + exp_fine(-table_ref[...]))
    head_rows, span = table_ref.shape
    spot = lax.broadcasted_iota(jnp.int32, (head_rows, 128), 0)
    logits = jnp.zeros((head_rows, 128), f32)
    for h in range(heads):
        logits = jnp.where(spot == h, scale_ref[h], logits)
    scale = exp_fine(jnp.minimum(logits, SCALE_CAP))
    expand_bias(sigma * (BIAS_RANGE * LOG2E), length, window, groups, masked_ref)
    mine = lax.broadcasted_iota(jnp.int32, (length, wide), 0)
    other = lax.broadcasted_iota(jnp.int32, (length, wide), 1) % length
    row_off = (mine // window // cut) != (other // window // cut)
    col_off = (mine % window // cut) != (other % window // cut)
    for g in range(groups):
        bias = masked_ref[0, g]
        masked_ref[1, g] = jnp.where(col_off, bias + MASK_FILL * LOG2E, bias)
        masked_ref[2, g] = jnp.where(row_off, bias + MASK_FILL * LOG2E, bias)
        masked_ref[3, g] = jnp.where(row_off | col_off, bias + MASK_FILL * LOG2E, bias)
    small[...] = jnp.zeros_like(small)

    def gather_rows(a, ref, out_ref, from_row, to_row):
        def shifted(i):
            if i + cut < rows:
                row, edge = ref[i + cut], col_get[a, (i + cut) // 2]
            else:
                row, edge = row_get[a, i + cut - rows], diag_get[a, (i + cut - rows) // 2]
            row, edge = row.astype(f32), edge.astype(f32)
            turned = [half_turn(row[k * window : (k + 1) * window], 0) for k in range(across)]
            turned.append(half_turn(edge, 0) if i % 2 == 0 else edge)
            return [jnp.where(low_sub, turned[k], turned[k + 1]) for k in range(across)]

        for i in range(from_row, to_row, 2):
            one, two = shifted(i), shifted(i + 1)
            for k in range(across):
                begin = (i // window * across + k) * length + i % window * window
                out_ref[begin : begin + 2 * window] = jnp.concatenate([one[k], two[k]], 0).astype(b16)

    row_base, col_base = ha * rows, wa * cols
    lane_ones = same_block(lanes, wide, head_dim, length)
    lane_lane = same_block(lanes, lanes, head_dim, head_dim)
    pick = same_block(head_rows, depth, 1, head_dim)
    half = lax.broadcasted_iota(jnp.int32, (1, 2 * length), 1) < length

    def project(begin_window, end_window):
        part_rows = slice(begin_window * length, end_window * length)
        qkv_ref[part_rows] = mxu(flat_ref[part_rows], w_qkv_ref[...], NN).astype(b16)
        high, low = split(jnp.square(qkv_ref[part_rows, :depth].astype(f32)))
        q_sums = mxu(pick, high, NT) + mxu(pick, low, NT)
        q_rows = lax.rsqrt(q_sums + 1.0) * scale[:, :1]
        for j in range(begin_window // 2, end_window // 2):
            shifted_j = 2 * j - begin_window
            base = q_rows[:, shifted_j * length : (shifted_j + 2) * length]
            turned = half_turn(base, 1)
            for g in range(groups):
                for p in range(GROUP // 2):
                    one, two = g * GROUP + 2 * p, g * GROUP + 2 * p + 1
                    place = slice(p * 2 * length, (p + 1) * 2 * length)
                    qrow_ref[2 * j, g, :, place] = jnp.where(half, base[one : one + 1], turned[two : two + 1])
                    qrow_ref[2 * j + 1, g, :, place] = jnp.where(half, turned[one : one + 1], base[two : two + 1])
        for g in range(groups):
            key = qkv_ref[part_rows, depth + g * lanes : depth + (g + 1) * lanes].astype(f32)
            high, low = split(jnp.square(key))
            kinv_ref[g, part_rows] = lax.rsqrt(mxu(high, lane_ones, NN) + mxu(low, lane_ones, NN) + 1.0)

    def norms(begin_window, end_window):
        part_rows = slice(begin_window * length, end_window * length)
        for g in range(groups):
            for part in range(2):
                place = slice(part * depth + g * lanes, part * depth + (g + 1) * lanes)
                high, low = split(jnp.square(qkv_ref[part_rows, place].astype(f32)))
                inv = lax.rsqrt(mxu(high, lane_lane, NN) + mxu(low, lane_lane, NN) + 1.0)
                norm_ref[part, g, part_rows] = inv * inv

    def load(ref, w, g, part):
        return ref[
            pl.ds(pl.multiple_of(w * length, length), length),
            part * depth + g * lanes : part * depth + (g + 1) * lanes,
        ]

    def forward(step, carry):
        units = [(step * fwd + k, g) for k in range(fwd) for g in range(groups)]
        scores = []
        for w, g in units:
            query, key = load(qkv_ref, w, g, 0), load(qkv_ref, w, g, 1)
            raw = mxu(key, tile_heads(query, head_dim), NT)
            last_row = (row_base + w // across * window) // (height - window)
            last_col = (col_base + w % across * window) // (width - window)
            kinv = kinv_ref[g, pl.ds(pl.multiple_of(w * length, length), length), :]
            scores.append(raw * kinv * (qrow_ref[w, g] * LOG2E) + masked_ref[last_row * 2 + last_col, g])
        for (w, g), score in zip(units, scores):
            expo = jnp.exp2(score - jnp.max(score, 0, keepdims=True))
            probs = expo * (1.0 / jnp.sum(expo, 0, keepdims=True))
            probs_ref[w, g] = probs
            att = gather_heads(mxu(probs.astype(b16), load(qkv_ref, w, g, 2), TN), head_dim, length)
            att_ref[
                pl.ds(pl.multiple_of(w * length, length), length), g * lanes : (g + 1) * lanes
            ] = att.astype(b16)
        return carry

    def norm_gradient(begin_window, end_window):
        part_rows = slice(begin_window * length, end_window * length)
        proj = mxu(att_ref[part_rows], w_proj_ref[...], NN)
        centre = proj - jnp.mean(proj, -1, keepdims=True)
        inv_std = lax.rsqrt(jnp.mean(centre * centre, -1, keepdims=True) + EPS_NORM)
        normed = centre * inv_std
        upstream = grad_ref[part_rows].astype(f32)
        d_gain = jnp.sum(upstream * normed, 0, keepdims=True)
        scaled = upstream * gain_ref[...].reshape(1, depth)
        d_proj = inv_std * (
            scaled
            - jnp.mean(scaled, -1, keepdims=True)
            - normed * jnp.mean(scaled * normed, -1, keepdims=True)
        )
        d_proj = d_proj.astype(b16)
        d_proj_ref[part_rows] = d_proj
        d_att_ref[part_rows] = mxu(d_proj, w_proj_ref[...], NT).astype(b16)
        return d_gain

    early = count - across
    halos[0, 0].wait()
    gather_rows(0, tok, flat_ref, 0, rows - window)
    loads[2].wait()
    project(0, early)
    lax.fori_loop(0, early // fwd, forward, 0)
    norms(0, early)
    halos[1, 0].wait()
    gather_rows(1, cot, grad_ref, 0, rows - window)
    loads[3].wait()
    d_gain = norm_gradient(0, early)
    halos[0, 1].wait()
    halos[0, 2].wait()
    gather_rows(0, tok, flat_ref, rows - window, rows)
    project(early, count)
    lax.fori_loop(early // fwd, count // fwd, forward, 0)
    halos[1, 1].wait()
    halos[1, 2].wait()
    gather_rows(1, cot, grad_ref, rows - window, rows)
    d_gain = d_gain + norm_gradient(early, count)
    small[heads : heads + 1, :] = d_gain[:, :span]
    small[heads + 1 : heads + 2, : depth - span] = d_gain[:, span:]
    per = len(chunk_refs) // 4
    chunks = [chunk_refs[c * per : (c + 1) * per] for c in range(4)]
    flying = {}

    def begin(c):
        core_send, core_mine, core_get = chunks[c][:3]
        w = core_send.shape[0] // 2
        for side_of in range(2):
            here = slice(side_of * w, (side_of + 1) * w)
            base = 2 * side_of * w
            theirs = pl.ds(pl.multiple_of(base + (1 - core) * w, 32), w)
            core_send[here] = product_ref[theirs, :].astype(b16)
        flying[c] = start(core_send, core_get, chunks[c][9], partner)
        for side_of in range(2):
            here = slice(side_of * w, (side_of + 1) * w)
            core_mine[here] = product_ref[pl.ds(pl.multiple_of(2 * side_of * w + core * w, 32), w), :]

    def cross(c):
        core_send, core_mine, core_get, plane_send, plane_get = chunks[c][:5]
        flying[c].wait()
        core_mine[...] = core_mine[...] + core_get[...].astype(f32)
        w = plane_send.shape[1]
        for k, (b, y, device) in enumerate(((1 - ba, 1 - wa, corner), (1 - ba, wa, image), (ba, 1 - wa, side))):
            place = pl.ds(pl.multiple_of((2 * b + y) * w, 32), w)
            plane_send[k] = core_mine[place, :].astype(b16)
            start(plane_send.at[k], plane_get.at[k], chunks[c][10], device)
        flying[c] = [all_of(plane_send, plane_get, chunks[c][10], image)]

    def scatter(c):
        core_mine, plane_get, near_send, near_get = chunks[c][1], chunks[c][4], chunks[c][5], chunks[c][6]
        for copy in flying[c]:
            copy.wait()
        w = plane_get.shape[1]
        total = core_mine[pl.ds(pl.multiple_of((2 * ba + wa) * w, 32), w), :]
        for k in range(3):
            total = total + plane_get[k].astype(f32)
        r = near_send.shape[1]
        for j in range(chips):
            near_send[j] = total[j * r : (j + 1) * r].astype(b16)
        for step in range(1, chips):
            far_chip = lax.rem(ha // 2 + step, chips)
            start(near_send.at[far_chip], near_get.at[step - 1], chunks[c][11], (2 * far_chip + core, wa, ba))
        flying[c] = [all_of(near_send.at[pl.ds(0, chips - 1)], near_get, chunks[c][11], partner)]

    def gather(c):
        near_send, near_get, whole = chunks[c][5:8]
        for copy in flying[c]:
            copy.wait()
        total = near_send[ha // 2].astype(f32)
        for step in range(1, chips):
            total = total + near_get[step - 1].astype(f32)
        whole[me] = total.astype(b16)
        for step in range(1, peers):
            start(whole.at[me], whole.at[me], chunks[c][12], peer(step)[1])
        several = whole.at[pl.ds(0, peers - 1)]
        flying[c] = [all_of(several, several, chunks[c][12], partner)]

    def spread_column(c):
        near_send, near_get, whole = chunks[c][5:8]
        for copy in flying[c]:
            copy.wait()
        total = near_send[ha // 2].astype(f32)
        for step in range(1, chips):
            total = total + near_get[step - 1].astype(f32)
        whole[me] = total.astype(b16)
        for step in range(1, chips):
            far_chip = lax.rem(ha // 2 + step, chips)
            start(whole.at[me], whole.at[me], chunks[c][12], (2 * far_chip + core, wa, ba))
        several = whole.at[pl.ds(0, chips - 1)]
        flying[c] = [all_of(several, several, chunks[c][12], partner)]

    def relay(c):
        whole = chunks[c][7]
        for copy in flying[c]:
            copy.wait()
        held = pl.ds(wa * chips, chips)
        flying[c] = [start(whole.at[held], whole.at[held], chunks[c][14], side)]

    def mirror(c):
        whole, core_all = chunks[c][7:9]
        for copy in flying[c]:
            copy.wait()
        flying[c] = start(whole, core_all, chunks[c][13], partner)

    def finish(c):
        put(c, chunks[c][7], core)
        flying[c].wait()
        put(c, chunks[c][8], 1 - core)

    unit = lanes // 2
    proj_at = 3 * depth // 2

    targets_of = [
        [(proj_at + k * unit, proj_at + (1 + k) * unit) for k in range(2)],
        [(k * unit, (3 + k) * unit) for k in range(2)],
        [((4 + k) * unit, (1 + k if k < 2 else 5 + k) * unit) for k in range(4)],
        [(2 * unit, 5 * unit), (3 * unit, 6 * unit), (8 * unit, 0), (proj_at + 2 * unit, proj_at)],
    ]

    def put(c, source, which):
        r = source.shape[1]
        blocks = peers * r // unit
        for k in range(blocks):
            zero, one = targets_of[c][k], targets_of[c][blocks + k]
            row = jnp.where(
                which == 0, jnp.where(ba == 0, zero[0], zero[1]), jnp.where(ba == 0, one[0], one[1])
            )
            for j in range(unit // r):
                grads_out[pl.ds(pl.multiple_of(row + j * r, 8), r), :] = source[k * (unit // r) + j].astype(f32)

    product = mxu(d_proj_ref[...], att_ref[...], TN)
    product_ref[:lanes] = product[:lanes]
    p_mid[...] = product[lanes : 2 * lanes]
    product_ref[lanes : 2 * lanes] = product[2 * lanes :]
    begin(0)

    def backward_group(g):
        def backward(step, total):
            units = [step * bwd + k for k in range(bwd)]
            grads = []
            for w in units:
                d_tall = tile_heads(load(d_att_ref, w, g, 0), head_dim)
                d_probs = mxu(load(qkv_ref, w, g, 2), d_tall, NT)
                d_value = mxu(probs_ref[w, g].astype(b16), d_tall, NN)
                d_qkv_ref[
                    pl.ds(pl.multiple_of(w * length, length), length),
                    2 * depth + g * lanes : 2 * depth + (g + 1) * lanes,
                ] = d_value.astype(b16)
                grads.append(d_probs)
            summed = d_bias_ref[g]
            for w, d_probs in zip(units, grads):
                place = pl.ds(pl.multiple_of(w * length, length), length)
                probs = probs_ref[w, g]
                d_scores = probs * (d_probs - jnp.sum(d_probs * probs, 0, keepdims=True))
                summed = summed + d_scores
                high, low = split(d_scores * kinv_ref[g, place, :] * qrow_ref[w, g])
                both = jnp.concatenate([high, low], 0)
                query, key = load(qkv_ref, w, g, 0), load(qkv_ref, w, g, 1)
                pair = mxu(both, tile_heads(query, head_dim), NN)
                raw_k_ref[place, :] = pair[:length] + pair[length:]
                tall = mxu(both, jnp.concatenate([key, key], 0), TN)
                raw_q_ref[place, :] = gather_heads(tall, head_dim, length)
            d_bias_ref[g] = summed
            return total

        d_bias_ref[g] = jnp.zeros((length, wide), f32)
        lax.fori_loop(0, count // bwd, backward, 0)
        for part, ref in enumerate((raw_q_ref, raw_k_ref)):
            place = slice(part * depth + g * lanes, part * depth + (g + 1) * lanes)
            value, grad = qkv_ref[:, place].astype(f32), ref[...]
            along = value * grad
            if part == 0:
                spot = depth - span + g * lanes
                small[
                    heads + 1 + spot // span : heads + 2 + spot // span, spot % span : spot % span + lanes
                ] = jnp.sum(along, 0, keepdims=True)
            d_qkv_ref[:, place] = (
                grad - value * norm_ref[part, g] * mxu_fine(along, lane_lane, NN)
            ).astype(b16)

    def dense(g):
        joined = jnp.concatenate(
            [d_qkv_ref[:, part * depth + g * lanes : part * depth + (g + 1) * lanes] for part in range(3)], 1
        )
        return mxu(joined, flat_ref[...], TN)

    norms(early, count)
    backward_group(0)
    product = dense(0)
    product_ref[:lanes] = product[:lanes]
    product_ref[lanes : 2 * lanes] = product[2 * lanes :]
    k_first[...] = product[lanes : 2 * lanes]
    begin(1)
    cross(0)
    backward_group(2)
    cross(1)
    product = dense(2)
    product_ref[:lanes] = product[:lanes]
    product_ref[lanes : 2 * lanes] = k_first[...]
    product_ref[2 * lanes : 4 * lanes] = product[lanes:]
    begin(2)
    scatter(0)
    backward_group(1)
    cross(2)
    product = dense(1)
    product_ref[:lanes] = product[:lanes]
    product_ref[lanes : lanes + unit] = product[lanes : lanes + unit]
    product_ref[lanes + unit : 2 * lanes] = p_mid[:unit]
    product_ref[2 * lanes : 3 * lanes] = product[2 * lanes :]
    product_ref[3 * lanes : 3 * lanes + unit] = product[lanes + unit : 2 * lanes]
    product_ref[3 * lanes + unit : 4 * lanes] = p_mid[unit:]
    begin(3)
    scatter(1)
    d_flat_ref[...] = mxu(d_qkv_ref[...], w_qkv_ref[...], NT).astype(b16)

    def back_tiles(i):
        begin_row = i // window * across * length + i % window * window
        return [
            half_turn(d_flat_ref[begin_row + k * length : begin_row + k * length + window].astype(f32), 0)
            for k in range(across)
        ]

    for i in range(0, rows, 2):
        one, two = back_tiles(i), back_tiles(i + 1)
        col_back[i // 2] = jnp.where(low_sub, one[-1], half_turn(two[-1], 0)).astype(b16)
        if i >= rows - cut:
            row_back[i - (rows - cut)] = jnp.concatenate(one, 0).astype(b16)
            row_back[i + 1 - (rows - cut)] = jnp.concatenate(two, 0).astype(b16)
    far = (rows - cut) // 2
    back = [
        start(row_back, row_back_get, back_sems.at[0], (below, wa, ba)),
        start(col_back.at[pl.ds(0, far)], col_back_get, back_sems.at[1], (ha, right, ba)),
        start(col_back.at[pl.ds(far, cut // 2)], diag_back_get, back_sems.at[2], (below, right, ba)),
    ]
    cross(3)
    spread_column(0)
    for k, row in enumerate(fold_bias([d_bias_ref[g] for g in range(groups)], length, window, span)):
        small[k : k + 1, :] = row
    tiny = start(small, small_core, tiny_sems.at[0], partner)

    def put_row(i, turned, edge, odd):
        ahead = [half_turn(edge, 0) if odd else edge] + turned
        out = [jnp.where(low_sub, ahead[k], ahead[k + 1]) for k in range(across)]
        d_tok_ref[i] = (jnp.concatenate(out, 0) + cot[i].astype(f32)).astype(b16)

    scatter(2)
    back[1].wait()
    for i in range(rows - cut):
        put_row(i + cut, back_tiles(i), col_back_get[i // 2].astype(f32), i % 2 == 1)
    spread_column(1)
    tiny.wait()
    small_half = small_a.shape[0]
    my_rows = pl.ds(pl.multiple_of(core * small_half, 8), small_half)
    small_a[...] = small[my_rows, :] + small_core[my_rows, :]
    tiny = start(small_a, small_image, tiny_sems.at[1], image)
    relay(0)
    back[0].wait()
    back[2].wait()
    for i in range(cut):
        whole_row = row_back_get[i].astype(f32)
        turned = [whole_row[k * window : (k + 1) * window] for k in range(across)]
        put_row(i, turned, diag_back_get[i // 2].astype(f32), i % 2 == 1)
    scatter(3)
    tiny.wait()
    small_b[...] = small_a[...] + small_image[...]
    tiny = start(small_b, small_side, tiny_sems.at[2], side)
    spread_column(2)
    mirror(0)
    relay(1)
    tiny.wait()
    small_c[...] = small_b[...] + small_side[...]
    for step in range(1, chips):
        far_chip = lax.rem(ha // 2 + step, chips)
        start(small_c, small_near.at[step - 1], tiny_sems.at[3], (2 * far_chip + core, wa, ba))
    tinies = [all_of(small_near, small_near, tiny_sems.at[3], partner)]
    finish(0)
    gather(3)
    relay(2)
    mirror(1)
    for copy in tinies:
        copy.wait()
    total = small_c[...]
    for step in range(1, chips):
        total = total + small_near[step - 1]
    small_total[my_rows, :] = total
    tiny = start(small_total.at[my_rows], small_total.at[my_rows], tiny_sems.at[4], partner)
    finish(1)
    mirror(2)
    tiny.wait()
    total = small_total[...]
    table_out[...] = (total[: head_rows] * (BIAS_RANGE * sigma * (1.0 - sigma)))[:heads, :entries]
    gain_row = jnp.concatenate([total[heads : heads + 1, :], total[heads + 1 : heads + 2, : depth - span]], 1)
    gain_out[...] = gain_row.reshape(depth)
    sums = jnp.concatenate([total[heads + 1 : heads + 2, depth - span :], total[heads + 2 : heads + 3, :]], 1)
    sums = mxu_fine(jnp.broadcast_to(sums, (8, depth)), same_block(depth, 128, head_dim, 1), NN)[:1]
    at = lax.broadcasted_iota(jnp.int32, (1, 128), 1)
    logits = jnp.zeros((1, 128), f32)
    for h in range(heads):
        logits = jnp.where(at == h, scale_ref[h], logits)
    scale_out[...] = jnp.where(logits < SCALE_CAP, sums, 0.0).reshape(128)[:heads]
    mirror(3)
    finish(2)
    finish(3)


def finish_kernel(tok_ref, grads_ref, table_ref, scale_ref, gain_ref, tok, wq, wp, table, scale, gain, sems):
    cut = wq.shape[0]
    pairs = (
        (grads_ref.at[pl.ds(0, cut)], wq), (grads_ref.at[pl.ds(cut, wp.shape[0])], wp), (tok_ref, tok),
        (table_ref, table), (scale_ref, scale), (gain_ref, gain),
    )
    copies = [pltpu.make_async_copy(src, dst, sems.at[k]) for k, (src, dst) in enumerate(pairs)]
    for copy in copies:
        copy.start()
    for copy in copies:
        copy.wait()


def whole_grads(tokens, cotangent, w_qkv, w_proj, table_logits, logit_scale, gain, height, width, window):
    size_h, size_w = lax.axis_size("ha"), lax.axis_size("wa")
    peers = size_h // 2 * size_w
    f32, b16 = jnp.float32, jnp.bfloat16
    images, rows, cols, depth = tokens.shape
    heads = logit_scale.shape[0]
    entries = table_logits.shape[1]
    groups = heads // GROUP
    lanes = depth // groups
    length = window * window
    wide = GROUP * length
    total = rows * cols
    count = total // length
    cut = window // 2
    span = 256
    head_rows = -(-heads // 16) * 16
    half = depth // 2
    chips = size_h // 2
    dma, vmem = pltpu.SemaphoreType.DMA, pltpu.VMEM
    chunk_scratch = []
    for w in (lanes // 2, lanes // 2, lanes, lanes):
        r = w // peers
        chunk_scratch += [
            vmem((2 * w, depth), b16), vmem((2 * w, depth), f32), vmem((2 * w, depth), b16),
            vmem((3, w // 2, depth), b16), vmem((3, w // 2, depth), b16),
            vmem((chips, r, depth), b16), vmem((chips - 1, r, depth), b16),
            vmem((peers, r, depth), b16), vmem((peers, r, depth), b16),
            dma((2,)), dma((2,)), dma((2,)), dma((2,)), dma((2,)), dma((2,)),
        ]
    small, part = (16, span), (8, span)
    anywhere = pl.BlockSpec(memory_space=pltpu.HBM)
    pinned = [
        pltpu.with_memory_space_constraint(x, pltpu.HBM)
        for x in (tokens, cotangent, w_qkv, w_proj, table_logits, gain, logit_scale)
    ]
    outs = pl.pallas_call(
        functools.partial(whole_kernel, (size_h, size_w), height, width, window),
        out_shape=[
            jax.ShapeDtypeStruct((rows, cols, depth), b16),
            jax.ShapeDtypeStruct((2 * depth, depth), f32),
            jax.ShapeDtypeStruct((heads, entries), f32),
            jax.ShapeDtypeStruct((heads,), f32),
            jax.ShapeDtypeStruct((depth,), f32),
        ],
        in_specs=[anywhere] * 7,
        out_specs=[VMEM] * 5,
        scratch_shapes=[
            vmem((rows, cols, depth), b16), vmem((rows, cols, depth), b16),
            vmem((depth, 3 * depth), b16), vmem((depth, depth), b16),
            vmem((heads, entries), f32), vmem((depth,), f32), pltpu.SMEM((heads,), f32),
            vmem((head_rows, span), f32), dma((7,)),
            vmem((2, rows // 2, window, depth), b16), vmem((2, cut, cols, depth), b16),
            vmem((2, rows // 2, window, depth), b16), vmem((2, cut // 2, window, depth), b16), dma((2, 3, 2)),
            vmem((total, depth), b16), vmem((total, depth), b16), vmem((total, depth), b16), vmem((total, depth), b16),
            vmem((total, 3 * depth), b16), vmem((total, depth), b16), vmem((total, depth), b16),
            vmem((total, 3 * depth), b16), vmem((count, groups, length, wide), f32), vmem((groups, total, wide), f32),
            vmem((count, groups, 1, wide), f32), vmem((4, groups, length, wide), f32),
            vmem((total, lanes), f32), vmem((total, lanes), f32), vmem((2, groups, total, lanes), f32),
            vmem((groups, length, wide), f32), vmem((lanes, depth), f32), vmem((lanes, depth), f32),
            vmem((4 * lanes, depth), f32),
            vmem((cut, cols, depth), b16), vmem((rows // 2, window, depth), b16), vmem((cut, cols, depth), b16),
            vmem(((rows - cut) // 2, window, depth), b16), vmem((cut // 2, window, depth), b16), dma((3, 2)),
            vmem(small, f32), vmem(small, f32), vmem(part, f32), vmem(part, f32), vmem(part, f32), vmem(part, f32),
            vmem(part, f32), vmem((chips - 1, *part), f32), vmem(small, f32), dma((5, 2)),
            *chunk_scratch,
        ],
        compiler_params=pltpu.CompilerParams(
            collective_id=0, has_side_effects=True, vmem_limit_bytes=VMEM_LIMIT
        ),
        name="whole_grads",
    )(*pinned)
    d_tok, half_qkv, half_proj, d_table, d_scale, d_gain = pl.pallas_call(
        finish_kernel,
        out_shape=[
            jax.ShapeDtypeStruct((rows, cols, depth), b16),
            jax.ShapeDtypeStruct((3 * depth // 2, depth), f32),
            jax.ShapeDtypeStruct((depth // 2, depth), f32),
            jax.ShapeDtypeStruct((heads, entries), f32),
            jax.ShapeDtypeStruct((heads,), f32),
            jax.ShapeDtypeStruct((depth,), f32),
        ],
        in_specs=[VMEM] * 5,
        out_specs=[anywhere] * 6,
        scratch_shapes=[dma((6,))],
        compiler_params=pltpu.CompilerParams(vmem_limit_bytes=FINISH_LIMIT),
        name="finish",
    )(*outs)
    return d_tok[None], half_qkv.T, half_proj.T, d_table, d_scale, d_gain


def can_join(tokens, logit_scale):
    size_h, size_w, size_b = (lax.axis_size(name) for name in ("ha", "wa", "ba"))
    images, rows, cols, depth = tokens.shape
    peers = size_h // 2 * size_w
    return (
        images == 1 and size_b == 2 and size_w == 2 and size_h % 2 == 0 and size_h > 2
        and logit_scale.shape[0] == 3 * GROUP and depth == 3 * 128 and WIN == 8
        and rows % WIN == 0 and cols % (2 * WIN) == 0 and rows > WIN
        and 64 % peers == 0 and 64 // peers % 8 == 0
    )


def shift_in(tokens, cotangent, shift):
    stacked = jnp.stack([tokens, cotangent])
    below = from_behind(stacked[:, :, :shift], "ha", -1)
    tall = jnp.concatenate([stacked[:, :, shift:], below], 2)
    beside = from_behind(tall[:, :, :, :shift], "wa", -1)
    moved = jnp.concatenate([tall[:, :, :, shift:], beside], 3)
    return (moved[0], moved[1])


def shift_out(grads, shift):
    rows = grads.shape[1]
    cols = grads.shape[2]
    right = from_behind(grads[:, :, cols - shift :], "wa", 1)
    wide = jnp.concatenate([right, grads[:, :, : cols - shift]], 2)
    lower = from_behind(wide[:, rows - shift :], "ha", 1)
    return jnp.concatenate([lower, wide[:, : rows - shift]], 1)


def shards(tokens, cotangent, w_qkv, w_proj, table_logits, logit_scale, gain):
    rows = tokens.shape[1]
    cols = tokens.shape[2]
    shift = WIN // 2
    height = rows * lax.axis_size("ha")
    width = cols * lax.axis_size("wa")
    row_base = lax.axis_index("ha") * rows
    col_base = lax.axis_index("wa") * cols
    if can_join(tokens, logit_scale):
        return whole_grads(
            tokens, cotangent, w_qkv, w_proj, table_logits, logit_scale, gain, height, width, WIN
        )
    params = (w_qkv, w_proj, table_logits, logit_scale, gain)
    moved, moved_grad = shift_in(tokens, cotangent, shift)
    d_moved, parts = local_grads(moved, moved_grad, row_base, col_base, height, width, WIN, params)
    back = shift_out(d_moved, shift)
    d_tokens = (cotangent.astype(jnp.float32) + back.astype(jnp.float32)).astype(jnp.bfloat16)
    d_wqkv, d_wproj, d_table, d_scale, d_gain = parts
    half_qkv, half_proj = (
        lax.psum_scatter(d_wqkv.astype(jnp.bfloat16), "ba", scatter_dimension=1, tiled=True).astype(jnp.float32),
        lax.psum_scatter(d_wproj.astype(jnp.bfloat16), "ba", scatter_dimension=1, tiled=True).astype(jnp.float32),
    )
    half_qkv, half_proj = lax.psum((half_qkv, half_proj), ("ha", "wa"))
    d_table, d_scale, d_gain = lax.psum((d_table, d_scale, d_gain), ("ha", "wa", "ba"))
    return (d_tokens, half_qkv, half_proj, d_table, d_scale, d_gain)


def solution(mesh):
    return jax.shard_map(
        shards,
        mesh=mesh,
        in_specs=(P("ba", "ha", "wa", None), P("ba", "ha", "wa", None), P(), P(), P(), P(), P()),
        out_specs=(P("ba", "ha", "wa", None), P(None, "ba"), P(None, "ba"), P(), P(), P()),
        check_vma=False,
    )
```
